32 devices in a mesh: ctx: 16 (over z, y, x), fsdp: 2 (over core).
Axes of the slice: x: 2, y: 2, z: 4, core: 2. Of those that a mesh axis runs over, the one named last changes fastest.
Arguments:
- tokens: bfloat16 [4, 2048, 576], P('fsdp', 'ctx'), may hold values from -6 to 6
- positions: int32 [4, 2048], P('fsdp', 'ctx'), may hold values from 0 to 2047, as said below
- norm_attn: bfloat16 [2, 576], P(None, 'fsdp'), may hold values from 0.5 to 1.5
- w_query: bfloat16 [2, 576, 576], P(None, 'fsdp'), may hold values from -0.25 to 0.25
- w_key: bfloat16 [2, 576, 192], P(None, 'fsdp'), may hold values from -0.25 to 0.25
- w_value: bfloat16 [2, 576, 192], P(None, 'fsdp'), may hold values from -0.25 to 0.25
- w_out: bfloat16 [2, 576, 576], P(None, 'fsdp'), may hold values from -2 to 2
- norm_ffn: bfloat16 [2, 576], P(None, 'fsdp'), may hold values from 0.5 to 1.5
- w_gate: bfloat16 [2, 576, 1536], P(None, 'fsdp'), may hold values from -0.25 to 0.25
- w_up: bfloat16 [2, 576, 1536], P(None, 'fsdp'), may hold values from -0.25 to 0.25
- w_down: bfloat16 [2, 1536, 576], P(None, 'fsdp'), may hold values from -0.15625 to 0.15625
- cotangent: bfloat16 [4, 2048, 576], P('fsdp', 'ctx'), may hold values from -6 to 6
Outputs:
- output: bfloat16 [4, 2048, 576], P('fsdp', 'ctx')
- grad_tokens: float32 [4, 2048, 576], P('fsdp', 'ctx')
- grad_norm_attn: float32 [2, 576], P(None, 'fsdp')
- grad_query: float32 [2, 576, 576], P(None, 'fsdp')
- grad_key: float32 [2, 576, 192], P(None, 'fsdp')
- grad_value: float32 [2, 576, 192], P(None, 'fsdp')
- grad_out: float32 [2, 576, 576], P(None, 'fsdp')
- grad_norm_ffn: float32 [2, 576], P(None, 'fsdp')
- grad_gate: float32 [2, 576, 1536], P(None, 'fsdp')
- grad_up: float32 [2, 576, 1536], P(None, 'fsdp')
- grad_down: float32 [2, 1536, 576], P(None, 'fsdp')
The draws below stay inside these ranges and needn't reach their ends.
Inputs may be any that keep to these rules, and one draw needn't show every extreme that they name: For each sequence the 2048 positions are 0 .. 2047 once each; index c of ctx holds, in order, the two runs of 64 consecutive positions of blocks b and 31 - b, with b a permutation over the devices drawn per sequence.
All inputs are finite; a program needn't handle non-finite values.
Results may differ from the reference program's by a relative error of at most 0.02.
Values may be sent and summed in bfloat16 or wider, within the bound.
A program may use at most 320 MiB of HBM per device.

```python
import jax
import jax.numpy as jnp
from jax import lax

D = 576
HEADS = 9
KV_HEADS = 3
HEAD = 64
FF = 1536
LAYERS = 2
BLK = 64
LEN = 2048
SEQ_ALL = 4


def draw_positions(key, part):
    pairs = LEN // (2 * BLK)
    orders = jax.vmap(lambda sub_key: jax.random.permutation(sub_key, pairs))(jax.random.split(jax.random.fold_in(key, 7), SEQ_ALL))
    offsets = jnp.arange(BLK, dtype=jnp.int32)
    first_block = orders[:, :, None] * BLK + offsets[None, None, :]
    second_block = (2 * pairs - 1 - orders)[:, :, None] * BLK + offsets[None, None, :]
    return jnp.concatenate([first_block, second_block], axis=2).reshape(SEQ_ALL, LEN).astype(jnp.int32)


def levels(rng, dims, pieces, low, top_value):
    factor_of, own = 1.0, jax.random.fold_in(rng, 6)
    for position, shards_of in pieces:
        steps = jnp.exp(jax.random.uniform(jax.random.fold_in(own, position), (shards_of,), jnp.float32, low / len(pieces), top_value / len(pieces)))
        factor_of = factor_of * jnp.repeat(steps, dims[position] // shards_of).reshape([-1 if axis == position else 1 for axis in range(len(dims))])
    return factor_of


def scatter_about(rng, extent, width, most, pieces=(), kind=jnp.bfloat16):
    level = levels(rng, extent, pieces, -0.22, 0.18) if pieces else 1.0
    entries = jax.random.normal(rng, extent, jnp.float32) * width * level
    return jnp.minimum(jnp.maximum(entries, -most), most).astype(kind)


def setup_inputs(seed: int = 0) -> dict:
    splits = jax.random.split(jax.random.key(seed), 13)
    return {
        "tokens": scatter_about(splits[0], (SEQ_ALL, LEN, D), 1.0, 6.0, ((0, 2), (1, 16))),
        "positions": draw_positions(jax.random.fold_in(splits[12], 71), 0),
        "norm_attn": jnp.clip(1.0 + 0.1 * jax.random.normal(splits[2], (LAYERS, D), jnp.float32), 0.5, 1.5).astype(jnp.bfloat16),
        "w_query": scatter_about(splits[3], (LAYERS, D, D), D ** -0.5, 0.25, ((1, 2),)),
        "w_key": scatter_about(splits[4], (LAYERS, D, KV_HEADS * HEAD), D ** -0.5, 0.25, ((1, 2),)),
        "w_value": scatter_about(splits[5], (LAYERS, D, KV_HEADS * HEAD), D ** -0.5, 0.25, ((1, 2),)),
        "w_out": scatter_about(splits[6], (LAYERS, D, D), (max(1, D * 32 // LEN)) ** -0.5, 2.0, ((1, 2),)),
        "norm_ffn": jnp.clip(1.0 + 0.1 * jax.random.normal(splits[7], (LAYERS, D), jnp.float32), 0.5, 1.5).astype(jnp.bfloat16),
        "w_gate": scatter_about(splits[8], (LAYERS, D, FF), D ** -0.5, 0.25, ((1, 2),)),
        "w_up": scatter_about(splits[9], (LAYERS, D, FF), D ** -0.5, 0.25, ((1, 2),)),
        "w_down": scatter_about(splits[10], (LAYERS, FF, D), FF ** -0.5, 0.15625, ((1, 2),)),
        "cotangent": scatter_about(splits[11], (SEQ_ALL, LEN, D), 1.0, 6.0, ((0, 2), (1, 16))),
    }


EPS = 1e-05
ROPE_BASE = 100000.0

@jax.custom_vjp
def low(v):
    return lax.optimization_barrier(v.astype(jnp.bfloat16)).astype(jnp.float32)

@jax.custom_vjp
def low_back(v):
    return v

def low_keep(v):
    return (low(v), None)

def low_pass(kept, grad):
    return (grad,)

def back_keep(v):
    return (v, None)

def back_low(kept, grad):
    return (low(grad),)
low.defvjp(low_keep, low_pass)
low_back.defvjp(back_keep, back_low)

def product(left, right):
    return jnp.dot(left, right, precision=lax.Precision.HIGHEST)

def rotate(tensor, positions_row, direction_sign):
    half_size = tensor.shape[-1] // 2
    frequency = jnp.exp(jnp.arange(half_size, dtype=jnp.float32) * (-jnp.log(ROPE_BASE) / half_size))
    angles = positions_row.astype(jnp.float32)[..., None] * frequency
    cosine = jnp.cos(angles)[..., None, :]
    sine_part = direction_sign * jnp.sin(angles)[..., None, :]
    first_half = tensor[..., :half_size]
    second_half = tensor[..., half_size:]
    return jnp.concatenate([first_half * cosine - second_half * sine_part, second_half * cosine + first_half * sine_part], axis=-1)

def normalize(values, gain):
    return values * lax.rsqrt(lax.optimization_barrier(jnp.mean(values * values, axis=-1, keepdims=True)) + EPS) * gain

def block(sequence, positions_row, weights):
    gain_attn, w_query, w_key, w_value, w_out, gain_ffn, w_gate, w_up, w_down = weights
    length = sequence.shape[0]
    normed = low(normalize(sequence, gain_attn))
    query_pre = low_back(product(normed, w_query)).reshape(length, HEADS, HEAD)
    key_pre = low_back(product(normed, w_key)).reshape(length, KV_HEADS, HEAD)
    values = low_back(low(product(normed, w_value))).reshape(length, KV_HEADS, HEAD)
    queries = low(rotate(query_pre, positions_row, 1.0)).reshape(length, KV_HEADS, HEADS // KV_HEADS, HEAD)
    keys = low(rotate(key_pre, positions_row, 1.0))
    visible = positions_row[None, :] <= positions_row[:, None]

    def one_group(operands):
        group_queries, group_keys, group_values = operands
        raw_scores = jnp.einsum('qge,ke->gqk', group_queries, group_keys, precision=lax.Precision.HIGHEST) * HEAD ** (-0.5)
        scores = low_back(jnp.where(visible[None], raw_scores, -1e+30))
        row_top = lax.optimization_barrier(jnp.max(scores, axis=-1, keepdims=True))
        exponent = jnp.exp(scores - row_top)
        probabilities = low(exponent / lax.optimization_barrier(jnp.sum(exponent, axis=-1, keepdims=True)))
        return jnp.einsum('gqk,ke->qge', probabilities, group_values, precision=lax.Precision.HIGHEST)
    mixed = lax.map(jax.checkpoint(one_group), (jnp.transpose(queries, (1, 0, 2, 3)), jnp.transpose(keys, (1, 0, 2)), jnp.transpose(values, (1, 0, 2))))
    mixed = low_back(low(jnp.transpose(mixed, (1, 0, 2, 3)).reshape(length, HEADS * HEAD)))
    middle = sequence + low_back(product(mixed, w_out))
    normed_ffn = low(normalize(middle, gain_ffn))
    gate_pre = low_back(product(normed_ffn, w_gate))
    up_pre = low_back(product(normed_ffn, w_up))
    hidden = low(jax.nn.silu(gate_pre) * up_pre)
    return middle + low_back(product(hidden, w_down))

def reference(tokens, positions, norm_attn, w_query, w_key, w_value, w_out, norm_ffn, w_gate, w_up, w_down, cotangent):
    params = (norm_attn.astype(jnp.float32), w_query.astype(jnp.float32), w_key.astype(jnp.float32), w_value.astype(jnp.float32), w_out.astype(jnp.float32), norm_ffn.astype(jnp.float32), w_gate.astype(jnp.float32), w_up.astype(jnp.float32), w_down.astype(jnp.float32))

    def forward(inputs, weights):

        def sequence_pass(operands):
            sequence, positions_row = operands
            for layer_index in range(LAYERS):
                sequence = block(sequence, positions_row, tuple((member[layer_index] for member in weights)))
            return sequence
        return lax.map(sequence_pass, (inputs, positions))
    result, pullback = jax.vjp(forward, tokens.astype(jnp.float32), params)
    grad_tokens, layer_grads = pullback(cotangent.astype(jnp.float32))
    return (result.astype(jnp.bfloat16), grad_tokens, layer_grads[0], layer_grads[1], layer_grads[2], layer_grads[3], layer_grads[4], layer_grads[5], layer_grads[6], layer_grads[7], layer_grads[8])
```

```python
import functools, itertools
import jax
import jax.numpy as jnp
from jax import lax
from jax.experimental import pallas as pl
from jax.experimental.pallas import tpu as pltpu

CTX, FSDP = "ctx", "fsdp"
MESH = pl.DeviceIdType.MESH


def factors(n):
    known = {16: (4, 2, 2), 64: (2, 4, 4, 2)}
    if n in known:
        return known[n]
    out, p = [], 2
    while n > 1:
        while n % p == 0:
            out.append(p)
            n //= p
        p += 1
    return tuple(out) or (1,)


class Grid:
    def __init__(self, n):
        self.n = n
        self.dims = factors(n)
        strides, s = [], 1
        for d in reversed(self.dims):
            strides.insert(0, s)
            s *= d
        self.strides = tuple(strides)
        self.all = list(itertools.product(*[range(d) for d in self.dims]))
        self.ident = {d: i for i, d in enumerate(self.all)}

    def locate(self):
        me = lax.axis_index(CTX)
        self.me = me
        self.at = [lax.rem(me // s, d) for s, d in zip(self.strides, self.dims)]

    def index(self, delta):
        out = 0
        for c, d, n, s in zip(self.at, delta, self.dims, self.strides):
            out = out + (lax.rem(c + d, n) if d else c) * s
        return out

    def peer(self, axis, j):
        return self.index(tuple(j if a == axis else 0 for a in range(len(self.dims))))

    def orders(self):
        rest = list(range(1, len(self.dims)))
        return [[0] + rest, [0] + rest[::-1]]


def entry_barrier(g, fsdp):
    sem = pltpu.get_barrier_semaphore()
    count = 0
    f = lax.axis_index(FSDP)
    for a, d in enumerate(g.dims):
        for j in range(1, d):
            pl.semaphore_signal(sem, inc=1, device_id=(g.peer(a, j), f), device_id_type=MESH)
            count += 1
    if fsdp:
        pl.semaphore_signal(sem, inc=1, device_id=(g.me, 1 - f), device_id_type=MESH)
        count += 1
    pl.semaphore_wait(sem, count)


class Gather:
    def __init__(self, g, order, own, slot, send, recv):
        self.g, self.order, self.own, self.slot, self.send, self.recv = g, order, own, slot, send, recv
        self.copies = {}

    def _copy(self, delta, axis, j, src):
        g = self.g
        label = tuple((g.dims[a] - j) % g.dims[a] if a == axis else delta[a] for a in range(len(g.dims)))
        i = g.ident[label]
        c = pltpu.make_async_remote_copy(
            src_ref=src, dst_ref=self.slot(g.index(delta)), send_sem=self.send.at[i], recv_sem=self.recv.at[i],
            device_id=(g.peer(axis, j), lax.axis_index(FSDP)), device_id_type=MESH)
        self.copies[label] = c
        return c

    def forward(self, delta, stage, src):
        for k in range(stage, len(self.order)):
            a = self.order[k]
            for j in range(1, self.g.dims[a]):
                self._copy(delta, a, j, src).start()

    def begin(self):
        self.forward((0,) * len(self.g.dims), 0, self.own)

    def labels(self, stage):
        g, order = self.g, self.order
        done = set(order[:stage])
        out = []
        for d in g.all:
            if d[order[stage]] and all(d[a] == 0 for a in order[stage + 1:]):
                out.append(d)
        return out

    def arrive(self, label, stage):
        i = self.g.ident[label]
        here = self.slot(self.g.index(label))
        self.copies[label].wait_recv()
        self.forward(label, stage + 1, here)

    def end(self):
        for c in self.copies.values():
            c.wait_send()


def gather_kernel(g, x_ref, o_ref, send, recv, local):
    g.locate()
    entry_barrier(g, False)
    parts = x_ref.shape[0]
    ords = g.orders()
    gs = []
    for p in range(parts):
        gs.append(Gather(g, ords[p % len(ords)], x_ref.at[p], (lambda p: lambda i: o_ref.at[p, i])(p), send.at[p], recv.at[p]))
    for q in gs:
        q.begin()
    mine = [pltpu.make_async_copy(x_ref.at[p], o_ref.at[p, g.me], local.at[p]) for p in range(parts)]
    for m in mine:
        m.start()
    for stage in range(len(g.dims)):
        lists = [q.labels(stage) for q in gs]
        for i in range(max(map(len, lists))):
            for q, l in zip(gs, lists):
                if i < len(l):
                    q.arrive(l[i], stage)
    for m in mine:
        m.wait()
    for q in gs:
        q.end()


def all_gather_ctx(x, n, cid):
    g = Grid(n)
    parts, rows, cols = x.shape
    return pl.pallas_call(
        functools.partial(gather_kernel, g),
        out_shape=jax.ShapeDtypeStruct((parts, n, rows, cols), x.dtype),
        in_specs=[pl.BlockSpec(memory_space=pltpu.VMEM)],
        out_specs=pl.BlockSpec(memory_space=pltpu.VMEM),
        scratch_shapes=[pltpu.SemaphoreType.DMA((parts, n)), pltpu.SemaphoreType.DMA((parts, n)), pltpu.SemaphoreType.DMA((parts,))],
        compiler_params=pltpu.CompilerParams(collective_id=cid, has_side_effects=True, vmem_limit_bytes=60 << 20),
        name="ctx_gather",
    )(x)


def add_into(out, refs):
    rows = out.shape[0]
    step = max(s for s in range(16, 129, 16) if rows % s == 0)

    def some(i, carry):
        at = pl.ds(pl.multiple_of(i * step, step), step)
        out[at] = sum(r[at].astype(jnp.float32) for r in refs).astype(out.dtype)
        return carry

    lax.fori_loop(0, rows // step, some, 0)


class Reduce:
    def __init__(self, g, order, src, acc, land, send, recv):
        self.g, self.order, self.src, self.acc, self.land, self.send, self.recv = g, order, src, acc, land, send, recv
        self.copies = {}
        self.fresh = set(g.all)

    def held(self, delta):
        return self.src(self.g.index(delta)) if delta in self.fresh else self.acc(self.g.ident[delta])

    def live(self, stage):
        gone = set(self.order[:stage])
        return [d for d in self.g.all if all(d[a] == 0 for a in gone)]

    def send_block(self, d, stage):
        g, a = self.g, self.order[stage]
        i = g.ident[d]
        c = pltpu.make_async_remote_copy(
            src_ref=self.held(d), dst_ref=self.land(i), send_sem=self.send.at[i], recv_sem=self.recv.at[i],
            device_id=(g.peer(a, d[a]), lax.axis_index(FSDP)), device_id_type=MESH)
        self.copies[d] = c
        c.start()

    def weight(self, d, stage):
        return sum(1 for a in self.order[stage:] if d[a])

    def add(self, d, stage, out=None):
        g, a = self.g, self.order[stage]
        refs = [self.held(d)]
        for j in range(1, g.dims[a]):
            label = tuple(j if b == a else d[b] for b in range(len(d)))
            self.copies[label].wait_recv()
            refs.append(self.land(g.ident[label]))
        add_into(self.acc(g.ident[d]) if out is None else out, refs)
        if out is None:
            self.fresh.discard(d)

    def end(self):
        for c in self.copies.values():
            c.wait_send()


def run_reduces(g, rs, outs):
    last = len(g.dims) - 1
    for r in rs:
        first = [d for d in g.all if d[r.order[0]]]
        first.sort(key=lambda d: -r.weight(d, 0))
        r.pending = first
    for i in range(max(len(r.pending) for r in rs)):
        for r in rs:
            if i < len(r.pending):
                r.send_block(r.pending[i], 0)
    for stage in range(len(g.dims)):
        lists = []
        for r in rs:
            l = [d for d in r.live(stage + 1)]
            l.sort(key=lambda d: -r.weight(d, stage + 1))
            lists.append(l)
        for i in range(max(map(len, lists))):
            for r, l, o in zip(rs, lists, outs):
                if i < len(l):
                    if stage == last:
                        r.add(l[i], stage, o)
                    else:
                        r.add(l[i], stage)
                        if l[i][r.order[stage + 1]]:
                            r.send_block(l[i], stage + 1)


def scatter_kernel(g, x_ref, o_ref, acc, land, send, recv):
    g.locate()
    entry_barrier(g, False)
    parts = x_ref.shape[0]
    ords = [o[::-1] for o in g.orders()]
    rs = []
    for p in range(parts):
        rs.append(Reduce(g, ords[p % 2], (lambda p: lambda i: x_ref.at[p, i])(p), (lambda p: lambda i: acc.at[p, i])(p),
                         (lambda p: lambda i: land.at[p, i])(p), send.at[p], recv.at[p]))
    run_reduces(g, rs, [o_ref.at[p] for p in range(parts)])
    for r in rs:
        r.end()


def reduce_scatter_ctx(x, n, cid):
    g = Grid(n)
    parts, _, rows, cols = x.shape
    return pl.pallas_call(
        functools.partial(scatter_kernel, g),
        out_shape=jax.ShapeDtypeStruct((parts, rows, cols), jnp.float32),
        in_specs=[pl.BlockSpec(memory_space=pltpu.VMEM)],
        out_specs=pl.BlockSpec(memory_space=pltpu.VMEM),
        scratch_shapes=[pltpu.VMEM((parts, n, rows, cols), x.dtype), pltpu.VMEM((parts, n, rows, cols), x.dtype),
                        pltpu.SemaphoreType.DMA((parts, n)), pltpu.SemaphoreType.DMA((parts, n))],
        compiler_params=pltpu.CompilerParams(collective_id=cid, has_side_effects=True, vmem_limit_bytes=60 << 20),
        name="ctx_reduce",
    )(x)


def reduce_all_kernel(g, x_ref, o_ref, acc, land, pair, fsum, send, recv, gsend, grecv, psend, precv):
    g.locate()
    entry_barrier(g, True)
    f = lax.axis_index(FSDP)
    parts = x_ref.shape[1]
    n = g.n
    gords = g.orders()
    ords = [o[::-1] for o in gords]
    pairs = {}
    rs, gs = [], []
    for p in range(parts):
        rs.append(Reduce(g, ords[p % 2], (lambda p: lambda i: fsum.at[p, i])(p), (lambda p: lambda i: acc.at[p, i])(p),
                         (lambda p: lambda i: land.at[p, i])(p), send.at[p], recv.at[p]))
        gs.append(Gather(g, gords[p % 2], o_ref.at[p, g.me], (lambda p: lambda i: o_ref.at[p, i])(p), gsend.at[p], grecv.at[p]))
    seq = []
    for r in rs:
        l = sorted(g.all, key=lambda d: -r.weight(d, 0) - (10 if d[r.order[0]] else 0))
        seq.append(l)
    for i in range(n):
        for p in range(parts):
            d = seq[p][i]
            k = g.index(d)
            c = pltpu.make_async_remote_copy(
                src_ref=x_ref.at[1 - f, p, k], dst_ref=pair.at[p, k], send_sem=psend.at[p, g.ident[d]], recv_sem=precv.at[p, g.ident[d]],
                device_id=(g.me, 1 - f), device_id_type=MESH)
            c.start()
            pairs[p, d] = c
    for i in range(n):
        for p in range(parts):
            d = seq[p][i]
            k = g.index(d)
            pairs[p, d].wait_recv()
            add_into(fsum.at[p, k], [x_ref.at[f, p, k], pair.at[p, k]])
            if d[rs[p].order[0]]:
                rs[p].send_block(d, 0)
    last = len(g.dims) - 1
    for stage in range(len(g.dims)):
        lists = []
        for r in rs:
            l = [d for d in r.live(stage + 1)]
            l.sort(key=lambda d: -r.weight(d, stage + 1))
            lists.append(l)
        for i in range(max(map(len, lists))):
            for p, (r, l) in enumerate(zip(rs, lists)):
                if i < len(l):
                    if stage == last:
                        r.add(l[i], stage, o_ref.at[p, g.me])
                        gs[p].begin()
                    else:
                        r.add(l[i], stage)
                        if l[i][r.order[stage + 1]]:
                            r.send_block(l[i], stage + 1)
    for stage in range(len(g.dims)):
        lists = [q.labels(stage) for q in gs]
        for i in range(max(map(len, lists))):
            for q, l in zip(gs, lists):
                if i < len(l):
                    q.arrive(l[i], stage)
    for c in pairs.values():
        c.wait_send()
    for r in rs:
        r.end()
    for q in gs:
        q.end()


def reduce_all(x, n, cid):
    g = Grid(n)
    _, parts, _, rows, cols = x.shape
    blk = (parts, n, rows, cols)
    return pl.pallas_call(
        functools.partial(reduce_all_kernel, g),
        out_shape=jax.ShapeDtypeStruct(blk, x.dtype),
        in_specs=[pl.BlockSpec(memory_space=pltpu.VMEM)],
        out_specs=pl.BlockSpec(memory_space=pltpu.VMEM),
        scratch_shapes=[pltpu.VMEM(blk, x.dtype)] * 4 + [pltpu.SemaphoreType.DMA((parts, n))] * 6,
        compiler_params=pltpu.CompilerParams(collective_id=cid, has_side_effects=True, vmem_limit_bytes=64 << 20),
        name="grad_reduce",
    )(x)


from jax.sharding import PartitionSpec as P

HEADS = 9
KV_HEADS = 3
HEAD = 64


EPS = 1e-05
ROPE_BASE = 100000.0


def rotate(tensor, positions_row, direction_sign):
    half_size = tensor.shape[-1] // 2
    frequency = jnp.exp(
        jnp.arange(half_size, dtype=jnp.float32) * (-jnp.log(ROPE_BASE) / half_size)
    )
    angles = positions_row.astype(jnp.float32)[..., None] * frequency
    cosine = jnp.cos(angles)[..., None, :]
    sine_part = direction_sign * jnp.sin(angles)[..., None, :]
    first_half = tensor[..., :half_size]
    second_half = tensor[..., half_size:]
    return jnp.concatenate(
        [
            first_half * cosine - second_half * sine_part,
            second_half * cosine + first_half * sine_part,
        ],
        axis=-1,
    )


def normalize(values, gain):
    return values * lax.rsqrt(jnp.mean(values * values, axis=-1, keepdims=True) + EPS) * gain


def normalize_back(values, gain, incoming):
    inverse = lax.rsqrt(jnp.mean(values * values, axis=-1, keepdims=True) + EPS)
    scaled = incoming * gain
    grad_values = inverse * scaled - values * (inverse * inverse * inverse) * jnp.mean(
        scaled * values, axis=-1, keepdims=True
    )
    grad_gain = jnp.sum(incoming * values * inverse, axis=(0, 1))
    return (grad_values, grad_gain)


def scores_of(queries, keys_all, query_places, key_places):
    raw_scores = jnp.einsum(
        "qhge,khe->hgqk", queries, keys_all, preferred_element_type=jnp.float32
    ) * queries.shape[-1] ** (-0.5)
    visible = key_places[None, :] <= query_places[:, None]
    return jnp.where(visible[None, None], raw_scores, -1e30)


def attend(operands):
    queries, keys_all, values_all, query_places, key_places = operands
    scores = scores_of(queries, keys_all, query_places, key_places)
    row_top = jnp.max(scores, axis=-1, keepdims=True)
    exponent = jnp.exp(scores - row_top)
    row_total = jnp.sum(exponent, axis=-1, keepdims=True)
    probabilities = (exponent / row_total).astype(jnp.bfloat16)
    mixed = jnp.einsum(
        "hgqk,khe->qhge", probabilities, values_all, preferred_element_type=jnp.float32
    )
    return (mixed, row_top + jnp.log(row_total))


def attend_back(operands):
    queries, keys_all, values_all, query_places, key_places, log_total, grad_mixed = operands
    score_scale = queries.shape[-1] ** (-0.5)
    scores = scores_of(queries, keys_all, query_places, key_places)
    probabilities = jnp.exp(scores - log_total)
    grad_probs = jnp.einsum(
        "qhge,khe->hgqk", grad_mixed, values_all, preferred_element_type=jnp.float32
    )
    grad_scores = (
        probabilities * (grad_probs - jnp.sum(probabilities * grad_probs, axis=-1, keepdims=True))
    ).astype(jnp.bfloat16)
    grad_queries = (
        jnp.einsum("hgqk,khe->qhge", grad_scores, keys_all, preferred_element_type=jnp.float32)
        * score_scale
    )
    grad_keys = (
        jnp.einsum("hgqk,qhge->khe", grad_scores, queries, preferred_element_type=jnp.float32)
        * score_scale
    )
    grad_values = jnp.einsum(
        "hgqk,qhge->khe",
        probabilities.astype(jnp.bfloat16),
        grad_mixed,
        preferred_element_type=jnp.float32,
    )
    return (grad_queries, grad_keys, grad_values)


def layer_forward(inputs, positions, places, weights, layer_index):
    gain_attn, w_query, w_key, w_value, w_out, gain_ffn, w_gate, w_up, w_down = weights
    seq_count, row_count, model_width = inputs.shape
    normed = normalize(inputs, gain_attn).astype(jnp.bfloat16)
    query_pre = jnp.einsum("srd,de->sre", normed, w_query, preferred_element_type=jnp.float32)
    key_pre = jnp.einsum("srd,de->sre", normed, w_key, preferred_element_type=jnp.float32)
    value_pre = jnp.einsum("srd,de->sre", normed, w_value, preferred_element_type=jnp.float32)
    queries = rotate(query_pre.reshape(seq_count, row_count, HEADS, HEAD), positions, 1.0).astype(
        jnp.bfloat16
    )
    queries = queries.reshape(seq_count, row_count, KV_HEADS, HEADS // KV_HEADS, HEAD)
    keys_own = rotate(key_pre.reshape(seq_count, row_count, KV_HEADS, HEAD), positions, 1.0).astype(
        jnp.bfloat16
    )
    keys_own = keys_own.reshape(seq_count, row_count, KV_HEADS * HEAD)
    values_own = value_pre.astype(jnp.bfloat16)
    devices = lax.axis_size("ctx")
    both = all_gather_ctx(jnp.concatenate([keys_own, values_own], axis=-1), devices, 2 + layer_index)
    both = both.reshape(seq_count, devices * row_count, 2 * KV_HEADS * HEAD)
    keys_all, values_all = both[..., : KV_HEADS * HEAD], both[..., KV_HEADS * HEAD :]
    length = keys_all.shape[1]
    mixed, log_total = lax.map(
        attend,
        (
            queries,
            keys_all.reshape(seq_count, length, KV_HEADS, HEAD),
            values_all.reshape(seq_count, length, KV_HEADS, HEAD),
            positions,
            places,
        ),
    )
    mixed_low = mixed.reshape(seq_count, row_count, model_width).astype(jnp.bfloat16)
    middle = inputs + jnp.einsum(
        "srd,de->sre", mixed_low, w_out, preferred_element_type=jnp.float32
    )
    normed_ffn = normalize(middle, gain_ffn).astype(jnp.bfloat16)
    gate_pre = jnp.einsum("srd,df->srf", normed_ffn, w_gate, preferred_element_type=jnp.float32)
    up_pre = jnp.einsum("srd,df->srf", normed_ffn, w_up, preferred_element_type=jnp.float32)
    hidden = (jax.nn.silu(gate_pre) * up_pre).astype(jnp.bfloat16)
    result = middle + jnp.einsum("srf,fd->srd", hidden, w_down, preferred_element_type=jnp.float32)
    record = (
        inputs,
        normed,
        queries,
        keys_own,
        values_own,
        keys_all,
        values_all,
        log_total,
        mixed_low,
        middle,
        normed_ffn,
        gate_pre,
        up_pre,
        hidden,
    )
    return (result, record)


def layer_backward(gradient, record, weights, positions, places, layer_index):
    gain_attn, w_query, w_key, w_value, w_out, gain_ffn, w_gate, w_up, w_down = weights
    (
        inputs,
        normed,
        queries,
        keys_own,
        values_own,
        kept_keys,
        kept_values,
        log_total,
        mixed_low,
        middle,
        normed_ffn,
        gate_pre,
        up_pre,
        hidden,
    ) = record
    seq_count, row_count, model_width = inputs.shape
    grad_low = gradient.astype(jnp.bfloat16)
    grad_wdown = jnp.einsum("srf,srd->fd", hidden, grad_low, preferred_element_type=jnp.float32)
    grad_hidden = jnp.einsum("srd,fd->srf", grad_low, w_down, preferred_element_type=jnp.float32)
    sigmoid_gate = jax.nn.sigmoid(gate_pre)
    grad_gate = (
        grad_hidden * up_pre * sigmoid_gate * (1.0 + gate_pre * (1.0 - sigmoid_gate))
    ).astype(jnp.bfloat16)
    grad_up = (grad_hidden * gate_pre * sigmoid_gate).astype(jnp.bfloat16)
    grad_wgate = jnp.einsum(
        "srd,srf->df", normed_ffn, grad_gate, preferred_element_type=jnp.float32
    )
    grad_wup = jnp.einsum("srd,srf->df", normed_ffn, grad_up, preferred_element_type=jnp.float32)
    grad_normed_ffn = jnp.einsum(
        "srf,df->srd", grad_gate, w_gate, preferred_element_type=jnp.float32
    ) + jnp.einsum("srf,df->srd", grad_up, w_up, preferred_element_type=jnp.float32)
    grad_middle_norm, grad_gain_ffn = normalize_back(middle, gain_ffn, grad_normed_ffn)
    grad_middle = gradient + grad_middle_norm
    branch_low = grad_middle.astype(jnp.bfloat16)
    grad_wout = jnp.einsum("srd,sre->de", mixed_low, branch_low, preferred_element_type=jnp.float32)
    grad_mixed = jnp.einsum(
        "sre,de->srd", branch_low, w_out, preferred_element_type=jnp.float32
    ).astype(jnp.bfloat16)
    grad_mixed = grad_mixed.reshape(seq_count, row_count, KV_HEADS, HEADS // KV_HEADS, HEAD)
    keys_all, values_all = kept_keys, kept_values
    length = keys_all.shape[1]
    grad_queries, grad_keys_all, grad_values_all = lax.map(
        attend_back,
        (
            queries,
            keys_all.reshape(seq_count, length, KV_HEADS, HEAD),
            values_all.reshape(seq_count, length, KV_HEADS, HEAD),
            positions,
            places,
            log_total,
            grad_mixed,
        ),
    )
    devices = lax.axis_size("ctx")
    both = jnp.concatenate(
        [
            grad_keys_all.reshape(seq_count, length, KV_HEADS * HEAD),
            grad_values_all.reshape(seq_count, length, KV_HEADS * HEAD),
        ],
        axis=-1,
    ).astype(jnp.bfloat16)
    both = reduce_scatter_ctx(both.reshape(seq_count, devices, row_count, -1), devices, 4 + layer_index)
    grad_keys, grad_values = both[..., : KV_HEADS * HEAD], both[..., KV_HEADS * HEAD :]
    grad_query_pre = (
        rotate(grad_queries.reshape(seq_count, row_count, HEADS, HEAD), positions, -1.0)
        .reshape(seq_count, row_count, model_width)
        .astype(jnp.bfloat16)
    )
    grad_key_pre = (
        rotate(grad_keys.reshape(seq_count, row_count, KV_HEADS, HEAD), positions, -1.0)
        .reshape(seq_count, row_count, KV_HEADS * HEAD)
        .astype(jnp.bfloat16)
    )
    grad_value_pre = grad_values.astype(jnp.bfloat16)
    grad_wquery = jnp.einsum(
        "srd,sre->de", normed, grad_query_pre, preferred_element_type=jnp.float32
    )
    grad_wkey = jnp.einsum("srd,sre->de", normed, grad_key_pre, preferred_element_type=jnp.float32)
    grad_wvalue = jnp.einsum(
        "srd,sre->de", normed, grad_value_pre, preferred_element_type=jnp.float32
    )
    grad_normed = jnp.einsum(
        "sre,de->srd", grad_query_pre, w_query, preferred_element_type=jnp.float32
    )
    grad_normed = grad_normed + jnp.einsum(
        "sre,de->srd", grad_key_pre, w_key, preferred_element_type=jnp.float32
    )
    grad_normed = grad_normed + jnp.einsum(
        "sre,de->srd", grad_value_pre, w_value, preferred_element_type=jnp.float32
    )
    grad_input_norm, grad_gain_attn = normalize_back(inputs, gain_attn, grad_normed)
    layer_grads = (
        grad_gain_attn,
        grad_wquery,
        grad_wkey,
        grad_wvalue,
        grad_wout,
        grad_gain_ffn,
        grad_wgate,
        grad_wup,
        grad_wdown,
    )
    return (grad_middle + grad_input_norm, layer_grads)


def pair_kernel(*refs):
    count = len(refs) // 2 - 1
    srcs, dsts, send, recv = refs[:count], refs[count : 2 * count], refs[-2], refs[-1]
    c, f = lax.axis_index(CTX), lax.axis_index(FSDP)
    sem = pltpu.get_barrier_semaphore()
    pl.semaphore_signal(sem, inc=1, device_id=(c, 1 - f), device_id_type=MESH)
    pl.semaphore_wait(sem, 1)
    copies = [
        pltpu.make_async_remote_copy(
            src_ref=s, dst_ref=d, send_sem=send.at[i], recv_sem=recv.at[i], device_id=(c, 1 - f), device_id_type=MESH
        )
        for i, (s, d) in enumerate(zip(srcs, dsts))
    ]
    for x in copies:
        x.start()
    for x in copies:
        x.wait()


def pair_exchange(arrays, cid):
    any_space = pl.BlockSpec(memory_space=pl.ANY)
    return pl.pallas_call(
        pair_kernel,
        out_shape=[jax.ShapeDtypeStruct(a.shape, a.dtype) for a in arrays],
        in_specs=[any_space] * len(arrays),
        out_specs=[any_space] * len(arrays),
        scratch_shapes=[pltpu.SemaphoreType.DMA((len(arrays),))] * 2,
        compiler_params=pltpu.CompilerParams(collective_id=cid, has_side_effects=True),
        name="pair_exchange",
    )(*arrays)


def tiled(grad):
    rows, cols = grad.shape[0] // 2, grad.shape[1]
    wide = -(-cols // 128) * 128
    grad = jnp.pad(grad.astype(jnp.bfloat16), ((0, 0), (0, wide - cols)))
    grad = grad.reshape(2, rows, wide // 128, 128).transpose(0, 2, 1, 3)
    return grad.reshape(2, -1, 16, 128)


def untiled(tiles, rows, cols):
    wide = -(-cols // 128)
    return tiles.reshape(wide, rows, 128).transpose(1, 0, 2).reshape(rows, wide * 128)[:, :cols].astype(jnp.float32)


def body(
    tokens,
    positions,
    norm_attn,
    w_query,
    w_key,
    w_value,
    w_out,
    norm_ffn,
    w_gate,
    w_up,
    w_down,
    cotangent,
):
    layer_count = norm_attn.shape[0]
    devices = lax.axis_size("ctx")
    places = lax.all_gather(positions, "ctx", axis=1, tiled=True)
    own = (norm_attn, w_query, w_key, w_value, w_out, norm_ffn, w_gate, w_up, w_down)
    other = pair_exchange(own, 0)
    first = lax.axis_index("fsdp") == 0
    full = [
        jnp.where(first, jnp.concatenate([o, t], axis=1), jnp.concatenate([t, o], axis=1)) for o, t in zip(own, other)
    ]
    current = tokens.astype(jnp.float32)
    records = []
    for layer_index in range(layer_count):
        weights = tuple(w[layer_index] for w in full)
        current, record = layer_forward(current, positions, places, weights, layer_index)
        records.append(record)
    output = current.astype(jnp.bfloat16)
    gradient = cotangent.astype(jnp.float32)
    collected = []
    for layer_index in reversed(range(layer_count)):
        weights = tuple(w[layer_index] for w in full)
        gradient, layer_grads = layer_backward(
            gradient, records[layer_index], weights, positions, places, layer_index
        )
        collected.insert(0, layer_grads)
    pieces, sizes = [], []
    for layer_grads in collected:
        for grad in layer_grads:
            if grad.ndim == 1:
                half = jnp.pad(grad.astype(jnp.bfloat16).reshape(2, -1), ((0, 0), (0, 2048 - grad.shape[0] // 2)))
                piece = half.reshape(2, 1, 16, 128)
            else:
                piece = tiled(grad)
            pieces.append(piece)
            sizes.append(piece.shape[1])
    count = sum(sizes)
    block = -(-count // (2 * devices))
    pieces.append(jnp.zeros((2, 2 * devices * block - count, 16, 128), jnp.bfloat16))
    blob = jnp.concatenate(pieces, axis=1).reshape(2, 2, devices, block * 16, 128)
    total = reduce_all(blob, devices, 1).reshape(-1, 16, 128)
    results, start = [], 0
    for size, weight in zip(sizes, own * layer_count):
        part = total[start : start + size]
        start += size
        if weight.ndim == 2:
            results.append(part.reshape(-1)[: weight.shape[1]].astype(jnp.float32))
        else:
            results.append(untiled(part, weight.shape[1], weight.shape[2]))
    stacked = [jnp.stack(results[k :: len(own)]) for k in range(len(own))]
    return (output, gradient, *stacked)


def solution(mesh):
    in_specs = (
        P("fsdp", "ctx", None),
        P("fsdp", "ctx"),
        P(None, "fsdp"),
        P(None, "fsdp", None),
        P(None, "fsdp", None),
        P(None, "fsdp", None),
        P(None, "fsdp", None),
        P(None, "fsdp"),
        P(None, "fsdp", None),
        P(None, "fsdp", None),
        P(None, "fsdp", None),
        P("fsdp", "ctx", None),
    )
    out_specs = (
        P("fsdp", "ctx", None),
        P("fsdp", "ctx", None),
        P(None, "fsdp"),
        P(None, "fsdp", None),
        P(None, "fsdp", None),
        P(None, "fsdp", None),
        P(None, "fsdp", None),
        P(None, "fsdp"),
        P(None, "fsdp", None),
        P(None, "fsdp", None),
        P(None, "fsdp", None),
    )
    return jax.shard_map(body, mesh=mesh, in_specs=in_specs, out_specs=out_specs, check_vma=False)
```

```python
import functools, itertools
import jax
import jax.numpy as jnp
from jax import lax
from jax.experimental import pallas as pl
from jax.experimental.pallas import tpu as pltpu
from jax.sharding import PartitionSpec as P

CTX, FSDP = "ctx", "fsdp"
MESH = pl.DeviceIdType.MESH
PARTS = 2


def factors(n):
    known = {16: (4, 2, 2), 64: (2, 4, 4, 2)}
    if n in known:
        return known[n]
    out, p = [], 2
    while n > 1:
        while n % p == 0:
            out.append(p)
            n //= p
        p += 1
    return tuple(out) or (1,)


class Grid:
    def __init__(self, n):
        self.n = n
        self.dims = factors(n)
        strides, s = [], 1
        for d in reversed(self.dims):
            strides.insert(0, s)
            s *= d
        self.strides = tuple(strides)
        self.all = list(itertools.product(*[range(d) for d in self.dims]))
        self.ident = {d: i for i, d in enumerate(self.all)}

    def locate(self):
        me = lax.axis_index(CTX)
        self.me = me
        self.at = [lax.rem(me // s, d) for s, d in zip(self.strides, self.dims)]

    def index(self, delta):
        out = 0
        for c, d, n, s in zip(self.at, delta, self.dims, self.strides):
            out = out + (c if isinstance(d, int) and d == 0 else lax.rem(c + d, n)) * s
        return out

    def slot(self, delta):
        return sum(d * s for d, s in zip(delta, self.strides))

    def peer(self, axis, j):
        return self.index(tuple(j if a == axis else 0 for a in range(len(self.dims))))

    def orders(self):
        rest = list(range(1, len(self.dims)))
        return [[0] + rest, [0] + rest[::-1]]


def put(x, d, a):
    return tuple(x if i == a else v for i, v in enumerate(d))


def entry_barrier(g, fsdp):
    sem = pltpu.get_barrier_semaphore()
    count = 0
    f = lax.axis_index(FSDP)
    for a, d in enumerate(g.dims):
        for j in range(1, d):
            pl.semaphore_signal(sem, inc=1, device_id=(g.peer(a, j), f), device_id_type=MESH)
            count += 1
    if fsdp:
        pl.semaphore_signal(sem, inc=1, device_id=(g.me, 1 - f), device_id_type=MESH)
        count += 1
    pl.semaphore_wait(sem, count)


class Gather:
    def __init__(self, g, order, own, slot, send, recv):
        self.g, self.order, self.own, self.slot, self.send, self.recv = g, order, own, slot, send, recv
        self.sent = []

    def copy(self, src, index, axis, step, label, way):
        g = self.g
        i = g.slot(label)
        return pltpu.make_async_remote_copy(
            src_ref=src, dst_ref=self.slot(index), send_sem=self.send.at[way, i], recv_sem=self.recv.at[i],
            device_id=(g.peer(axis, step % g.dims[axis]), lax.axis_index(FSDP)), device_id_type=MESH)

    def start(self, copy, cond):
        self.sent.append((copy, cond))
        if cond is None:
            copy.start()
        else:
            pl.when(cond)(copy.start)

    def spread(self, delta, stage, src):
        g = self.g
        index = g.index(delta)
        for a in self.order[stage:]:
            n, c = g.dims[a], g.at[a]
            if n > 2:
                self.start(self.copy(src, index, a, 1, put(n - 1, delta, a), 0), c < n - 1)
                self.start(self.copy(src, index, a, -1, put(1, delta, a), 1), c > 0)
            else:
                for j in range(1, n):
                    self.start(self.copy(src, index, a, j, put(n - j, delta, a), 0), None)

    def begin(self):
        self.spread((0,) * len(self.g.dims), 0, self.own)

    def labels(self, stage):
        g, a = self.g, self.order[stage]
        n = g.dims[a]
        before = [range(g.dims[i]) if i in self.order[:stage] else range(1) for i in range(len(g.dims))]
        out = []
        if n > 2:
            c = g.at[a]
            near = [sorted((s for s in range(n) if s != k), key=lambda s: abs(s - k)) for k in range(n)]
            steps = []
            for t in range(n - 1):
                v = (near[0][t]) % n
                for k in range(1, n):
                    v = jnp.where(c == k, (near[k][t] - k) % n, v)
                steps.append(v)
        else:
            steps = list(range(1, n))
        for s in steps:
            for d in itertools.product(*before):
                out.append(put(s, d, a))
        return out

    def arrive(self, label, stage):
        g, a = self.g, self.order[stage]
        n, c = g.dims[a], g.at[a]
        index = g.index(label)
        here = self.slot(index)
        pltpu.make_async_remote_copy(
            src_ref=here, dst_ref=here, send_sem=self.send.at[0, 0], recv_sem=self.recv.at[g.slot(label)],
            device_id=(g.peer(a, 1), lax.axis_index(FSDP)), device_id_type=MESH).wait_recv()
        if n > 2:
            k = label[a]
            below = c + k >= n
            up = jnp.logical_and(below, c < n - 1)
            down = jnp.logical_and(jnp.logical_not(below), c > 0)
            self.start(self.copy(here, index, a, 1, put(k - 1, label, a), 0), up)
            self.start(self.copy(here, index, a, -1, put(k + 1, label, a), 1), down)
        self.spread(label, stage + 1, here)

    def end(self):
        for copy, cond in self.sent:
            if cond is None:
                copy.wait_send()
            else:
                pl.when(cond)(copy.wait_send)


def run_gathers(g, gs, stages=None):
    for stage in range(len(g.dims)):
        lists = [q.labels(stage) for q in gs]
        for i in range(max(map(len, lists))):
            for q, l in zip(gs, lists):
                if i < len(l):
                    q.arrive(l[i], stage)


def add_into(out, refs):
    rows = out.shape[0]
    step = max(s for s in range(16, 129, 16) if rows % s == 0)

    def some(i, carry):
        at = pl.ds(pl.multiple_of(i * step, step), step)
        out[at] = sum(r[at].astype(jnp.float32) for r in refs).astype(out.dtype)
        return carry

    lax.fori_loop(0, rows // step, some, 0)


def chosen(table, c):
    v = table[0]
    for k in range(1, len(table)):
        v = jnp.where(c == k, table[k], v)
    return v


class Reduce:
    def __init__(self, g, order, own, acc, land, send, recv):
        self.g, self.order, self.own, self.acc, self.land, self.send, self.recv = g, order, own, acc, land, send, recv
        self.sent = []
        self.stage = 0

    def held(self, delta):
        ref = self.own if self.stage == 0 else self.acc
        return ref(self.g.index(delta))

    def ship(self, src, label, axis, step, way, at_label):
        g = self.g
        copy = pltpu.make_async_remote_copy(
            src_ref=src, dst_ref=self.land.at[way, g.slot(at_label)], send_sem=self.send.at[g.slot(label)],
            recv_sem=self.recv.at[way, g.slot(at_label)],
            device_id=(g.peer(axis, step), lax.axis_index(FSDP)), device_id_type=MESH)
        copy.start()
        self.sent.append(copy)

    def landed(self, way, label):
        g = self.g
        ref = self.land.at[way, g.slot(label)]
        pltpu.make_async_remote_copy(
            src_ref=ref, dst_ref=ref, send_sem=self.send.at[0], recv_sem=self.recv.at[way, g.slot(label)],
            device_id=(g.peer(self.order[0], 1), lax.axis_index(FSDP)), device_id_type=MESH).wait_recv()
        return ref

    def labels(self, stage):
        gone = self.order[:stage]
        ranges = [range(1) if i in gone else range(n) for i, n in enumerate(self.g.dims)]
        far = lambda d: -sum(1 for i in self.order[stage:] if d[i])
        return sorted(itertools.product(*ranges), key=far)

    def steps(self, stage):
        g, a = self.g, self.order[stage]
        n, c = g.dims[a], g.at[a]
        keep = [d for d in self.labels(stage) if d[a] == 0]
        out = []
        if n == 2:
            if stage == 0:
                out += [functools.partial(self.swap, put(1, d, a), a) for d in keep]
            out += [functools.partial(self.take, d, stage) for d in keep]
        else:
            if stage == 0:
                out.append(self.copy_all)
            far = [sorted((k for k in range(1, n)), key=lambda k: -abs((p + k) % n - p)) for p in range(n)]
            for t in range(n - 1):
                k = chosen([far[p][t] for p in range(n)], c)
                out += [functools.partial(self.pass_on, put(k, d, a), stage) for d in keep]
            out += [functools.partial(self.close, d, stage) for d in keep]
        return out

    def copy_all(self):
        for d in self.g.all:
            i = self.g.index(d)
            add_into(self.acc(i), [self.own(i)])
        self.stage = 1

    def swap(self, d, axis):
        self.ship(self.held(d), d, axis, 1, 0, put(1, d, axis))

    def next_ship(self, d, stage):
        if stage + 1 < len(self.order):
            a = self.order[stage + 1]
            if self.g.dims[a] == 2 and d[a]:
                self.ship(self.acc(self.g.index(d)), d, a, 1, 0, d)

    def take(self, d, stage):
        a = self.order[stage]
        i = self.g.index(d)
        ref = self.own(i) if stage == 0 and self.stage == 0 else self.acc(i)
        add_into(self.acc(i), [ref, self.landed(0, put(1, d, a))])
        self.next_ship(d, stage)

    def pass_on(self, d, stage):
        g, a = self.g, self.order[stage]
        n, c = g.dims[a], g.at[a]
        k = d[a]
        up = c + k < n
        way = jnp.where(up, 0, 1)
        kept = self.acc(g.index(d))

        @pl.when(jnp.where(up, c > 0, c < n - 1))
        def _():
            add_into(kept, [kept, self.landed(way, d)])

        self.ship(kept, d, a, jnp.where(up, 1, n - 1), way, put(jnp.where(up, k - 1, lax.rem(k + 1, n)), d, a))

    def close(self, d, stage):
        g, a = self.g, self.order[stage]
        n, c = g.dims[a], g.at[a]
        kept = self.acc(g.index(d))

        @pl.when(c > 0)
        def _():
            add_into(kept, [kept, self.landed(0, d)])

        @pl.when(c < n - 1)
        def _():
            add_into(kept, [kept, self.landed(1, d)])

        self.next_ship(d, stage)

    def end(self):
        for copy in self.sent:
            copy.wait_send()


def interleave(lists):
    for i in range(max(map(len, lists))):
        for l in lists:
            if i < len(l):
                yield l[i]


def scatter_kernel(g, x_ref, o_ref, acc, land, send, recv):
    g.locate()
    entry_barrier(g, False)
    rows = x_ref.shape[1] // 2
    rs = []
    for p, order in enumerate(g.orders()):
        at = pl.ds(p * rows, rows)
        own = (lambda at: lambda i: x_ref.at[i, at])(at)
        kept = (lambda at: lambda i: acc.at[i, at])(at)
        rs.append(Reduce(g, order[::-1], own, kept, land.at[p], send.at[p], recv.at[p]))
    for stage in range(len(g.dims)):
        for step in interleave([r.steps(stage) for r in rs]):
            step()
        for r in rs:
            r.stage = 1
    o_ref[...] = acc[g.me].astype(jnp.float32)
    for r in rs:
        r.end()


def reduce_scatter_ctx(x, n, cid):
    g = Grid(n)
    _, rows, cols = x.shape
    dma = pltpu.SemaphoreType.DMA
    return pl.pallas_call(
        functools.partial(scatter_kernel, g),
        out_shape=jax.ShapeDtypeStruct((rows, cols), jnp.float32),
        in_specs=[pl.BlockSpec(memory_space=pltpu.VMEM)],
        out_specs=pl.BlockSpec(memory_space=pltpu.VMEM),
        scratch_shapes=[
            pltpu.VMEM((n, rows, cols), x.dtype),
            pltpu.VMEM((2, 2, n, rows // 2, cols), x.dtype),
            dma((2, n)),
            dma((2, 2, n)),
        ],
        compiler_params=pltpu.CompilerParams(collective_id=cid, has_side_effects=True, vmem_limit_bytes=60 << 20),
        name="ctx_reduce",
    )(x)


def reduce_all_kernel(g, x_ref, o_ref, own, kept, land, send, recv, gsend, grecv, psend, precv, lsem):
    g.locate()
    entry_barrier(g, True)
    f = lax.axis_index(FSDP)
    parts = x_ref.shape[1]
    orders = g.orders()
    rs, gs, local = [], [], []
    for p in range(parts):
        order = orders[p % 2]
        at = (lambda p: lambda i: kept.at[p, i])(p)
        rs.append(Reduce(g, order[::-1], at, at, land.at[p], send.at[p], recv.at[p]))
        gs.append(Gather(g, order, o_ref.at[p, g.me], (lambda p: lambda i: o_ref.at[p, i])(p), gsend.at[p], grecv.at[p]))
        c = pltpu.make_async_copy(x_ref.at[f, p], own.at[p], lsem.at[p])
        c.start()
        local.append(c)
    turns = [sorted(g.all, key=lambda d, a=r.order[0], r=r: (d[a] == 0, -sum(1 for v in d if v))) for r in rs]
    pairs = {}
    for i in range(g.n):
        for p in range(parts):
            d = turns[p][i]
            k = g.index(d)
            c = pltpu.make_async_remote_copy(
                src_ref=x_ref.at[1 - f, p, k], dst_ref=kept.at[p, k], send_sem=psend.at[p, g.slot(d)],
                recv_sem=precv.at[p, g.slot(d)], device_id=(g.me, 1 - f), device_id_type=MESH)
            c.start()
            pairs[p, d] = c
    for c in local:
        c.wait()
    first = [r.steps(0) for r in rs]
    for i in range(g.n):
        for p, r in enumerate(rs):
            d = turns[p][i]
            k = g.index(d)
            pairs[p, d].wait_recv()
            add_into(kept.at[p, k], [kept.at[p, k], own.at[p, k]])
            a = r.order[0]
            if g.dims[a] == 2 and d[a]:
                r.swap(d, a)
    for r in rs:
        r.stage = 1
    for stage in range(len(g.dims)):
        lists = []
        for r, steps in zip(rs, first):
            if stage == 0:
                lists.append([s for s in steps if getattr(s, "func", s).__name__ in ("take", "pass_on", "close")])
            else:
                lists.append(r.steps(stage))
        for step in interleave(lists):
            step()
    for p, q in enumerate(gs):
        add_into(o_ref.at[p, g.me], [kept.at[p, g.me]])
        q.begin()
    run_gathers(g, gs)
    for c in pairs.values():
        c.wait_send()
    for r in rs:
        r.end()
    for q in gs:
        q.end()


def reduce_all(x, n, cid):
    g = Grid(n)
    _, parts, _, rows, cols = x.shape
    blk = (parts, n, rows, cols)
    dma = pltpu.SemaphoreType.DMA
    return pl.pallas_call(
        functools.partial(reduce_all_kernel, g),
        out_shape=jax.ShapeDtypeStruct(blk, x.dtype),
        in_specs=[pl.BlockSpec(memory_space=pl.ANY)],
        out_specs=pl.BlockSpec(memory_space=pltpu.VMEM),
        scratch_shapes=[
            pltpu.VMEM(blk, x.dtype),
            pltpu.VMEM(blk, x.dtype),
            pltpu.VMEM((parts, 2, n, rows, cols), x.dtype),
            dma((parts, n)),
            dma((parts, 2, n)),
            dma((parts, 2, n)),
            dma((parts, n)),
            dma((parts, n)),
            dma((parts, n)),
            dma((parts,)),
        ],
        compiler_params=pltpu.CompilerParams(collective_id=cid, has_side_effects=True, vmem_limit_bytes=64 << 20),
        name="grad_reduce",
    )(x)


def gather_kernel(g, count, spots, *refs):
    k = 2 if count else 1
    xs, ws = refs[:k], picked(refs[k : k + count], spots)
    refs = refs[k + count :]
    os, fulls = refs[:k], refs[k : k + len(spots)]
    refs = refs[k + len(spots) :]
    send, recv, local = refs[:3]
    g.locate()
    entry_barrier(g, bool(count))
    rows = xs[0].shape[0] // 2
    gs = []
    for p, order in enumerate(g.orders()):
        at = pl.ds(p * rows, rows)
        slot = (lambda at: lambda i: os[0].at[i, at])(at)
        gs.append(Gather(g, order, xs[0].at[at], slot, send.at[p], recv.at[p]))
    if count:
        gs.append(Gather(g, g.orders()[0], xs[1], lambda i: os[1].at[i], send.at[2], recv.at[2]))
    for q in gs:
        q.begin()
    mine = [pltpu.make_async_copy(x, o.at[g.me], local.at[i]) for i, (x, o) in enumerate(zip(xs, os))]
    for c in mine:
        c.start()
    swap = Swap(ws, fulls, *refs[3:]) if count else None
    if count:
        swap.begin()
    run_gathers(g, gs)
    for c in mine:
        c.wait()
    if count:
        swap.end()
    for q in gs:
        q.end()


class Swap:
    def __init__(self, srcs, dsts, send, recv, load, store, *stages):
        c, f = lax.axis_index(CTX), lax.axis_index(FSDP)
        self.remote, self.loads, self.stores = [], [], []
        for i, (s, d, v) in enumerate(zip(srcs, dsts, stages)):
            self.remote.append(
                pltpu.make_async_remote_copy(
                    src_ref=s, dst_ref=d.at[f], send_sem=send.at[i], recv_sem=recv.at[i], device_id=(c, 1 - f),
                    device_id_type=MESH))
            self.loads.append(pltpu.make_async_copy(s, v, load.at[i]))
            self.stores.append(pltpu.make_async_copy(v, d.at[f], store.at[i]))

    def begin(self):
        for c in self.remote + self.loads:
            c.start()
        for a, b in zip(self.loads, self.stores):
            a.wait()
            b.start()

    def end(self):
        for c in self.stores + self.remote:
            c.wait()

    @staticmethod
    def scratch(picks):
        return [pltpu.SemaphoreType.DMA((len(picks),))] * 4 + [pltpu.VMEM(shape_of(a, l), a.dtype) for a, l in picks]


def distinct(picks):
    arrays, places = [], []
    for a, l in picks:
        spot = next((i for i, b in enumerate(arrays) if b is a), None)
        if spot is None:
            spot = len(arrays)
            arrays.append(a)
        places.append((spot, l))
    return arrays, places


def picked(refs, places):
    return [refs[i] if l is None else refs[i].at[l] for i, l in places]


def shape_of(a, l):
    return a.shape if l is None else a.shape[1:]


def all_gather_ctx(x, n, cid, places=None, weights=()):
    g = Grid(n)
    arrays, spots = distinct(weights)
    count = len(arrays)
    xs = [x] if places is None else [x, places]
    dma = pltpu.SemaphoreType.DMA
    vmem, anywhere = pl.BlockSpec(memory_space=pltpu.VMEM), pl.BlockSpec(memory_space=pl.ANY)
    parts = len(xs) + 1
    return pl.pallas_call(
        functools.partial(gather_kernel, g, count, spots),
        out_shape=[jax.ShapeDtypeStruct((n, *v.shape), v.dtype) for v in xs]
        + [jax.ShapeDtypeStruct((2, *shape_of(a, l)), a.dtype) for a, l in weights],
        in_specs=[vmem] * len(xs) + [anywhere] * count,
        out_specs=[vmem] * len(xs) + [anywhere] * len(weights),
        scratch_shapes=[dma((parts, 2, n)), dma((parts, n)), dma((2,))] + (Swap.scratch(weights) if count else []),
        compiler_params=pltpu.CompilerParams(collective_id=cid, has_side_effects=True, vmem_limit_bytes=60 << 20),
        name="ctx_gather",
    )(*xs, *arrays)


def exchange_kernel(count, spots, *refs):
    srcs, dsts = picked(refs[:count], spots), refs[count : count + len(spots)]
    c, f = lax.axis_index(CTX), lax.axis_index(FSDP)
    sem = pltpu.get_barrier_semaphore()
    pl.semaphore_signal(sem, inc=1, device_id=(c, 1 - f), device_id_type=MESH)
    pl.semaphore_wait(sem, 1)
    swap = Swap(srcs, dsts, *refs[count + len(spots) :])
    swap.begin()
    swap.end()


def exchange(picks, cid):
    arrays, spots = distinct(picks)
    anywhere = pl.BlockSpec(memory_space=pl.ANY)
    return pl.pallas_call(
        functools.partial(exchange_kernel, len(arrays), spots),
        out_shape=[jax.ShapeDtypeStruct((2, *shape_of(a, l)), a.dtype) for a, l in picks],
        in_specs=[anywhere] * len(arrays),
        out_specs=[anywhere] * len(picks),
        scratch_shapes=Swap.scratch(picks),
        compiler_params=pltpu.CompilerParams(collective_id=cid, has_side_effects=True),
        name="exchange",
    )(*arrays)


HEADS = 9
KV_HEADS = 3
HEAD = 64
GROUP = HEADS // KV_HEADS
EPS = 1e-05
ROPE_BASE = 100000.0
F32, BF16 = jnp.float32, jnp.bfloat16
CHUNK = 256
ROOM = 62 << 20


def nn(a, b):
    return lax.dot_general(a, b, (((1,), (0,)), ((), ())), preferred_element_type=F32)


def nt(a, b):
    return lax.dot_general(a, b, (((1,), (1,)), ((), ())), preferred_element_type=F32)


def tn(a, b):
    return lax.dot_general(a, b, (((0,), (0,)), ((), ())), preferred_element_type=F32)


def rms(v, gain):
    return v * lax.rsqrt(jnp.mean(v * v, axis=-1, keepdims=True) + EPS) * gain


def rms_back(v, gain, e):
    r = lax.rsqrt(jnp.mean(v * v, axis=-1, keepdims=True) + EPS)
    eg = e * gain
    dv = r * eg - v * (r * r * r) * jnp.mean(eg * v, axis=-1, keepdims=True)
    return dv, jnp.sum(e * v * r, axis=0, keepdims=True)


def rope(t, cos, sin):
    width = t.shape[1]
    out = []
    for lo in range(0, width, 128):
        w = min(128, width - lo)
        u = t[:, lo : lo + w]
        if w == 128:
            lane = lax.broadcasted_iota(jnp.int32, u.shape, 1) % HEAD
            other = jnp.where(lane < HEAD // 2, pltpu.roll(u, 128 - HEAD // 2, 1), pltpu.roll(u, HEAD // 2, 1))
        else:
            other = jnp.concatenate([u[:, HEAD // 2 :], u[:, : HEAD // 2]], axis=1)
        out.append((lo, w, u * cos[:, :w] + other * sin[:, :w]))
    return out


def call(kernel, outs, args, name, scratch=(), prefetch=0, blob=None):
    vmem = pl.BlockSpec(memory_space=pltpu.VMEM)
    smem = pl.BlockSpec(memory_space=pltpu.SMEM)
    anywhere = pl.BlockSpec(memory_space=pl.ANY)
    if blob is not None:
        new = isinstance(blob, tuple)
        return pl.pallas_call(
            kernel,
            out_shape=[jax.ShapeDtypeStruct(s, t) for s, t in outs] + [jax.ShapeDtypeStruct(blob if new else blob.shape, BF16)],
            in_specs=[vmem] * len(args) + ([] if new else [anywhere]),
            out_specs=[vmem] * len(outs) + [anywhere],
            scratch_shapes=list(scratch),
            input_output_aliases={} if new else {len(args): len(outs)},
            compiler_params=pltpu.CompilerParams(vmem_limit_bytes=ROOM),
            name=name,
        )(*args, *([] if new else [blob]))
    return pl.pallas_call(
        kernel,
        out_shape=[jax.ShapeDtypeStruct(s, t) for s, t in outs],
        in_specs=[smem] * prefetch + [vmem] * (len(args) - prefetch),
        out_specs=[vmem] * len(outs),
        scratch_shapes=list(scratch),
        compiler_params=pltpu.CompilerParams(vmem_limit_bytes=ROOM),
        name=name,
    )(*args)


def pre_kernel(x_ref, gain_ref, wq_ref, wk_ref, wv_ref, cos_ref, sin_ref, a_ref, q_ref, kv_ref):
    a = rms(x_ref[...].astype(F32), gain_ref[...]).astype(BF16)
    a_ref[...] = a
    cos, sin = cos_ref[...], sin_ref[...]
    for lo, w, piece in rope(nn(a, wq_ref[...]), cos, sin):
        q_ref[:, lo : lo + w] = piece.astype(BF16)
    keys = jnp.concatenate([piece for _, _, piece in rope(nn(a, wk_ref[...]), cos, sin)], axis=1)
    kv_ref[...] = jnp.concatenate([keys, nn(a, wv_ref[...])], axis=1).astype(BF16)


def pre(x, gain, wq, wk, wv, cos, sin):
    m, d = x.shape
    e = wk.shape[1]
    return call(pre_kernel, [((m, d), BF16), ((m, d), BF16), ((m, 2 * e), BF16)], (x, gain, wq, wk, wv, cos, sin), "pre")


def half_of(u, src, dst):
    if src != dst:
        u = pltpu.roll(u, HEAD, 1)
    lane = lax.broadcasted_iota(jnp.int32, u.shape, 1)
    return jnp.where((lane < HEAD) if dst == 0 else (lane >= HEAD), u, 0.0)


def head_chunk(ref, s, h):
    lo = (h // 2) * 128
    width = ref.shape[-1]
    if lo + 128 <= width:
        return ref[s, :, lo : lo + 128].astype(F32)
    u = ref[s, :, lo:width].astype(F32)
    return jnp.concatenate([u, jnp.zeros_like(u)], axis=1)


def pack_heads(ref, s, dst, g, half, scale):
    rows = ref.shape[1] // 2
    for i in range(GROUP):
        h = g * GROUP + i
        u = half_of(head_chunk(ref, s, h) * scale, h % 2, half).astype(BF16)
        for part in range(2):
            dst[g * 2 + part, i * rows : (i + 1) * rows, :] = u[part * rows : (part + 1) * rows]


def sort_rows(block_ref, s, src, dst, n, rows):
    def one(j, carry):
        b = block_ref[j, s, 0] // rows
        dst[pl.ds(pl.multiple_of(b * rows, rows), rows), :] = src[j, s, 0:rows, :]
        dst[pl.ds(pl.multiple_of((2 * n - 1 - b) * rows, rows), rows), :] = src[j, s, rows : 2 * rows, :]
        return carry

    lax.fori_loop(0, n, one, 0)


def visible(c, block, rows, shape):
    key = lax.broadcasted_iota(jnp.int32, shape, 0) + c * CHUNK
    query = lax.broadcasted_iota(jnp.int32, shape, 1) % rows + block * rows
    return key <= query


def key_lanes(g):
    return (g // 2) * 128, g % 2


def value_lanes(g):
    return ((KV_HEADS + g) // 2) * 128, (KV_HEADS + g) % 2


def attend_kernel(n, block_ref, mine_ref, q_ref, kv_ref, o_ref, lse_ref, sorted_ref, qp_ref, st_ref):
    rows = q_ref.shape[1] // 2
    wide = GROUP * rows

    def sequence(s, carry):
        sort_rows(block_ref, s, kv_ref, sorted_ref, n, rows)
        for g in range(KV_HEADS):
            pack_heads(q_ref, s, qp_ref, g, key_lanes(g)[1], HEAD**-0.5)
        low = mine_ref[s, 0] // rows
        for g in range(KV_HEADS):
            klo, _ = key_lanes(g)
            vlo, vhalf = value_lanes(g)
            for part in range(2):
                block = low if part == 0 else 2 * n - 1 - low
                last = block * rows // CHUNK
                qp = qp_ref[g * 2 + part]

                def score(c, top, masked):
                    at = pl.ds(pl.multiple_of(c * CHUNK, CHUNK), CHUNK)
                    st = nt(sorted_ref[at, klo : klo + 128], qp)
                    if masked:
                        st = jnp.where(visible(c, block, rows, st.shape), st, -1e30)
                    st_ref[at, :] = st
                    return jnp.maximum(top, jnp.max(st.reshape(CHUNK // 8, 8, wide), axis=0))

                top = lax.fori_loop(0, last, lambda c, t: score(c, t, False), jnp.full((8, wide), -1e30, F32))
                top = jnp.max(score(last, top, True), axis=0, keepdims=True)

                def mix(c, state):
                    total, acc = state
                    at = pl.ds(pl.multiple_of(c * CHUNK, CHUNK), CHUNK)
                    p = jnp.exp(st_ref[at, :] - top)
                    total = total + jnp.sum(p.reshape(CHUNK // 8, 8, wide), axis=0)
                    return total, acc + tn(sorted_ref[at, vlo : vlo + 128], p.astype(BF16))

                total, acc = lax.fori_loop(0, last + 1, mix, (jnp.zeros((8, wide), F32), jnp.zeros((128, wide), F32)))
                total = jnp.sum(total, axis=0, keepdims=True)
                lse_ref[s, g * 2 + part] = top + jnp.log(total)
                out = (acc[vhalf * HEAD : (vhalf + 1) * HEAD] / total).T
                for i in range(GROUP):
                    h = g * GROUP + i
                    o_ref[s, part * rows : (part + 1) * rows, h * HEAD : (h + 1) * HEAD] = out[i * rows : (i + 1) * rows]
        return carry

    lax.fori_loop(0, q_ref.shape[0], sequence, 0)


def attend(blocks, mine, q, kv):
    seqs, r, d = q.shape
    n = kv.shape[0]
    wide = GROUP * r // 2
    scratch = [
        pltpu.VMEM((n * r, kv.shape[-1]), BF16),
        pltpu.VMEM((2 * KV_HEADS, wide, 128), BF16),
        pltpu.VMEM((n * r, wide), F32),
    ]
    outs = [((seqs, r, d), F32), ((seqs, 2 * KV_HEADS, 1, wide), F32)]
    return call(functools.partial(attend_kernel, n), outs, (blocks, mine, q, kv), "attend", scratch, 2)


def attend_back_kernel(
    n, block_ref, mine_ref, q_ref, kv_ref, do_ref, o_ref, lse_ref, dq_ref, dkv_ref, sorted_ref, qp_ref, dop_ref, acc_ref, delta_ref
):
    rows = q_ref.shape[1] // 2
    wide = GROUP * rows

    def sequence(s, carry):
        sort_rows(block_ref, s, kv_ref, sorted_ref, n, rows)
        for g in range(KV_HEADS):
            pack_heads(q_ref, s, qp_ref, g, key_lanes(g)[1], HEAD**-0.5)
            pack_heads(do_ref, s, dop_ref, g, value_lanes(g)[1], 1.0)
        acc_ref[...] = jnp.zeros_like(acc_ref)
        low = mine_ref[s, 0] // rows
        for g in range(KV_HEADS):
            klo, khalf = key_lanes(g)
            vlo, vhalf = value_lanes(g)
            pieces = []
            for part in range(2):
                block = low if part == 0 else 2 * n - 1 - low
                last = block * rows // CHUNK
                qp, dop = qp_ref[g * 2 + part], dop_ref[g * 2 + part]
                lse = lse_ref[s, g * 2 + part]
                sums = []
                for i in range(GROUP):
                    h = g * GROUP + i
                    lanes = slice(h * HEAD, (h + 1) * HEAD)
                    at = slice(part * rows, (part + 1) * rows)
                    both = do_ref[s, at, lanes].astype(F32) * o_ref[s, at, lanes]
                    sums.append(jnp.sum(both, axis=1, keepdims=True))
                delta_ref[...] = jnp.concatenate(sums, axis=0) + jnp.zeros((wide, 128), F32)
                delta = delta_ref[...].T[0:1]

                def step(c, dq, masked):
                    at = pl.ds(pl.multiple_of(c * CHUNK, CHUNK), CHUNK)
                    keys = sorted_ref[at, klo : klo + 128]
                    p = jnp.exp(nt(keys, qp) - lse)
                    if masked:
                        p = jnp.where(visible(c, block, rows, p.shape), p, 0.0)
                    dp = nt(sorted_ref[at, vlo : vlo + 128], dop)
                    ds = (p * (dp - delta)).astype(BF16)
                    acc_ref[at, vlo : vlo + 128] += nn(p.astype(BF16), dop)
                    acc_ref[at, klo : klo + 128] += nn(ds, qp)
                    return dq + tn(ds, keys)

                dq = lax.fori_loop(0, last, lambda c, t: step(c, t, False), jnp.zeros((wide, 128), F32))
                dq = step(last, dq, True) * HEAD**-0.5
                for i in range(GROUP):
                    h = g * GROUP + i
                    dq_ref[s, part * rows : (part + 1) * rows, h * HEAD : (h + 1) * HEAD] = dq[
                        i * rows : (i + 1) * rows, khalf * HEAD : (khalf + 1) * HEAD
                    ]

        def one(j, carry):
            b = block_ref[j, s, 0] // rows
            dkv_ref[j, s, 0:rows, :] = acc_ref[pl.ds(pl.multiple_of(b * rows, rows), rows), :].astype(BF16)
            dkv_ref[j, s, rows : 2 * rows, :] = acc_ref[
                pl.ds(pl.multiple_of((2 * n - 1 - b) * rows, rows), rows), :
            ].astype(BF16)
            return carry

        lax.fori_loop(0, n, one, 0)
        return carry

    lax.fori_loop(0, q_ref.shape[0], sequence, 0)


def attend_back(blocks, mine, q, kv, do, o, lse):
    seqs, r, d = q.shape
    n = kv.shape[0]
    wide = GROUP * r // 2
    scratch = [
        pltpu.VMEM((n * r, kv.shape[-1]), BF16),
        pltpu.VMEM((2 * KV_HEADS, wide, 128), BF16),
        pltpu.VMEM((2 * KV_HEADS, wide, 128), BF16),
        pltpu.VMEM((n * r, kv.shape[-1]), F32),
        pltpu.VMEM((wide, 128), F32),
    ]
    outs = [((seqs, r, d), F32), (kv.shape, BF16)]
    args = (blocks, mine, q, kv, do, o, lse)
    return call(functools.partial(attend_back_kernel, n), outs, args, "attend_back", scratch, 2)


def post_kernel(o_ref, x_ref, wo_ref, gain_ref, wg_ref, wu_ref, wd_ref, h_ref, b_ref, gate_ref, up_ref, y_ref):
    h = x_ref[...].astype(F32) + nn(o_ref[...].astype(BF16), wo_ref[...])
    h_ref[...] = h
    y_ref[...] = h
    b_ref[...] = rms(h, gain_ref[...]).astype(BF16)

    def some(i, carry):
        at = pl.ds(pl.multiple_of(i * CHUNK, CHUNK), CHUNK)
        b = b_ref[...]
        gate, up = nn(b, wg_ref[:, at]), nn(b, wu_ref[:, at])
        gate_ref[:, at], up_ref[:, at] = gate, up
        m = (gate * jax.nn.sigmoid(gate) * up).astype(BF16)
        y_ref[...] += nn(m, wd_ref[at, :])
        return carry

    lax.fori_loop(0, wg_ref.shape[1] // CHUNK, some, 0)


def post(o, x, wo, gain, wg, wu, wd):
    m, d = x.shape
    ff = wg.shape[1]
    outs = [((m, d), F32), ((m, d), BF16), ((m, ff), F32), ((m, ff), F32), ((m, d), F32)]
    return call(post_kernel, outs, (o, x, wo, gain, wg, wu, wd), "post")


def put_tiles(blob, base, value, count):
    rows = value.shape[0] // 2
    if value.shape[1] < count * 128:
        value = jnp.concatenate([value, jnp.zeros((2 * rows, count * 128 - value.shape[1]), value.dtype)], axis=1)
    for f in range(2):
        for j in range(count):
            piece = value[f * rows : (f + 1) * rows, j * 128 : (j + 1) * 128]
            blob[f, pl.ds(base + j * (rows // 16), rows // 16)] = piece.reshape(rows // 16, 16, 128)


def put_norm(blob, at, dg):
    half = dg.shape[1] // 2
    for f in range(2):
        v = dg[:, f * half : (f + 1) * half]
        v = jnp.concatenate([v, jnp.zeros((1, 384 - half), F32)], axis=1)
        rows = jnp.concatenate([v[:, 0:128], v[:, 128:256], v[:, 256:384], jnp.zeros((13, 128), F32)], axis=0)
        blob[f, at] = rows.astype(BF16)


def wide_of(cols):
    return -(-cols // 128)


def ffn_back_kernel(base, new, *refs):
    dy_ref, h_ref, b_ref, gate_ref, up_ref, o_ref, gain_ref, wo_ref, wg_ref, wu_ref, wd_ref = refs[:11]
    dh_ref, do_ref, out_ref, blob_ref, dyb_ref, db_ref, bt_ref, sem = refs[11 if new else 12 :]
    m, d = h_ref.shape
    ff = wg_ref.shape[1]
    half = d // 2 // 16
    gate_at, up_at = 0, (ff // 128) * half
    down_at = 2 * up_at
    down_rows = ff // 2 // 16
    out_at = down_at + wide_of(d) * down_rows
    norm_at = out_at + wide_of(d) * half
    dyb_ref[...] = dy_ref[...].astype(BF16)
    db_ref[...] = jnp.zeros_like(db_ref)
    bt_ref[...] = b_ref[...].T

    def some(i, carry):
        at = pl.ds(pl.multiple_of(i * CHUNK, CHUNK), CHUNK)
        dyb = dyb_ref[...]
        dm = nt(dyb, wd_ref[at, :])
        gate, up = gate_ref[:, at], up_ref[:, at]
        sig = jax.nn.sigmoid(gate)
        silu = gate * sig
        mid = (silu * up).astype(BF16)
        dgate = (dm * up * sig * (1.0 + gate * (1.0 - sig))).astype(BF16)
        dup = (dm * silu).astype(BF16)
        db_ref[...] += nt(dgate, wg_ref[:, at]) + nt(dup, wu_ref[:, at])
        bt = bt_ref[...]
        put_tiles(blob_ref, gate_at + i * (CHUNK // 128) * half, nn(bt, dgate).astype(BF16), CHUNK // 128)
        put_tiles(blob_ref, up_at + i * (CHUNK // 128) * half, nn(bt, dup).astype(BF16), CHUNK // 128)
        gd = tn(mid, dyb).astype(BF16)
        gd = jnp.concatenate([gd, jnp.zeros((CHUNK, wide_of(d) * 128 - d), BF16)], axis=1)
        per = ff // 2 // CHUNK
        f = i // per
        for j in range(wide_of(d)):
            start = down_at + j * down_rows + (i - f * per) * (CHUNK // 16)
            blob_ref[f, pl.ds(start, CHUNK // 16)] = gd[:, j * 128 : (j + 1) * 128].reshape(CHUNK // 16, 16, 128)
        return carry

    lax.fori_loop(0, ff // CHUNK, some, 0)
    first = pltpu.make_async_copy(blob_ref.at[:, pl.ds(0, out_at)], out_ref.at[:, pl.ds(base, out_at)], sem.at[0])
    first.start()
    dv, dg = rms_back(h_ref[...], gain_ref[...], db_ref[...])
    dh = dy_ref[...].astype(F32) + dv
    dh_ref[...] = dh
    dhb = dh.astype(BF16)
    do_ref[...] = nt(dhb, wo_ref[...]).astype(BF16)
    put_tiles(blob_ref, out_at, tn(o_ref[...].astype(BF16), dhb).astype(BF16), wide_of(d))
    put_norm(blob_ref, norm_at, dg)
    rest = norm_at + 1 - out_at
    second = pltpu.make_async_copy(
        blob_ref.at[:, pl.ds(out_at, rest)], out_ref.at[:, pl.ds(base + out_at, rest)], sem.at[1]
    )
    second.start()
    first.wait()
    second.wait()


def ffn_tiles(d, ff):
    return 2 * (ff // 128) * (d // 32) + wide_of(d) * (ff // 32) + wide_of(d) * (d // 32) + 1


def pre_tiles(d, e):
    return wide_of(d) * (d // 32) + wide_of(2 * e) * (d // 32) + 1


def ffn_back(blob, base, dy, h, b, gate, up, o, gain, wo, wg, wu, wd):
    m, d = h.shape
    ff = wg.shape[1]
    scratch = [
        pltpu.VMEM((2, ffn_tiles(d, ff), 16, 128), BF16),
        pltpu.VMEM((m, d), BF16),
        pltpu.VMEM((m, d), F32),
        pltpu.VMEM((d, m), BF16),
        pltpu.SemaphoreType.DMA((2,)),
    ]
    kernel = functools.partial(ffn_back_kernel, base, isinstance(blob, tuple))
    args = (dy, h, b, gate, up, o, gain, wo, wg, wu, wd)
    return call(kernel, [((m, d), F32), ((m, d), BF16)], args, "ffn_back", scratch, blob=blob)


def pre_back_kernel(base, *refs):
    dq_ref, dkv_ref, a_ref, x_ref, dh_ref, gain_ref, wq_ref, wk_ref, wv_ref, cos_ref, sin_ref = refs[:11]
    dx_ref, out_ref, blob_ref, dqp_ref, sem = refs[12:]
    d = x_ref.shape[1]
    e = wk_ref.shape[1]
    half = d // 2 // 16
    cos, sin = cos_ref[...], -sin_ref[...]
    for lo, w, piece in rope(dq_ref[...], cos, sin):
        dqp_ref[:, lo : lo + w] = piece.astype(BF16)
    dqp = dqp_ref[...]
    dkv = dkv_ref[...]
    dkp = jnp.concatenate([piece for _, _, piece in rope(dkv[:, :e], cos, sin)], axis=1).astype(BF16)
    dvr = dkv[:, e:].astype(BF16)
    da = nt(dqp, wq_ref[...]) + nt(dkp, wk_ref[...]) + nt(dvr, wv_ref[...])
    dv, dg = rms_back(x_ref[...].astype(F32), gain_ref[...], da)
    kv_at = wide_of(d) * half
    norm_at = kv_at + wide_of(2 * e) * half
    put_norm(blob_ref, norm_at, dg)
    left = blob_ref.shape[1] - norm_at - 1
    if left:
        blob_ref[:, pl.ds(norm_at + 1, left)] = jnp.zeros((2, left, 16, 128), BF16)
    at = a_ref[...].T
    put_tiles(blob_ref, 0, nn(at, dqp).astype(BF16), wide_of(d))
    put_tiles(blob_ref, kv_at, jnp.concatenate([nn(at, dkp), nn(at, dvr)], axis=1).astype(BF16), wide_of(2 * e))
    done = pltpu.make_async_copy(blob_ref, out_ref.at[:, pl.ds(base, blob_ref.shape[1])], sem)
    done.start()
    dx_ref[...] = dh_ref[...] + dv
    done.wait()


def pre_back(blob, base, tiles, dq, dkv, a, x, dh, gain, wq, wk, wv, cos, sin):
    m, d = x.shape
    scratch = [pltpu.VMEM((2, tiles, 16, 128), BF16), pltpu.VMEM((m, d), BF16), pltpu.SemaphoreType.DMA(())]
    args = (dq, dkv, a, x, dh, gain, wq, wk, wv, cos, sin)
    return call(functools.partial(pre_back_kernel, base), [((m, d), F32)], args, "pre_back", scratch, blob=blob)


def unpack_kernel(places, blob, *outs):
    g_attn, gq, gk, gv, go, g_ffn, gg, gu, gd = outs
    half, d, e, ff = gq.shape[1], gq.shape[2], gk.shape[2], gg.shape[2]
    t = half // 16

    def take(base, at, rows, cols, out, l, skip=0):
        for lo in range(0, cols, 128):
            w = min(128, cols - lo)
            j = (skip + lo) // 128
            if (skip + lo) % 128 == 0:
                u = blob[pl.ds(base + at + j * (rows // 16), rows // 16)].reshape(rows, 128)[:, :w]
            else:
                u = blob[pl.ds(base + at + j * (rows // 16), rows // 16)].reshape(rows, 128)[:, 64:]
                if w > 64:
                    v = blob[pl.ds(base + at + (j + 1) * (rows // 16), rows // 16)].reshape(rows, 128)[:, : w - 64]
                    u = jnp.concatenate([u.astype(F32), v.astype(F32)], axis=1)
            out[l, :, lo : lo + w] = u.astype(F32)

    def norm(base, at, out, l):
        u = blob[base + at].astype(F32)
        row = jnp.concatenate([u[0:1], u[1:2], u[2:3]], axis=1)
        out[l : l + 1, :] = row[:, :half]

    for l, (ffn, att) in enumerate(places):
        up_at = (ff // 128) * t
        down_at = 2 * up_at
        out_at = down_at + wide_of(d) * (gd.shape[1] // 16)
        take(ffn, 0, half, ff, gg, l)
        take(ffn, up_at, half, ff, gu, l)
        take(ffn, down_at, gd.shape[1], d, gd, l)
        take(ffn, out_at, half, d, go, l)
        norm(ffn, out_at + wide_of(d) * t, g_ffn, l)
        take(att, 0, half, d, gq, l)
        kv_at = wide_of(d) * t
        take(att, kv_at, half, e, gk, l)
        take(att, kv_at, half, e, gv, l, e)
        norm(att, kv_at + wide_of(2 * e) * t, g_attn, l)


def unpack(blob, places, shapes):
    return call(functools.partial(unpack_kernel, places), [(s, F32) for s in shapes], (blob,), "unpack")


def body(tokens, positions, norm_attn, w_query, w_key, w_value, w_out, norm_ffn, w_gate, w_up, w_down, cotangent):
    layers = norm_attn.shape[0]
    n = lax.axis_size(CTX)
    seqs, r, d = tokens.shape
    m = seqs * r
    e, ff = w_key.shape[2], w_gate.shape[2]
    own = (w_query, w_key, w_value, w_out, w_gate, w_up, w_down)
    shards = [(w, l) for l in range(layers) for w in own]
    full = exchange([(norm_attn, None), (norm_ffn, None), *shards[:3]], 0)
    gains = [jnp.swapaxes(v, 0, 1).reshape(layers, 1, d).astype(F32) for v in full[:2]]
    full = full[2:]
    frequency = jnp.exp(jnp.arange(HEAD // 2, dtype=F32) * (-jnp.log(ROPE_BASE) / (HEAD // 2)))
    angles = positions.reshape(m, 1).astype(F32) * frequency
    cos, sin = jnp.cos(angles), jnp.sin(angles)
    cos = jnp.concatenate([cos] * 4, axis=1)
    sin = jnp.concatenate([-sin, sin] * 2, axis=1)
    x = tokens.reshape(m, d)
    kept = []
    weights = []

    def joined(w):
        return w.reshape(2 * w.shape[1], w.shape[2])

    for l in range(layers):
        wq, wk, wv = (joined(w) for w in full[l * len(own) : l * len(own) + 3])
        a, q, kv = pre(x, gains[0][l], wq, wk, wv, cos, sin)
        q = q.reshape(seqs, r, d)
        if l == 0:
            kv, places, *rest = all_gather_ctx(kv, n, 1, positions, shards[3:])
            full = [*full, *rest]
        else:
            (kv,) = all_gather_ctx(kv, n, 1 + l)
        wo, wg, wu, wd = (joined(w) for w in full[l * len(own) + 3 : (l + 1) * len(own)])
        weights.append((wq, wk, wv, wo, wg, wu, wd))
        kv = kv.reshape(n, seqs, r, 2 * e)
        o, lse = attend(places, positions, q, kv)
        h, b, gate, up, y = post(o.reshape(m, d), x, wo, gains[1][l], wg, wu, wd)
        kept.append((x, a, q, kv, o, lse, h, b, gate, up))
        x = y
    output = x.reshape(seqs, r, d).astype(BF16)
    dy = cotangent.reshape(m, d)
    one, two = ffn_tiles(d, ff), pre_tiles(d, e)
    unit = 2 * PARTS * n
    whole = -(-layers * (one + two) // unit) * unit
    blob = (2, whole, 16, 128)
    spots = []
    for l in reversed(range(layers)):
        wq, wk, wv, wo, wg, wu, wd = weights[l]
        x, a, q, kv, o, lse, h, b, gate, up = kept[l]
        start = (layers - 1 - l) * (one + two)
        spots.insert(0, (start, start + one))
        dh, do, blob = ffn_back(blob, start, dy, h, b, gate, up, o.reshape(m, d), gains[1][l], wo, wg, wu, wd)
        dq, dkv = attend_back(places, positions, q, kv, do.reshape(seqs, r, d), o, lse)
        dkv = reduce_scatter_ctx(dkv.reshape(n, m, 2 * e), n, 1 + layers + l)
        tiles = two if l else whole - start - one
        dy, blob = pre_back(
            blob, start + one, tiles, dq.reshape(m, d), dkv, a, x, dh, gains[0][l], wq, wk, wv, cos, sin
        )
    total = reduce_all(blob.reshape(2, PARTS, n, -1, 128), n, 1 + 2 * layers)
    shapes = [norm_attn.shape, *[w.shape for w in own[:4]], norm_ffn.shape, *[w.shape for w in own[4:]]]
    grads = unpack(total.reshape(whole, 16, 128), spots, shapes)
    return (output, dy.reshape(seqs, r, d), *grads)


def solution(mesh):
    in_specs = (
        P("fsdp", "ctx", None),
        P("fsdp", "ctx"),
        P(None, "fsdp"),
        P(None, "fsdp", None),
        P(None, "fsdp", None),
        P(None, "fsdp", None),
        P(None, "fsdp", None),
        P(None, "fsdp"),
        P(None, "fsdp", None),
        P(None, "fsdp", None),
        P(None, "fsdp", None),
        P("fsdp", "ctx", None),
    )
    out_specs = (
        P("fsdp", "ctx", None),
        P("fsdp", "ctx", None),
        P(None, "fsdp"),
        P(None, "fsdp", None),
        P(None, "fsdp", None),
        P(None, "fsdp", None),
        P(None, "fsdp", None),
        P(None, "fsdp"),
        P(None, "fsdp", None),
        P(None, "fsdp", None),
        P(None, "fsdp", None),
    )
    return jax.shard_map(body, mesh=mesh, in_specs=in_specs, out_specs=out_specs, check_vma=False)
```

```python
import functools
import itertools
import math

import jax
import jax.numpy as jnp
from jax import lax
from jax.experimental import pallas as pl
from jax.experimental.pallas import tpu as pltpu
from jax.sharding import PartitionSpec as P

CTX, FSDP = "ctx", "fsdp"
MESH = pl.DeviceIdType.MESH
SHARES = ((0, 6), (1, 6), (2, 2), (3, 2))


def factors(n):
    known = {16: (4, 2, 2), 64: (2, 4, 4, 2)}
    if n in known:
        return known[n]
    out, p = [], 2
    while n > 1:
        while n % p == 0:
            out.append(p)
            n //= p
        p += 1
    return tuple(out) or (1,)


class Grid:
    def __init__(self, n):
        self.n = n
        self.dims = factors(n)
        strides, s = [], 1
        for d in reversed(self.dims):
            strides.insert(0, s)
            s *= d
        self.strides = tuple(strides)
        self.all = list(itertools.product(*[range(d) for d in self.dims]))
        self.ident = {d: i for i, d in enumerate(self.all)}

    def locate(self):
        me = lax.axis_index(CTX)
        self.me = me
        self.at = [lax.rem(me // s, d) for s, d in zip(self.strides, self.dims)]

    def index(self, delta):
        out = 0
        for c, d, n, s in zip(self.at, delta, self.dims, self.strides):
            out = out + (c if isinstance(d, int) and d == 0 else lax.rem(c + d, n)) * s
        return out

    def slot(self, delta):
        return sum(d * s for d, s in zip(delta, self.strides))

    def peer(self, axis, j):
        return self.index(tuple(j if a == axis else 0 for a in range(len(self.dims))))

    def orders(self):
        rest = list(range(1, len(self.dims)))
        return [[0] + rest, [0] + rest[::-1]]


def put(x, d, a):
    return tuple(x if i == a else v for i, v in enumerate(d))


def entry_barrier(g, fsdp):
    sem = pltpu.get_barrier_semaphore()
    count = 0
    f = lax.axis_index(FSDP)
    for a, d in enumerate(g.dims):
        for j in range(1, d):
            pl.semaphore_signal(sem, inc=1, device_id=(g.peer(a, j), f), device_id_type=MESH)
            count += 1
    if fsdp:
        pl.semaphore_signal(sem, inc=1, device_id=(g.me, 1 - f), device_id_type=MESH)
        count += 1
    pl.semaphore_wait(sem, count)


class Gather:
    def __init__(self, g, order, own, slot, send, recv):
        self.g, self.order, self.own, self.slot, self.send, self.recv = g, order, own, slot, send, recv
        self.sent = []

    def copy(self, src, index, axis, step, label, way):
        g = self.g
        i = g.slot(label)
        return pltpu.make_async_remote_copy(
            src_ref=src, dst_ref=self.slot(index), send_sem=self.send.at[way, i], recv_sem=self.recv.at[i],
            device_id=(g.peer(axis, step % g.dims[axis]), lax.axis_index(FSDP)), device_id_type=MESH)

    def start(self, copy, cond):
        self.sent.append((copy, cond))
        if cond is None:
            copy.start()
        else:
            pl.when(cond)(copy.start)

    def spread(self, delta, stage, src):
        g = self.g
        index = g.index(delta)
        for a in self.order[stage:]:
            n, c = g.dims[a], g.at[a]
            if n > 2:
                self.start(self.copy(src, index, a, 1, put(n - 1, delta, a), 0), c < n - 1)
                self.start(self.copy(src, index, a, -1, put(1, delta, a), 1), c > 0)
            else:
                for j in range(1, n):
                    self.start(self.copy(src, index, a, j, put(n - j, delta, a), 0), None)

    def begin(self):
        self.spread((0,) * len(self.g.dims), 0, self.own)

    def labels(self, stage):
        g, a = self.g, self.order[stage]
        n = g.dims[a]
        before = [range(g.dims[i]) if i in self.order[:stage] else range(1) for i in range(len(g.dims))]
        out = []
        if n > 2:
            c = g.at[a]
            near = [sorted((s for s in range(n) if s != k), key=lambda s: abs(s - k)) for k in range(n)]
            steps = []
            for t in range(n - 1):
                v = (near[0][t]) % n
                for k in range(1, n):
                    v = jnp.where(c == k, (near[k][t] - k) % n, v)
                steps.append(v)
        else:
            steps = list(range(1, n))
        for s in steps:
            for d in itertools.product(*before):
                out.append(put(s, d, a))
        return out

    def arrive(self, label, stage):
        g, a = self.g, self.order[stage]
        n, c = g.dims[a], g.at[a]
        index = g.index(label)
        here = self.slot(index)
        pltpu.make_async_remote_copy(
            src_ref=here, dst_ref=here, send_sem=self.send.at[0, 0], recv_sem=self.recv.at[g.slot(label)],
            device_id=(g.peer(a, 1), lax.axis_index(FSDP)), device_id_type=MESH).wait_recv()
        if n > 2:
            k = label[a]
            below = c + k >= n
            up = jnp.logical_and(below, c < n - 1)
            down = jnp.logical_and(jnp.logical_not(below), c > 0)
            self.start(self.copy(here, index, a, 1, put(k - 1, label, a), 0), up)
            self.start(self.copy(here, index, a, -1, put(k + 1, label, a), 1), down)
        self.spread(label, stage + 1, here)

    def end(self):
        for copy, cond in self.sent:
            if cond is None:
                copy.wait_send()
            else:
                pl.when(cond)(copy.wait_send)


def run_gathers(g, gs, stages=None):
    for stage in range(len(g.dims)):
        lists = [q.labels(stage) for q in gs]
        for i in range(max(map(len, lists))):
            for q, l in zip(gs, lists):
                if i < len(l):
                    q.arrive(l[i], stage)


def add_into(out, refs):
    rows = out.shape[0]
    step = max(s for s in range(16, 129, 16) if rows % s == 0)

    def some(i, carry):
        at = pl.ds(pl.multiple_of(i * step, step), step)
        out[at] = sum(r[at].astype(jnp.float32) for r in refs).astype(out.dtype)
        return carry

    lax.fori_loop(0, rows // step, some, 0)


def chosen(table, c):
    v = table[0]
    for k in range(1, len(table)):
        v = jnp.where(c == k, table[k], v)
    return v


class Reduce:
    def __init__(self, g, order, own, acc, land, send, recv):
        self.g, self.order, self.own, self.acc, self.land, self.send, self.recv = g, order, own, acc, land, send, recv
        self.sent = []
        self.stage = 0

    def held(self, delta):
        ref = self.own if self.stage == 0 else self.acc
        return ref(self.g.index(delta))

    @staticmethod
    def room(g, order):
        starts, total = [], 0
        for stage, a in enumerate(order):
            live = math.prod(g.dims[b] for b in order[stage:])
            starts.append(total)
            total += live // 2 if g.dims[a] == 2 else 2 * live
        return starts, total

    def spot(self, stage, way, label):
        g, a = self.g, self.order[stage]
        axes = self.order[stage + 1 :] if g.dims[a] == 2 else self.order[stage:]
        rank, live = 0, 1
        for b in axes:
            rank = rank + label[b] * live
            live *= g.dims[b]
        return self.room(g, self.order)[0][stage] + way * live + rank

    def ship(self, src, label, stage, step, way, at_label):
        g, axis = self.g, self.order[stage]
        spot = self.spot(stage, way, at_label)
        copy = pltpu.make_async_remote_copy(
            src_ref=src, dst_ref=self.land.at[spot], send_sem=self.send.at[g.slot(label)], recv_sem=self.recv.at[spot],
            device_id=(g.peer(axis, step), lax.axis_index(FSDP)), device_id_type=MESH)
        copy.start()
        self.sent.append(copy)

    def landed(self, stage, way, label):
        g = self.g
        spot = self.spot(stage, way, label)
        ref = self.land.at[spot]
        pltpu.make_async_remote_copy(
            src_ref=ref, dst_ref=ref, send_sem=self.send.at[0], recv_sem=self.recv.at[spot],
            device_id=(g.peer(self.order[0], 1), lax.axis_index(FSDP)), device_id_type=MESH).wait_recv()
        return ref

    def labels(self, stage):
        gone = self.order[:stage]
        ranges = [range(1) if i in gone else range(n) for i, n in enumerate(self.g.dims)]
        far = lambda d: -sum(1 for i in self.order[stage:] if d[i])
        return sorted(itertools.product(*ranges), key=far)

    def steps(self, stage):
        g, a = self.g, self.order[stage]
        n, c = g.dims[a], g.at[a]
        keep = [d for d in self.labels(stage) if d[a] == 0]
        out = []
        if n == 2:
            if stage == 0:
                out += [functools.partial(self.swap, put(1, d, a)) for d in keep]
            out += [functools.partial(self.take, d, stage) for d in keep]
        else:
            if stage == 0:
                out.append(self.copy_all)
            far = [sorted((k for k in range(1, n)), key=lambda k: -abs((p + k) % n - p)) for p in range(n)]
            for t in range(n - 1):
                k = chosen([far[p][t] for p in range(n)], c)
                out += [functools.partial(self.pass_on, put(k, d, a), stage) for d in keep]
            out += [functools.partial(self.close, d, stage) for d in keep]
        return out

    def copy_all(self):
        for d in self.g.all:
            i = self.g.index(d)
            add_into(self.acc(i), [self.own(i)])
        self.stage = 1

    def swap(self, d):
        self.ship(self.held(d), d, 0, 1, 0, d)

    def next_ship(self, d, stage):
        if stage + 1 < len(self.order):
            a = self.order[stage + 1]
            if self.g.dims[a] == 2 and d[a]:
                self.ship(self.acc(self.g.index(d)), d, stage + 1, 1, 0, d)

    def take(self, d, stage):
        a = self.order[stage]
        i = self.g.index(d)
        ref = self.own(i) if stage == 0 and self.stage == 0 else self.acc(i)
        add_into(self.acc(i), [ref, self.landed(stage, 0, put(1, d, a))])
        self.next_ship(d, stage)

    def pass_on(self, d, stage):
        g, a = self.g, self.order[stage]
        n, c = g.dims[a], g.at[a]
        k = d[a]
        up = c + k < n
        way = jnp.where(up, 0, 1)
        kept = self.acc(g.index(d))

        @pl.when(jnp.where(up, c > 0, c < n - 1))
        def _():
            add_into(kept, [kept, self.landed(stage, way, d)])

        self.ship(kept, d, stage, jnp.where(up, 1, n - 1), way, put(jnp.where(up, k - 1, lax.rem(k + 1, n)), d, a))

    def close(self, d, stage):
        g, a = self.g, self.order[stage]
        n, c = g.dims[a], g.at[a]
        kept = self.acc(g.index(d))

        @pl.when(c > 0)
        def _():
            add_into(kept, [kept, self.landed(stage, 0, d)])

        @pl.when(c < n - 1)
        def _():
            add_into(kept, [kept, self.landed(stage, 1, d)])

        self.next_ship(d, stage)

    def end(self):
        for copy in self.sent:
            copy.wait_send()


def interleave(lists):
    for i in range(max(map(len, lists))):
        for l in lists:
            if i < len(l):
                yield l[i]


def scatter_kernel(g, x_ref, o_ref, acc, land, send, recv):
    g.locate()
    entry_barrier(g, False)
    rows = x_ref.shape[1] // 2
    rs = []
    for p, order in enumerate(g.orders()):
        at = pl.ds(p * rows, rows)
        own = (lambda at: lambda i: x_ref.at[i, at])(at)
        kept = (lambda at: lambda i: acc.at[i, at])(at)
        rs.append(Reduce(g, order[::-1], own, kept, land.at[p], send.at[p], recv.at[p]))
    for stage in range(len(g.dims)):
        for step in interleave([r.steps(stage) for r in rs]):
            step()
        for r in rs:
            r.stage = 1
    o_ref[...] = acc[g.me].astype(jnp.float32)
    for r in rs:
        r.end()


def reduce_scatter_ctx(x, n, cid):
    g = Grid(n)
    _, rows, cols = x.shape
    room = max(Reduce.room(g, o[::-1])[1] for o in g.orders())
    dma = pltpu.SemaphoreType.DMA
    return pl.pallas_call(
        functools.partial(scatter_kernel, g),
        out_shape=jax.ShapeDtypeStruct((rows, cols), jnp.float32),
        in_specs=[pl.BlockSpec(memory_space=pltpu.VMEM)],
        out_specs=pl.BlockSpec(memory_space=pltpu.VMEM),
        scratch_shapes=[
            pltpu.VMEM((n, rows, cols), x.dtype),
            pltpu.VMEM((2, room, rows // 2, cols), x.dtype),
            dma((2, n)),
            dma((2, room)),
        ],
        compiler_params=pltpu.CompilerParams(collective_id=cid, has_side_effects=True, vmem_limit_bytes=60 << 20),
        name="ctx_reduce",
    )(x)


def row_cuts(rows, shares):
    tiles, total, seen, out = rows // 16, sum(shares), 0, []
    for s in shares:
        start = tiles * seen // total
        seen += s
        out.append((start * 16, (tiles * seen // total - start) * 16))
    return out


def reduce_parts(g, rows):
    rest = list(range(1, len(g.dims)))
    orders = [[0] + rest, [0] + rest[::-1], rest + [0], rest[::-1] + [0]]
    return [(*cut, orders[k]) for cut, (k, _) in zip(row_cuts(rows, [s for _, s in SHARES]), SHARES) if cut[1]]


def reduce_all_kernel(g, x_ref, o_ref, own, kept, send, recv, gsend, grecv, psend, precv, lsem, *lands):
    g.locate()
    entry_barrier(g, True)
    f = lax.axis_index(FSDP)
    cuts = reduce_parts(g, x_ref.shape[2])
    rs, gs = [], []
    for p, (r0, rn, order) in enumerate(cuts):
        at = (lambda r: lambda i: kept.at[i, r])(pl.ds(r0, rn))
        to = (lambda r: lambda i: o_ref.at[i, r])(pl.ds(r0, rn))
        rs.append(Reduce(g, order[::-1], at, at, lands[p], send.at[p], recv.at[p]))
        gs.append(Gather(g, order, to(g.me), to, gsend.at[p], grecv.at[p]))
    local = pltpu.make_async_copy(x_ref.at[f], own, lsem)
    local.start()
    turns = [sorted(g.all, key=lambda d, a=r.order[0]: (d[a] == 0, -sum(1 for v in d if v))) for r in rs]
    pairs = {}
    for i in range(g.n):
        for p, (r0, rn, _) in enumerate(cuts):
            d = turns[p][i]
            k = g.index(d)
            at = pl.ds(r0, rn)
            c = pltpu.make_async_remote_copy(
                src_ref=x_ref.at[1 - f, k, at], dst_ref=kept.at[k, at], send_sem=psend.at[p, g.slot(d)],
                recv_sem=precv.at[p, g.slot(d)], device_id=(g.me, 1 - f), device_id_type=MESH)
            c.start()
            pairs[p, d] = c
    local.wait()
    for i in range(g.n):
        for p, r in enumerate(rs):
            d = turns[p][i]
            k = g.index(d)
            pairs[p, d].wait_recv()
            add_into(r.acc(k), [r.acc(k), own.at[k, pl.ds(cuts[p][0], cuts[p][1])]])
            a = r.order[0]
            if g.dims[a] == 2 and d[a]:
                r.swap(d)
    first = [[s for s in r.steps(0) if getattr(s, "func", s).__name__ in ("take", "pass_on", "close")] for r in rs]
    for r in rs:
        r.stage = 1
    for stage in range(len(g.dims)):
        lists = first if stage == 0 else [r.steps(stage) for r in rs]
        for step in interleave(lists):
            step()
    for r, q in zip(rs, gs):
        add_into(q.own, [r.acc(g.me)])
        q.begin()
    run_gathers(g, gs)
    for c in pairs.values():
        c.wait_send()
    for r in rs:
        r.end()
    for q in gs:
        q.end()


def reduce_all(x, n, cid):
    g = Grid(n)
    _, _, rows, cols = x.shape
    cuts = reduce_parts(g, rows)
    parts = len(cuts)
    rooms = [Reduce.room(g, order[::-1])[1] for _, _, order in cuts]
    dma = pltpu.SemaphoreType.DMA
    return pl.pallas_call(
        functools.partial(reduce_all_kernel, g),
        out_shape=jax.ShapeDtypeStruct((n, rows, cols), x.dtype),
        in_specs=[pl.BlockSpec(memory_space=pl.ANY)],
        out_specs=pl.BlockSpec(memory_space=pltpu.VMEM),
        scratch_shapes=[
            pltpu.VMEM((n, rows, cols), x.dtype),
            pltpu.VMEM((n, rows, cols), x.dtype),
            dma((parts, n)),
            dma((parts, max(rooms))),
            dma((parts, 2, n)),
            dma((parts, n)),
            dma((parts, n)),
            dma((parts, n)),
            dma(()),
        ]
        + [pltpu.VMEM((room, rn, cols), x.dtype) for room, (_, rn, _) in zip(rooms, cuts)],
        compiler_params=pltpu.CompilerParams(collective_id=cid, has_side_effects=True, vmem_limit_bytes=64 << 20),
        name="grad_reduce",
    )(x)


def gather_kernel(g, count, spots, *refs):
    k = 2 if count else 1
    xs, ws = refs[:k], picked(refs[k : k + count], spots)
    refs = refs[k + count :]
    os, fulls = refs[:k], refs[k : k + len(spots)]
    refs = refs[k + len(spots) :]
    send, recv, local = refs[:3]
    g.locate()
    entry_barrier(g, bool(count))
    rows = xs[0].shape[0] // 2
    gs = []
    for p, order in enumerate(g.orders()):
        at = pl.ds(p * rows, rows)
        slot = (lambda at: lambda i: os[0].at[i, at])(at)
        gs.append(Gather(g, order, xs[0].at[at], slot, send.at[p], recv.at[p]))
    if count:
        gs.append(Gather(g, g.orders()[0], xs[1], lambda i: os[1].at[i], send.at[2], recv.at[2]))
    for q in gs:
        q.begin()
    mine = [pltpu.make_async_copy(x, o.at[g.me], local.at[i]) for i, (x, o) in enumerate(zip(xs, os))]
    for c in mine:
        c.start()
    swap = Swap(ws, fulls, *refs[3:]) if count else None
    if count:
        swap.begin()
    run_gathers(g, gs)
    for c in mine:
        c.wait()
    if count:
        swap.end()
    for q in gs:
        q.end()


class Swap:
    def __init__(self, srcs, dsts, send, recv, load, store, *stages):
        c, f = lax.axis_index(CTX), lax.axis_index(FSDP)
        self.remote, self.loads, self.stores = [], [], []
        for i, (s, d, v) in enumerate(zip(srcs, dsts, stages)):
            self.remote.append(
                pltpu.make_async_remote_copy(
                    src_ref=s, dst_ref=d.at[f], send_sem=send.at[i], recv_sem=recv.at[i], device_id=(c, 1 - f),
                    device_id_type=MESH))
            self.loads.append(pltpu.make_async_copy(s, v, load.at[i]))
            self.stores.append(pltpu.make_async_copy(v, d.at[f], store.at[i]))

    def begin(self):
        for c in self.remote + self.loads:
            c.start()
        for a, b in zip(self.loads, self.stores):
            a.wait()
            b.start()

    def end(self):
        for c in self.stores + self.remote:
            c.wait()

    @staticmethod
    def scratch(picks):
        return [pltpu.SemaphoreType.DMA((len(picks),))] * 4 + [pltpu.VMEM(shape_of(a, l), a.dtype) for a, l in picks]


def distinct(picks):
    arrays, places = [], []
    for a, l in picks:
        spot = next((i for i, b in enumerate(arrays) if b is a), None)
        if spot is None:
            spot = len(arrays)
            arrays.append(a)
        places.append((spot, l))
    return arrays, places


def picked(refs, places):
    return [refs[i] if l is None else refs[i].at[l] for i, l in places]


def shape_of(a, l):
    return a.shape if l is None else a.shape[1:]


def all_gather_ctx(x, n, cid, places=None, weights=()):
    g = Grid(n)
    arrays, spots = distinct(weights)
    count = len(arrays)
    xs = [x] if places is None else [x, places]
    dma = pltpu.SemaphoreType.DMA
    vmem, anywhere = pl.BlockSpec(memory_space=pltpu.VMEM), pl.BlockSpec(memory_space=pl.ANY)
    parts = len(xs) + 1
    return pl.pallas_call(
        functools.partial(gather_kernel, g, count, spots),
        out_shape=[jax.ShapeDtypeStruct((n, *v.shape), v.dtype) for v in xs]
        + [jax.ShapeDtypeStruct((2, *shape_of(a, l)), a.dtype) for a, l in weights],
        in_specs=[vmem] * len(xs) + [anywhere] * count,
        out_specs=[vmem] * len(xs) + [anywhere] * len(weights),
        scratch_shapes=[dma((parts, 2, n)), dma((parts, n)), dma((2,))] + (Swap.scratch(weights) if count else []),
        compiler_params=pltpu.CompilerParams(collective_id=cid, has_side_effects=True, vmem_limit_bytes=60 << 20),
        name="ctx_gather",
    )(*xs, *arrays)


def exchange_kernel(count, spots, *refs):
    srcs, dsts = picked(refs[:count], spots), refs[count : count + len(spots)]
    c, f = lax.axis_index(CTX), lax.axis_index(FSDP)
    sem = pltpu.get_barrier_semaphore()
    pl.semaphore_signal(sem, inc=1, device_id=(c, 1 - f), device_id_type=MESH)
    pl.semaphore_wait(sem, 1)
    swap = Swap(srcs, dsts, *refs[count + len(spots) :])
    swap.begin()
    swap.end()


def exchange(picks, cid):
    arrays, spots = distinct(picks)
    anywhere = pl.BlockSpec(memory_space=pl.ANY)
    return pl.pallas_call(
        functools.partial(exchange_kernel, len(arrays), spots),
        out_shape=[jax.ShapeDtypeStruct((2, *shape_of(a, l)), a.dtype) for a, l in picks],
        in_specs=[anywhere] * len(arrays),
        out_specs=[anywhere] * len(picks),
        scratch_shapes=Swap.scratch(picks),
        compiler_params=pltpu.CompilerParams(collective_id=cid, has_side_effects=True),
        name="exchange",
    )(*arrays)


HEADS = 9
KV_HEADS = 3
HEAD = 64
GROUP = HEADS // KV_HEADS
EPS = 1e-05
ROPE_BASE = 100000.0
F32, BF16 = jnp.float32, jnp.bfloat16
CHUNK = 256
ROOM = 62 << 20


def nn(a, b):
    return lax.dot_general(a, b, (((1,), (0,)), ((), ())), preferred_element_type=F32)


def nt(a, b):
    return lax.dot_general(a, b, (((1,), (1,)), ((), ())), preferred_element_type=F32)


def tn(a, b):
    return lax.dot_general(a, b, (((0,), (0,)), ((), ())), preferred_element_type=F32)


def rms(v, gain):
    return v * lax.rsqrt(jnp.mean(v * v, axis=-1, keepdims=True) + EPS) * gain


def rms_back(v, gain, e):
    r = lax.rsqrt(jnp.mean(v * v, axis=-1, keepdims=True) + EPS)
    eg = e * gain
    dv = r * eg - v * (r * r * r) * jnp.mean(eg * v, axis=-1, keepdims=True)
    return dv, jnp.sum(e * v * r, axis=0, keepdims=True)


def rope(t, cos, sin):
    width = t.shape[1]
    out = []
    for lo in range(0, width, 128):
        w = min(128, width - lo)
        u = t[:, lo : lo + w]
        if w == 128:
            lane = lax.broadcasted_iota(jnp.int32, u.shape, 1) % HEAD
            other = jnp.where(lane < HEAD // 2, pltpu.roll(u, 128 - HEAD // 2, 1), pltpu.roll(u, HEAD // 2, 1))
        else:
            other = jnp.concatenate([u[:, HEAD // 2 :], u[:, : HEAD // 2]], axis=1)
        out.append((lo, w, u * cos[:, :w] + other * sin[:, :w]))
    return out


def call(kernel, outs, args, name, scratch=(), prefetch=0, blob=None):
    vmem = pl.BlockSpec(memory_space=pltpu.VMEM)
    smem = pl.BlockSpec(memory_space=pltpu.SMEM)
    anywhere = pl.BlockSpec(memory_space=pl.ANY)
    if blob is not None:
        new = isinstance(blob, tuple)
        return pl.pallas_call(
            kernel,
            out_shape=[jax.ShapeDtypeStruct(s, t) for s, t in outs] + [jax.ShapeDtypeStruct(blob if new else blob.shape, BF16)],
            in_specs=[vmem] * len(args) + ([] if new else [anywhere]),
            out_specs=[vmem] * len(outs) + [anywhere],
            scratch_shapes=list(scratch),
            input_output_aliases={} if new else {len(args): len(outs)},
            compiler_params=pltpu.CompilerParams(vmem_limit_bytes=ROOM),
            name=name,
        )(*args, *([] if new else [blob]))
    return pl.pallas_call(
        kernel,
        out_shape=[jax.ShapeDtypeStruct(s, t) for s, t in outs],
        in_specs=[smem] * prefetch + [vmem] * (len(args) - prefetch),
        out_specs=[vmem] * len(outs),
        scratch_shapes=list(scratch),
        compiler_params=pltpu.CompilerParams(vmem_limit_bytes=ROOM),
        name=name,
    )(*args)


def gain_of(ref, l):
    return jnp.concatenate([ref[0, l : l + 1].astype(F32), ref[1, l : l + 1].astype(F32)], axis=1)


def rows_of(ref):
    return jnp.concatenate([ref[s].astype(F32).T for s in range(ref.shape[0])], axis=0)


def put_turned(ref, value):
    r = ref.shape[2]
    for s in range(ref.shape[0]):
        ref[s] = value[s * r : (s + 1) * r].T.astype(ref.dtype)


def pre_kernel(l, x_ref, gain_ref, wq_ref, wk_ref, wv_ref, cos_ref, sin_ref, a_ref, q_ref, kv_ref, *turned):
    if turned:
        x = rows_of(x_ref)
        turned[0][...] = x
    else:
        x = x_ref[...]
    a = rms(x, gain_of(gain_ref, l)).astype(BF16)
    a_ref[...] = a
    cos, sin = cos_ref[...], sin_ref[...]
    for lo, w, piece in rope(nn(a, wq_ref[...]), cos, sin):
        q_ref[:, lo : lo + w] = piece.astype(BF16)
    keys = jnp.concatenate([piece for _, _, piece in rope(nn(a, wk_ref[...]), cos, sin)], axis=1)
    kv_ref[...] = jnp.concatenate([keys, nn(a, wv_ref[...])], axis=1).astype(BF16)


def pre(l, x, gain, wq, wk, wv, cos, sin):
    m, d, e = cos.shape[0], wq.shape[0], wk.shape[1]
    outs = [((m, d), BF16), ((m, d), BF16), ((m, 2 * e), BF16)] + ([((m, d), F32)] if x.ndim == 3 else [])
    return call(functools.partial(pre_kernel, l), outs, (x, gain, wq, wk, wv, cos, sin), "pre")


def half_of(u, src, dst):
    if src != dst:
        u = pltpu.roll(u, HEAD, 1)
    lane = lax.broadcasted_iota(jnp.int32, u.shape, 1)
    return jnp.where((lane < HEAD) if dst == 0 else (lane >= HEAD), u, 0.0)


def head_chunk(ref, s, h):
    lo = (h // 2) * 128
    width = ref.shape[-1]
    if lo + 128 <= width:
        return ref[s, :, lo : lo + 128].astype(F32)
    u = ref[s, :, lo:width].astype(F32)
    return jnp.concatenate([u, jnp.zeros_like(u)], axis=1)


def pack_heads(ref, s, dst, g, half, scale):
    rows = ref.shape[1] // 2
    for i in range(GROUP):
        h = g * GROUP + i
        u = half_of(head_chunk(ref, s, h) * scale, h % 2, half).astype(BF16)
        for part in range(2):
            dst[g * 2 + part, i * rows : (i + 1) * rows, :] = u[part * rows : (part + 1) * rows]


def sort_rows(block_ref, s, src, dst, n, rows):
    def one(j, carry):
        b = block_ref[j, s, 0] // rows
        dst[pl.ds(pl.multiple_of(b * rows, rows), rows), :] = src[j, s, 0:rows, :]
        dst[pl.ds(pl.multiple_of((2 * n - 1 - b) * rows, rows), rows), :] = src[j, s, rows : 2 * rows, :]
        return carry

    lax.fori_loop(0, n, one, 0)


def visible(c, block, rows, shape):
    key = lax.broadcasted_iota(jnp.int32, shape, 0) + c * CHUNK
    query = lax.broadcasted_iota(jnp.int32, shape, 1) % rows + block * rows
    return key <= query


def key_lanes(g):
    return (g // 2) * 128, g % 2


def value_lanes(g):
    return ((KV_HEADS + g) // 2) * 128, (KV_HEADS + g) % 2


def turn_rows(src, lo, dst, count):
    def one(c, carry):
        at = pl.ds(pl.multiple_of(c * CHUNK, CHUNK), CHUNK)
        dst[:, at] = src[at, lo : lo + 256].astype(F32).T.astype(BF16)
        return carry

    lax.fori_loop(0, count, one, 0)


def attend_kernel(
    n, block_ref, mine_ref, q_ref, kv_ref, o_ref, lse_ref, sorted_ref, turned_ref, qp_ref, st_ref, acc_ref, stat_ref
):
    rows = q_ref.shape[1] // 2
    wide = GROUP * rows
    groups = range(KV_HEADS)
    vlo = HEAD * KV_HEADS // 128 * 128
    voff = HEAD * KV_HEADS - vlo

    def sequence(s, carry):
        sort_rows(block_ref, s, kv_ref, sorted_ref, n, rows)
        turn_rows(sorted_ref, vlo, turned_ref, n * 2 * rows // CHUNK)
        for g in groups:
            pack_heads(q_ref, s, qp_ref, g, key_lanes(g)[1], HEAD**-0.5)
        low = mine_ref[s, 0] // rows
        for part in range(2):
            block = low if part == 0 else 2 * n - 1 - low
            last = block * rows // CHUNK
            stat_ref[...] = jnp.full_like(stat_ref, -1e30)

            def score(c, masked):
                at = pl.ds(pl.multiple_of(c * CHUNK, CHUNK), CHUNK)
                for g in groups:
                    klo, _ = key_lanes(g)
                    st = nt(sorted_ref[at, klo : klo + 128], qp_ref[g * 2 + part])
                    if masked:
                        st = jnp.where(visible(c, block, rows, st.shape), st, -1e30)
                    st_ref[g, at, :] = st
                    stat_ref[g] = jnp.maximum(stat_ref[g], jnp.max(st.reshape(CHUNK // 8, 8, wide), axis=0))

            def scores(c, carry):
                score(c, False)
                return carry

            lax.fori_loop(0, last, scores, 0)
            score(last, True)
            tops = [jnp.max(stat_ref[g], axis=0, keepdims=True) for g in groups]
            stat_ref[...] = jnp.zeros_like(stat_ref)
            acc_ref[...] = jnp.zeros_like(acc_ref)

            def mix(c, tops):
                at = pl.ds(pl.multiple_of(c * CHUNK, CHUNK), CHUNK)
                for g in groups:
                    p = jnp.exp(st_ref[g, at, :] - tops[g])
                    stat_ref[g] += jnp.sum(p.reshape(CHUNK // 8, 8, wide), axis=0)
                    acc_ref[g] += nn(turned_ref[voff + g * HEAD : voff + (g + 1) * HEAD, at], p.astype(BF16))
                return tops

            tops = lax.fori_loop(0, last + 1, mix, tuple(tops))
            for g in groups:
                total = jnp.sum(stat_ref[g], axis=0, keepdims=True)
                lse_ref[s, g * 2 + part] = tops[g] + jnp.log(total)
                out = (acc_ref[g] / total).T
                for i in range(GROUP):
                    h = g * GROUP + i
                    o_ref[s, part * rows : (part + 1) * rows, h * HEAD : (h + 1) * HEAD] = out[i * rows : (i + 1) * rows]
        return carry

    lax.fori_loop(0, q_ref.shape[0], sequence, 0)


def attend(blocks, mine, q, kv):
    seqs, r, d = q.shape
    n = kv.shape[0]
    wide = GROUP * r // 2
    scratch = [
        pltpu.VMEM((n * r, kv.shape[-1]), BF16),
        pltpu.VMEM((256, n * r), BF16),
        pltpu.VMEM((2 * KV_HEADS, wide, 128), BF16),
        pltpu.VMEM((KV_HEADS, n * r, wide), F32),
        pltpu.VMEM((KV_HEADS, HEAD, wide), F32),
        pltpu.VMEM((KV_HEADS, 8, wide), F32),
    ]
    outs = [((seqs, r, d), F32), ((seqs, 2 * KV_HEADS, 1, wide), F32)]
    return call(functools.partial(attend_kernel, n), outs, (blocks, mine, q, kv), "attend", scratch, 2)


def attend_back_kernel(
    n, block_ref, mine_ref, q_ref, kv_ref, do_ref, o_ref, lse_ref, dq_ref, dkv_ref,
    sorted_ref, turned_ref, qp_ref, dop_ref, acc_ref, delta_ref, dqt_ref,
):
    rows = q_ref.shape[1] // 2
    wide = GROUP * rows
    groups = range(KV_HEADS)

    def sequence(s, carry):
        sort_rows(block_ref, s, kv_ref, sorted_ref, n, rows)
        turn_rows(sorted_ref, 0, turned_ref, n * 2 * rows // CHUNK)
        for g in groups:
            pack_heads(q_ref, s, qp_ref, g, key_lanes(g)[1], HEAD**-0.5)
            pack_heads(do_ref, s, dop_ref, g, value_lanes(g)[1], 1.0)
        acc_ref[...] = jnp.zeros_like(acc_ref)
        low = mine_ref[s, 0] // rows
        for part in range(2):
            block = low if part == 0 else 2 * n - 1 - low
            last = block * rows // CHUNK
            deltas = []
            for g in groups:
                sums = []
                for i in range(GROUP):
                    h = g * GROUP + i
                    lanes = slice(h * HEAD, (h + 1) * HEAD)
                    at = slice(part * rows, (part + 1) * rows)
                    both = do_ref[s, at, lanes].astype(F32) * o_ref[s, at, lanes]
                    sums.append(jnp.sum(both, axis=1, keepdims=True))
                delta_ref[...] = jnp.concatenate(sums, axis=0) + jnp.zeros((wide, 128), F32)
                deltas.append(delta_ref[...].T[0:1])
            dqt_ref[...] = jnp.zeros_like(dqt_ref)

            def step(c, deltas, masked):
                at = pl.ds(pl.multiple_of(c * CHUNK, CHUNK), CHUNK)
                sums = [None] * (2 * KV_HEADS * HEAD // 128)
                for g in groups:
                    klo, _ = key_lanes(g)
                    vlo, _ = value_lanes(g)
                    qp, dop = qp_ref[g * 2 + part], dop_ref[g * 2 + part]
                    p = jnp.exp(nt(sorted_ref[at, klo : klo + 128], qp) - lse_ref[s, g * 2 + part])
                    if masked:
                        p = jnp.where(visible(c, block, rows, p.shape), p, 0.0)
                    dp = nt(sorted_ref[at, vlo : vlo + 128], dop)
                    ds = (p * (dp - deltas[g])).astype(BF16)
                    for lo, v in ((vlo // 128, nn(p.astype(BF16), dop)), (klo // 128, nn(ds, qp))):
                        sums[lo] = v if sums[lo] is None else sums[lo] + v
                    dqt_ref[g] += nn(turned_ref[g * HEAD : (g + 1) * HEAD, at], ds)
                for k, v in enumerate(sums):
                    acc_ref[at, k * 128 : (k + 1) * 128] += v
                return deltas

            deltas = lax.fori_loop(0, last, lambda c, t: step(c, t, False), tuple(deltas))
            step(last, deltas, True)
            for g in groups:
                dq = dqt_ref[g].T * HEAD**-0.5
                for i in range(GROUP):
                    h = g * GROUP + i
                    dq_ref[s, part * rows : (part + 1) * rows, h * HEAD : (h + 1) * HEAD] = dq[i * rows : (i + 1) * rows]

        def one(j, carry):
            b = block_ref[j, s, 0] // rows
            dkv_ref[j, s, 0:rows, :] = acc_ref[pl.ds(pl.multiple_of(b * rows, rows), rows), :].astype(BF16)
            dkv_ref[j, s, rows : 2 * rows, :] = acc_ref[
                pl.ds(pl.multiple_of((2 * n - 1 - b) * rows, rows), rows), :
            ].astype(BF16)
            return carry

        lax.fori_loop(0, n, one, 0)
        return carry

    lax.fori_loop(0, q_ref.shape[0], sequence, 0)


def attend_back(blocks, mine, q, kv, do, o, lse):
    seqs, r, d = q.shape
    n = kv.shape[0]
    wide = GROUP * r // 2
    scratch = [
        pltpu.VMEM((n * r, kv.shape[-1]), BF16),
        pltpu.VMEM((256, n * r), BF16),
        pltpu.VMEM((2 * KV_HEADS, wide, 128), BF16),
        pltpu.VMEM((2 * KV_HEADS, wide, 128), BF16),
        pltpu.VMEM((n * r, kv.shape[-1]), F32),
        pltpu.VMEM((wide, 128), F32),
        pltpu.VMEM((KV_HEADS, HEAD, wide), F32),
    ]
    outs = [((seqs, r, d), F32), (kv.shape, BF16)]
    args = (blocks, mine, q, kv, do, o, lse)
    return call(functools.partial(attend_back_kernel, n), outs, args, "attend_back", scratch, 2)


def down_at(wd_ref, i):
    per = wd_ref.shape[2] // CHUNK
    f = i // per
    return f, pl.ds(pl.multiple_of((i - f * per) * CHUNK, CHUNK), CHUNK)


def post_kernel(l, o_ref, x_ref, wo_ref, gain_ref, wg_ref, wu_ref, wd_ref, h_ref, b_ref, gate_ref, up_ref, y_ref, *turned):
    sum_ref = turned[0] if turned else y_ref
    h = x_ref[...] + nn(o_ref[...].astype(BF16), wo_ref[...])
    h_ref[...] = h
    sum_ref[...] = h
    b_ref[...] = rms(h, gain_of(gain_ref, l)).astype(BF16)

    def some(i, carry):
        at = pl.ds(pl.multiple_of(i * CHUNK, CHUNK), CHUNK)
        b = b_ref[...]
        gate, up = nn(b, wg_ref[:, at]), nn(b, wu_ref[:, at])
        gate_ref[:, at], up_ref[:, at] = gate, up
        m = (gate * jax.nn.sigmoid(gate) * up).astype(BF16)
        f, spot = down_at(wd_ref, i)
        sum_ref[...] += nt(m, wd_ref[f, :, spot])
        return carry

    lax.fori_loop(0, wg_ref.shape[1] // CHUNK, some, 0)
    if turned:
        put_turned(y_ref, sum_ref[...])


def post(l, o, x, wo, gain, wg, wu, wd, turned=None):
    m, d = x.shape
    ff = wg.shape[1]
    outs = [((m, d), F32), ((m, d), BF16), ((m, ff), F32), ((m, ff), F32), (turned, BF16) if turned else ((m, d), F32)]
    scratch = [pltpu.VMEM((m, d), F32)] if turned else []
    return call(functools.partial(post_kernel, l), outs, (o, x, wo, gain, wg, wu, wd), "post", scratch)


def put_tiles(blob, base, value, count):
    rows = value.shape[0] // 2
    if value.shape[1] < count * 128:
        value = jnp.concatenate([value, jnp.zeros((2 * rows, count * 128 - value.shape[1]), value.dtype)], axis=1)
    for f in range(2):
        for j in range(count):
            piece = value[f * rows : (f + 1) * rows, j * 128 : (j + 1) * 128]
            blob[f, pl.ds(base + j * (rows // 16), rows // 16)] = piece.reshape(rows // 16, 16, 128)


def put_norm(blob, at, dg):
    half = dg.shape[1] // 2
    for f in range(2):
        v = dg[:, f * half : (f + 1) * half]
        v = jnp.concatenate([v, jnp.zeros((1, 384 - half), F32)], axis=1)
        rows = jnp.concatenate([v[:, 0:128], v[:, 128:256], v[:, 256:384], jnp.zeros((13, 128), F32)], axis=0)
        blob[f, at] = rows.astype(BF16)


def wide_of(cols):
    return -(-cols // 128)


def ffn_back_kernel(l, base, new, *refs):
    dy_ref, h_ref, b_ref, gate_ref, up_ref, o_ref, gain_ref, wo_ref, wg_ref, wu_ref, wd_ref = refs[:11]
    dh_ref, do_ref, out_ref, blob_ref, dyb_ref, dyt_ref, db_ref, bt_ref, sem = refs[11 if new else 12 :]
    m, d = h_ref.shape
    ff = wg_ref.shape[1]
    half = d // 2 // 16
    up_at = (ff // 128) * half
    low_at = 2 * up_at
    out_at = low_at + (ff // 256) * (d // 16)
    norm_at = out_at + wide_of(d) * half
    dy = rows_of(dy_ref) if len(dy_ref.shape) == 3 else dy_ref[...]
    dh_ref[...] = dy
    dyb_ref[...] = dy.astype(BF16)
    dyt_ref[...] = dyb_ref[...].T
    db_ref[...] = jnp.zeros_like(db_ref)
    bt_ref[...] = b_ref[...].T

    def some(i, carry):
        at = pl.ds(pl.multiple_of(i * CHUNK, CHUNK), CHUNK)
        f, spot = down_at(wd_ref, i)
        dm = nn(dyb_ref[...], wd_ref[f, :, spot])
        gate, up = gate_ref[:, at], up_ref[:, at]
        sig = jax.nn.sigmoid(gate)
        silu = gate * sig
        mid = (silu * up).astype(BF16)
        dgate = (dm * up * sig * (1.0 + gate * (1.0 - sig))).astype(BF16)
        dup = (dm * silu).astype(BF16)
        db_ref[...] += nt(dgate, wg_ref[:, at]) + nt(dup, wu_ref[:, at])
        bt = bt_ref[...]
        put_tiles(blob_ref, i * (CHUNK // 128) * half, nn(bt, dgate).astype(BF16), CHUNK // 128)
        put_tiles(blob_ref, up_at + i * (CHUNK // 128) * half, nn(bt, dup).astype(BF16), CHUNK // 128)
        gd = nn(dyt_ref[...], mid).astype(BF16)
        per = wd_ref.shape[2] // CHUNK
        for j in range(CHUNK // 128):
            start = low_at + ((i - f * per) * (CHUNK // 128) + j) * (d // 16)
            blob_ref[f, pl.ds(start, d // 16)] = gd[:, j * 128 : (j + 1) * 128].reshape(d // 16, 16, 128)
        return carry

    lax.fori_loop(0, ff // CHUNK, some, 0)
    first = pltpu.make_async_copy(blob_ref.at[:, pl.ds(0, out_at)], out_ref.at[:, pl.ds(base, out_at)], sem.at[0])
    first.start()
    dv, dg = rms_back(h_ref[...], gain_of(gain_ref, l), db_ref[...])
    dh = dh_ref[...] + dv
    dh_ref[...] = dh
    dhb = dh.astype(BF16)
    do_ref[...] = nt(dhb, wo_ref[...]).astype(BF16)
    put_tiles(blob_ref, out_at, tn(o_ref[...].astype(BF16), dhb).astype(BF16), wide_of(d))
    put_norm(blob_ref, norm_at, dg)
    rest = norm_at + 1 - out_at
    second = pltpu.make_async_copy(
        blob_ref.at[:, pl.ds(out_at, rest)], out_ref.at[:, pl.ds(base + out_at, rest)], sem.at[1]
    )
    second.start()
    first.wait()
    second.wait()


def ffn_tiles(d, ff):
    return 2 * (ff // 128) * (d // 32) + (ff // 256) * (d // 16) + wide_of(d) * (d // 32) + 1


def ffn_back(l, blob, base, dy, h, b, gate, up, o, gain, wo, wg, wu, wd):
    m, d = h.shape
    ff = wg.shape[1]
    scratch = [
        pltpu.VMEM((2, ffn_tiles(d, ff), 16, 128), BF16),
        pltpu.VMEM((m, d), BF16),
        pltpu.VMEM((d, m), BF16),
        pltpu.VMEM((m, d), F32),
        pltpu.VMEM((d, m), BF16),
        pltpu.SemaphoreType.DMA((2,)),
    ]
    kernel = functools.partial(ffn_back_kernel, l, base, isinstance(blob, tuple))
    args = (dy, h, b, gate, up, o, gain, wo, wg, wu, wd)
    return call(kernel, [((m, d), F32), ((m, d), BF16)], args, "ffn_back", scratch, blob=blob)


def pre_tiles(d, e):
    return wide_of(d) * (d // 32) + wide_of(2 * e) * (d // 32) + 1


def pre_back_kernel(l, base, *refs):
    dq_ref, dkv_ref, a_ref, x_ref, dh_ref, gain_ref, wq_ref, wk_ref, wv_ref, cos_ref, sin_ref = refs[:11]
    dx_ref, out_ref, blob_ref, dqp_ref, sem = refs[12:]
    d = x_ref.shape[1]
    e = wk_ref.shape[1]
    half = d // 2 // 16
    cos, sin = cos_ref[...], -sin_ref[...]
    for lo, w, piece in rope(dq_ref[...], cos, sin):
        dqp_ref[:, lo : lo + w] = piece.astype(BF16)
    dqp = dqp_ref[...]
    dkv = dkv_ref[...]
    dkp = jnp.concatenate([piece for _, _, piece in rope(dkv[:, :e], cos, sin)], axis=1).astype(BF16)
    dvr = dkv[:, e:].astype(BF16)
    da = nt(dqp, wq_ref[...]) + nt(dkp, wk_ref[...]) + nt(dvr, wv_ref[...])
    dv, dg = rms_back(x_ref[...], gain_of(gain_ref, l), da)
    kv_at = wide_of(d) * half
    norm_at = kv_at + wide_of(2 * e) * half
    put_norm(blob_ref, norm_at, dg)
    left = blob_ref.shape[1] - norm_at - 1
    if left:
        blob_ref[:, pl.ds(norm_at + 1, left)] = jnp.zeros((2, left, 16, 128), BF16)
    at = a_ref[...].T
    put_tiles(blob_ref, 0, nn(at, dqp).astype(BF16), wide_of(d))
    put_tiles(blob_ref, kv_at, jnp.concatenate([nn(at, dkp), nn(at, dvr)], axis=1).astype(BF16), wide_of(2 * e))
    done = pltpu.make_async_copy(blob_ref, out_ref.at[:, pl.ds(base, blob_ref.shape[1])], sem)
    done.start()
    if len(dx_ref.shape) == 3:
        put_turned(dx_ref, dh_ref[...] + dv)
    else:
        dx_ref[...] = dh_ref[...] + dv
    done.wait()


def pre_back(l, shape, blob, base, tiles, dq, dkv, a, x, dh, gain, wq, wk, wv, cos, sin):
    m, d = x.shape
    scratch = [pltpu.VMEM((2, tiles, 16, 128), BF16), pltpu.VMEM((m, d), BF16), pltpu.SemaphoreType.DMA(())]
    args = (dq, dkv, a, x, dh, gain, wq, wk, wv, cos, sin)
    return call(functools.partial(pre_back_kernel, l, base), [(shape, F32)], args, "pre_back", scratch, blob=blob)


def unpack_kernel(places, blob, *outs):
    g_attn, gq, gk, gv, go, g_ffn, gg, gu, gd = outs
    half, d, e, ff = gq.shape[1], gq.shape[2], gk.shape[2], gg.shape[2]
    t = half // 16

    def take(base, at, rows, cols, out, l, skip=0):
        for lo in range(0, cols, 128):
            w = min(128, cols - lo)
            j = (skip + lo) // 128
            if (skip + lo) % 128 == 0:
                u = blob[pl.ds(base + at + j * (rows // 16), rows // 16)].reshape(rows, 128)[:, :w]
            else:
                u = blob[pl.ds(base + at + j * (rows // 16), rows // 16)].reshape(rows, 128)[:, 64:]
                if w > 64:
                    v = blob[pl.ds(base + at + (j + 1) * (rows // 16), rows // 16)].reshape(rows, 128)[:, : w - 64]
                    u = jnp.concatenate([u.astype(F32), v.astype(F32)], axis=1)
            out[l, :, lo : lo + w] = u.astype(F32)

    def norm(base, at, out, l):
        u = blob[base + at].astype(F32)
        row = jnp.concatenate([u[0:1], u[1:2], u[2:3]], axis=1)
        out[l : l + 1, :] = row[:, :half]

    for l, (ffn, att) in enumerate(places):
        up_at = (ff // 128) * t
        low_at = 2 * up_at
        out_at = low_at + (ff // 256) * (d // 16)
        take(ffn, 0, half, ff, gg, l)
        take(ffn, up_at, half, ff, gu, l)
        take(ffn, low_at, d, ff // 2, gd, l)
        take(ffn, out_at, half, d, go, l)
        norm(ffn, out_at + wide_of(d) * t, g_ffn, l)
        take(att, 0, half, d, gq, l)
        kv_at = wide_of(d) * t
        take(att, kv_at, half, e, gk, l)
        take(att, kv_at, half, e, gv, l, e)
        norm(att, kv_at + wide_of(2 * e) * t, g_attn, l)


def unpack(blob, places, shapes):
    return call(functools.partial(unpack_kernel, places), [(s, F32) for s in shapes], (blob,), "unpack")


def body(tokens, positions, norm_attn, w_query, w_key, w_value, w_out, norm_ffn, w_gate, w_up, w_down, cotangent):
    layers = norm_attn.shape[0]
    n = lax.axis_size(CTX)
    seqs, r, d = tokens.shape
    m = seqs * r
    e, ff = w_key.shape[2], w_gate.shape[2]
    own = (w_query, w_key, w_value, w_out, w_gate, w_up, jnp.swapaxes(w_down, 1, 2))
    shards = [(w, l) for l in range(layers) for w in own]
    full = exchange([(norm_attn, None), (norm_ffn, None), *shards[:3]], 0)
    gain_attn, gain_ffn, *full = full
    frequency = jnp.exp(jnp.arange(HEAD // 2, dtype=F32) * (-jnp.log(ROPE_BASE) / (HEAD // 2)))
    angles = positions.reshape(m, 1).astype(F32) * frequency
    cos, sin = jnp.cos(angles), jnp.sin(angles)
    cos = jnp.concatenate([cos] * 4, axis=1)
    sin = jnp.concatenate([-sin, sin] * 2, axis=1)
    x = jnp.swapaxes(tokens, 1, 2)
    kept = []
    weights = []

    def joined(w):
        return w.reshape(2 * w.shape[1], w.shape[2])

    for l in range(layers):
        wq, wk, wv = (joined(w) for w in full[l * len(own) : l * len(own) + 3])
        a, q, kv, *turned = pre(l, x, gain_attn, wq, wk, wv, cos, sin)
        if turned:
            (x,) = turned
        q = q.reshape(seqs, r, d)
        if l == 0:
            kv, places, *rest = all_gather_ctx(kv, n, 1, positions, shards[3:])
            full = [*full, *rest]
        else:
            (kv,) = all_gather_ctx(kv, n, 1 + l)
        wo, wg, wu = (joined(w) for w in full[l * len(own) + 3 : l * len(own) + 6])
        wd = full[l * len(own) + 6]
        weights.append((wq, wk, wv, wo, wg, wu, wd))
        kv = kv.reshape(n, seqs, r, 2 * e)
        o, lse = attend(places, positions, q, kv)
        turned = (seqs, d, r) if l == layers - 1 else None
        h, b, gate, up, y = post(l, o.reshape(m, d), x, wo, gain_ffn, wg, wu, wd, turned)
        kept.append((x, a, q, kv, o, lse, h, b, gate, up))
        x = y
    output = jnp.swapaxes(x, 1, 2)
    dy = jnp.swapaxes(cotangent, 1, 2)
    one, two = ffn_tiles(d, ff), pre_tiles(d, e)
    unit = 2 * n
    whole = -(-layers * (one + two) // unit) * unit
    blob = (2, whole, 16, 128)
    spots = []
    for l in reversed(range(layers)):
        wq, wk, wv, wo, wg, wu, wd = weights[l]
        x, a, q, kv, o, lse, h, b, gate, up = kept[l]
        start = (layers - 1 - l) * (one + two)
        spots.insert(0, (start, start + one))
        dh, do, blob = ffn_back(l, blob, start, dy, h, b, gate, up, o.reshape(m, d), gain_ffn, wo, wg, wu, wd)
        dq, dkv = attend_back(places, positions, q, kv, do.reshape(seqs, r, d), o, lse)
        dkv = reduce_scatter_ctx(dkv.reshape(n, m, 2 * e), n, 1 + layers + l)
        tiles = two if l else whole - start - one
        shape = (m, d) if l else (seqs, d, r)
        dy, blob = pre_back(
            l, shape, blob, start + one, tiles, dq.reshape(m, d), dkv, a, x, dh, gain_attn, wq, wk, wv, cos, sin
        )
    total = reduce_all(blob.reshape(2, n, -1, 128), n, 1 + 2 * layers)
    shapes = [norm_attn.shape, *[w.shape for w in own[:4]], norm_ffn.shape, *[w.shape for w in own[4:]]]
    grads = unpack(total.reshape(whole, 16, 128), spots, shapes)
    return (output, jnp.swapaxes(dy, 1, 2), *grads[:-1], jnp.swapaxes(grads[-1], 1, 2))


def solution(mesh):
    in_specs = (
        P("fsdp", "ctx", None),
        P("fsdp", "ctx"),
        P(None, "fsdp"),
        P(None, "fsdp", None),
        P(None, "fsdp", None),
        P(None, "fsdp", None),
        P(None, "fsdp", None),
        P(None, "fsdp"),
        P(None, "fsdp", None),
        P(None, "fsdp", None),
        P(None, "fsdp", None),
        P("fsdp", "ctx", None),
    )
    out_specs = (
        P("fsdp", "ctx", None),
        P("fsdp", "ctx", None),
        P(None, "fsdp"),
        P(None, "fsdp", None),
        P(None, "fsdp", None),
        P(None, "fsdp", None),
        P(None, "fsdp", None),
        P(None, "fsdp"),
        P(None, "fsdp", None),
        P(None, "fsdp", None),
        P(None, "fsdp", None),
    )
    return jax.shard_map(body, mesh=mesh, in_specs=in_specs, out_specs=out_specs, check_vma=False)
```

```python
import functools
import itertools
import math

import jax
import jax.numpy as jnp
from jax import lax
from jax.experimental import pallas as pl
from jax.experimental.pallas import tpu as pltpu
from jax.sharding import PartitionSpec as P

CTX, FSDP = "ctx", "fsdp"
MESH = pl.DeviceIdType.MESH
SHARES = ((0, 6), (1, 6), (2, 2), (3, 2))


def factors(n):
    known = {16: (4, 2, 2), 64: (2, 4, 4, 2)}
    if n in known:
        return known[n]
    out, p = [], 2
    while n > 1:
        while n % p == 0:
            out.append(p)
            n //= p
        p += 1
    return tuple(out) or (1,)


class Grid:
    def __init__(self, n):
        self.n = n
        self.dims = factors(n)
        strides, s = [], 1
        for d in reversed(self.dims):
            strides.insert(0, s)
            s *= d
        self.strides = tuple(strides)
        self.all = list(itertools.product(*[range(d) for d in self.dims]))
        self.ident = {d: i for i, d in enumerate(self.all)}

    def locate(self):
        me = lax.axis_index(CTX)
        self.me = me
        self.at = [lax.rem(me // s, d) for s, d in zip(self.strides, self.dims)]

    def index(self, delta):
        out = 0
        for c, d, n, s in zip(self.at, delta, self.dims, self.strides):
            out = out + (c if isinstance(d, int) and d == 0 else lax.rem(c + d, n)) * s
        return out

    def slot(self, delta):
        return sum(d * s for d, s in zip(delta, self.strides))

    def peer(self, axis, j):
        return self.index(tuple(j if a == axis else 0 for a in range(len(self.dims))))

    def orders(self):
        rest = list(range(1, len(self.dims)))
        return [[0] + rest, [0] + rest[::-1]]


def put(x, d, a):
    return tuple(x if i == a else v for i, v in enumerate(d))


def entry_barrier(g, fsdp):
    sem = pltpu.get_barrier_semaphore()
    count = 0
    f = lax.axis_index(FSDP)
    for a, d in enumerate(g.dims):
        for j in range(1, d):
            pl.semaphore_signal(sem, inc=1, device_id=(g.peer(a, j), f), device_id_type=MESH)
            count += 1
    if fsdp:
        pl.semaphore_signal(sem, inc=1, device_id=(g.me, 1 - f), device_id_type=MESH)
        count += 1
    pl.semaphore_wait(sem, count)


class Gather:
    def __init__(self, g, order, own, slot, send, recv):
        self.g, self.order, self.own, self.slot, self.send, self.recv = g, order, own, slot, send, recv
        self.sent = []

    def copy(self, src, index, axis, step, label, way):
        g = self.g
        i = g.slot(label)
        return pltpu.make_async_remote_copy(
            src_ref=src, dst_ref=self.slot(index), send_sem=self.send.at[way, i], recv_sem=self.recv.at[i],
            device_id=(g.peer(axis, step % g.dims[axis]), lax.axis_index(FSDP)), device_id_type=MESH)

    def start(self, copy, cond):
        self.sent.append((copy, cond))
        if cond is None:
            copy.start()
        else:
            pl.when(cond)(copy.start)

    def spread(self, delta, stage, src):
        g = self.g
        index = g.index(delta)
        for a in self.order[stage:]:
            n, c = g.dims[a], g.at[a]
            if n > 2:
                self.start(self.copy(src, index, a, 1, put(n - 1, delta, a), 0), c < n - 1)
                self.start(self.copy(src, index, a, -1, put(1, delta, a), 1), c > 0)
            else:
                for j in range(1, n):
                    self.start(self.copy(src, index, a, j, put(n - j, delta, a), 0), None)

    def begin(self):
        self.spread((0,) * len(self.g.dims), 0, self.own)

    def labels(self, stage):
        g, a = self.g, self.order[stage]
        n = g.dims[a]
        before = [range(g.dims[i]) if i in self.order[:stage] else range(1) for i in range(len(g.dims))]
        out = []
        if n > 2:
            c = g.at[a]
            near = [sorted((s for s in range(n) if s != k), key=lambda s: abs(s - k)) for k in range(n)]
            steps = []
            for t in range(n - 1):
                v = (near[0][t]) % n
                for k in range(1, n):
                    v = jnp.where(c == k, (near[k][t] - k) % n, v)
                steps.append(v)
        else:
            steps = list(range(1, n))
        for s in steps:
            for d in itertools.product(*before):
                out.append(put(s, d, a))
        return out

    def arrive(self, label, stage):
        g, a = self.g, self.order[stage]
        n, c = g.dims[a], g.at[a]
        index = g.index(label)
        here = self.slot(index)
        pltpu.make_async_remote_copy(
            src_ref=here, dst_ref=here, send_sem=self.send.at[0, 0], recv_sem=self.recv.at[g.slot(label)],
            device_id=(g.peer(a, 1), lax.axis_index(FSDP)), device_id_type=MESH).wait_recv()
        if n > 2:
            k = label[a]
            below = c + k >= n
            up = jnp.logical_and(below, c < n - 1)
            down = jnp.logical_and(jnp.logical_not(below), c > 0)
            self.start(self.copy(here, index, a, 1, put(k - 1, label, a), 0), up)
            self.start(self.copy(here, index, a, -1, put(k + 1, label, a), 1), down)
        self.spread(label, stage + 1, here)

    def end(self):
        for copy, cond in self.sent:
            if cond is None:
                copy.wait_send()
            else:
                pl.when(cond)(copy.wait_send)


def run_gathers(g, gs, stages=None):
    for stage in range(len(g.dims)):
        lists = [q.labels(stage) for q in gs]
        for i in range(max(map(len, lists))):
            for q, l in zip(gs, lists):
                if i < len(l):
                    q.arrive(l[i], stage)


def add_into(out, refs):
    rows = out.shape[0]
    step = max(s for s in range(16, 129, 16) if rows % s == 0)

    def some(i, carry):
        at = pl.ds(pl.multiple_of(i * step, step), step)
        out[at] = sum(r[at].astype(jnp.float32) for r in refs).astype(out.dtype)
        return carry

    lax.fori_loop(0, rows // step, some, 0)


def chosen(table, c):
    v = table[0]
    for k in range(1, len(table)):
        v = jnp.where(c == k, table[k], v)
    return v


class Reduce:
    def __init__(self, g, order, own, acc, land, send, recv):
        self.g, self.order, self.own, self.acc, self.land, self.send, self.recv = g, order, own, acc, land, send, recv
        self.sent = []
        self.stage = 0

    def held(self, delta):
        ref = self.own if self.stage == 0 else self.acc
        return ref(self.g.index(delta))

    @staticmethod
    def room(g, order):
        starts, total = [], 0
        for stage, a in enumerate(order):
            live = math.prod(g.dims[b] for b in order[stage:])
            starts.append(total)
            total += live // 2 if g.dims[a] == 2 else 2 * live
        return starts, total

    def spot(self, stage, way, label):
        g, a = self.g, self.order[stage]
        axes = self.order[stage + 1 :] if g.dims[a] == 2 else self.order[stage:]
        rank, live = 0, 1
        for b in axes:
            rank = rank + label[b] * live
            live *= g.dims[b]
        return self.room(g, self.order)[0][stage] + way * live + rank

    def ship(self, src, label, stage, step, way, at_label):
        g, axis = self.g, self.order[stage]
        spot = self.spot(stage, way, at_label)
        copy = pltpu.make_async_remote_copy(
            src_ref=src, dst_ref=self.land.at[spot], send_sem=self.send.at[g.slot(label)], recv_sem=self.recv.at[spot],
            device_id=(g.peer(axis, step), lax.axis_index(FSDP)), device_id_type=MESH)
        copy.start()
        self.sent.append(copy)

    def landed(self, stage, way, label):
        g = self.g
        spot = self.spot(stage, way, label)
        ref = self.land.at[spot]
        pltpu.make_async_remote_copy(
            src_ref=ref, dst_ref=ref, send_sem=self.send.at[0], recv_sem=self.recv.at[spot],
            device_id=(g.peer(self.order[0], 1), lax.axis_index(FSDP)), device_id_type=MESH).wait_recv()
        return ref

    def labels(self, stage):
        gone = self.order[:stage]
        ranges = [range(1) if i in gone else range(n) for i, n in enumerate(self.g.dims)]
        far = lambda d: -sum(1 for i in self.order[stage:] if d[i])
        return sorted(itertools.product(*ranges), key=far)

    def steps(self, stage):
        g, a = self.g, self.order[stage]
        n, c = g.dims[a], g.at[a]
        keep = [d for d in self.labels(stage) if d[a] == 0]
        out = []
        if n == 2:
            if stage == 0:
                out += [functools.partial(self.swap, put(1, d, a)) for d in keep]
            out += [functools.partial(self.take, d, stage) for d in keep]
        else:
            if stage == 0:
                out.append(self.copy_all)
            far = [sorted((k for k in range(1, n)), key=lambda k: -abs((p + k) % n - p)) for p in range(n)]
            for t in range(n - 1):
                k = chosen([far[p][t] for p in range(n)], c)
                out += [functools.partial(self.pass_on, put(k, d, a), stage) for d in keep]
            out += [functools.partial(self.close, d, stage) for d in keep]
        return out

    def copy_all(self):
        for d in self.g.all:
            i = self.g.index(d)
            add_into(self.acc(i), [self.own(i)])
        self.stage = 1

    def swap(self, d):
        self.ship(self.held(d), d, 0, 1, 0, d)

    def next_ship(self, d, stage):
        if stage + 1 < len(self.order):
            a = self.order[stage + 1]
            if self.g.dims[a] == 2 and d[a]:
                self.ship(self.acc(self.g.index(d)), d, stage + 1, 1, 0, d)

    def take(self, d, stage):
        a = self.order[stage]
        i = self.g.index(d)
        ref = self.own(i) if stage == 0 and self.stage == 0 else self.acc(i)
        add_into(self.acc(i), [ref, self.landed(stage, 0, put(1, d, a))])
        self.next_ship(d, stage)

    def pass_on(self, d, stage):
        g, a = self.g, self.order[stage]
        n, c = g.dims[a], g.at[a]
        k = d[a]
        up = c + k < n
        way = jnp.where(up, 0, 1)
        kept = self.acc(g.index(d))

        @pl.when(jnp.where(up, c > 0, c < n - 1))
        def _():
            add_into(kept, [kept, self.landed(stage, way, d)])

        self.ship(kept, d, stage, jnp.where(up, 1, n - 1), way, put(jnp.where(up, k - 1, lax.rem(k + 1, n)), d, a))

    def close(self, d, stage):
        g, a = self.g, self.order[stage]
        n, c = g.dims[a], g.at[a]
        kept = self.acc(g.index(d))

        @pl.when(c > 0)
        def _():
            add_into(kept, [kept, self.landed(stage, 0, d)])

        @pl.when(c < n - 1)
        def _():
            add_into(kept, [kept, self.landed(stage, 1, d)])

        self.next_ship(d, stage)

    def end(self):
        for copy in self.sent:
            copy.wait_send()


def interleave(lists):
    for i in range(max(map(len, lists))):
        for l in lists:
            if i < len(l):
                yield l[i]


def scatter_kernel(g, x_ref, o_ref, acc, send, recv, *lands):
    g.locate()
    entry_barrier(g, False)
    rs = []
    for p, (r0, rn, order) in enumerate(reduce_parts(g, x_ref.shape[1])):
        at = pl.ds(r0, rn)
        own = (lambda at: lambda i: x_ref.at[i, at])(at)
        kept = (lambda at: lambda i: acc.at[i, at])(at)
        rs.append(Reduce(g, order[::-1], own, kept, lands[p], send.at[p], recv.at[p]))
    for stage in range(len(g.dims)):
        for step in interleave([r.steps(stage) for r in rs]):
            step()
        for r in rs:
            r.stage = 1
    o_ref[...] = acc[g.me].astype(jnp.float32)
    for r in rs:
        r.end()


def reduce_scatter_ctx(x, n, cid):
    g = Grid(n)
    _, rows, cols = x.shape
    cuts = reduce_parts(g, rows)
    rooms = [Reduce.room(g, order[::-1])[1] for _, _, order in cuts]
    dma = pltpu.SemaphoreType.DMA
    scratch = [pltpu.VMEM((n, rows, cols), x.dtype), dma((len(cuts), n)), dma((len(cuts), max(rooms)))]
    scratch += [pltpu.VMEM((room, rn, cols), x.dtype) for room, (_, rn, _) in zip(rooms, cuts)]
    out = ((rows, cols), jnp.float32)
    return pl.pallas_call(
        functools.partial(scatter_kernel, g),
        out_shape=jax.ShapeDtypeStruct(*out),
        in_specs=[pl.BlockSpec(memory_space=pltpu.VMEM)],
        out_specs=pl.BlockSpec(memory_space=pltpu.VMEM),
        scratch_shapes=scratch,
        compiler_params=pltpu.CompilerParams(
            collective_id=cid, has_side_effects=True, vmem_limit_bytes=grant([(x.shape, x.dtype), out], scratch)
        ),
        name="ctx_reduce",
    )(x)


def row_cuts(rows, shares):
    tiles, total, seen, out = rows // 16, sum(shares), 0, []
    for s in shares:
        start = tiles * seen // total
        seen += s
        out.append((start * 16, (tiles * seen // total - start) * 16))
    return out


def reduce_parts(g, rows):
    rest = list(range(1, len(g.dims)))
    orders = [[0] + rest, [0] + rest[::-1], rest + [0], rest[::-1] + [0]]
    return [(*cut, orders[k]) for cut, (k, _) in zip(row_cuts(rows, [s for _, s in SHARES]), SHARES) if cut[1]]


def reduce_all_kernel(g, x_ref, o_ref, kept, send, recv, gsend, grecv, psend, precv, *lands):
    g.locate()
    entry_barrier(g, True)
    f = lax.axis_index(FSDP)
    cuts = reduce_parts(g, x_ref.shape[2])
    rs, gs = [], []
    for p, (r0, rn, order) in enumerate(cuts):
        at = (lambda r: lambda i: kept.at[i, r])(pl.ds(r0, rn))
        to = (lambda r: lambda i: o_ref.at[i, r])(pl.ds(r0, rn))
        rs.append(Reduce(g, order[::-1], at, at, lands[p], send.at[p], recv.at[p]))
        gs.append(Gather(g, order, to(g.me), to, gsend.at[p], grecv.at[p]))
    turns = [sorted(g.all, key=lambda d, a=r.order[0]: (d[a] == 0, -sum(1 for v in d if v))) for r in rs]
    pairs = {}
    for i in range(g.n):
        for p, (r0, rn, _) in enumerate(cuts):
            d = turns[p][i]
            k = g.index(d)
            at = pl.ds(r0, rn)
            c = pltpu.make_async_remote_copy(
                src_ref=x_ref.at[1 - f, k, at], dst_ref=kept.at[k, at], send_sem=psend.at[p, g.slot(d)],
                recv_sem=precv.at[p, g.slot(d)], device_id=(g.me, 1 - f), device_id_type=MESH)
            c.start()
            pairs[p, d] = c
    for i in range(g.n):
        for p, r in enumerate(rs):
            d = turns[p][i]
            k = g.index(d)
            pairs[p, d].wait_recv()
            add_into(r.acc(k), [r.acc(k), x_ref.at[f, k, pl.ds(cuts[p][0], cuts[p][1])]])
            a = r.order[0]
            if g.dims[a] == 2 and d[a]:
                r.swap(d)
    first = [[s for s in r.steps(0) if getattr(s, "func", s).__name__ in ("take", "pass_on", "close")] for r in rs]
    for r in rs:
        r.stage = 1
    for stage in range(len(g.dims)):
        lists = first if stage == 0 else [r.steps(stage) for r in rs]
        for step in interleave(lists):
            step()
    for r, q in zip(rs, gs):
        add_into(q.own, [r.acc(g.me)])
        q.begin()
    run_gathers(g, gs)
    for c in pairs.values():
        c.wait_send()
    for r in rs:
        r.end()
    for q in gs:
        q.end()


def reduce_all(x, n, cid):
    g = Grid(n)
    _, _, rows, cols = x.shape
    cuts = reduce_parts(g, rows)
    parts = len(cuts)
    rooms = [Reduce.room(g, order[::-1])[1] for _, _, order in cuts]
    dma = pltpu.SemaphoreType.DMA
    scratch = [
        pltpu.VMEM((n, rows, cols), x.dtype),
        dma((parts, n)),
        dma((parts, max(rooms))),
        dma((parts, 2, n)),
        dma((parts, n)),
        dma((parts, n)),
        dma((parts, n)),
    ] + [pltpu.VMEM((room, rn, cols), x.dtype) for room, (_, rn, _) in zip(rooms, cuts)]
    out = ((n, rows, cols), x.dtype)
    return pl.pallas_call(
        functools.partial(reduce_all_kernel, g),
        out_shape=jax.ShapeDtypeStruct(*out),
        in_specs=[pl.BlockSpec(memory_space=pltpu.VMEM)],
        out_specs=pl.BlockSpec(memory_space=pltpu.VMEM),
        scratch_shapes=scratch,
        compiler_params=pltpu.CompilerParams(
            collective_id=cid, has_side_effects=True, vmem_limit_bytes=grant([out], scratch)
        ),
        name="grad_reduce",
    )(x)


def gather_kernel(g, count, spots, *refs):
    k = 2 if count else 1
    xs, ws = refs[:k], picked(refs[k : k + count], spots)
    refs = refs[k + count :]
    os, fulls = refs[:k], refs[k : k + len(spots)]
    refs = refs[k + len(spots) :]
    send, recv, local = refs[:3]
    g.locate()
    entry_barrier(g, bool(count))
    rows = xs[0].shape[0] // 2
    gs = []
    for p, order in enumerate(g.orders()):
        at = pl.ds(p * rows, rows)
        slot = (lambda at: lambda i: os[0].at[i, at])(at)
        gs.append(Gather(g, order, xs[0].at[at], slot, send.at[p], recv.at[p]))
    if count:
        gs.append(Gather(g, g.orders()[0], xs[1], lambda i: os[1].at[i], send.at[2], recv.at[2]))
    for q in gs:
        q.begin()
    mine = [pltpu.make_async_copy(x, o.at[g.me], local.at[i]) for i, (x, o) in enumerate(zip(xs, os))]
    for c in mine:
        c.start()
    swap = Swap(ws, fulls, *refs[3:]) if count else None
    if count:
        swap.begin()
    run_gathers(g, gs)
    for c in mine:
        c.wait()
    if count:
        swap.end()
    for q in gs:
        q.end()


class Swap:
    def __init__(self, srcs, dsts, send, recv, load, store, *stages):
        c, f = lax.axis_index(CTX), lax.axis_index(FSDP)
        self.remote, self.loads, self.stores = [], [], []
        for i, (s, d, v) in enumerate(zip(srcs, dsts, stages)):
            self.remote.append(
                pltpu.make_async_remote_copy(
                    src_ref=s, dst_ref=d.at[f], send_sem=send.at[i], recv_sem=recv.at[i], device_id=(c, 1 - f),
                    device_id_type=MESH))
            self.loads.append(pltpu.make_async_copy(s, d.at[f] if v is None else v, load.at[i]))
            if v is not None:
                self.stores.append(pltpu.make_async_copy(v, d.at[f], store.at[i]))

    def begin(self):
        for c in self.remote + self.loads:
            c.start()
        for i, a in enumerate(self.loads):
            a.wait()
            if self.stores:
                self.stores[i].start()

    def end(self):
        for c in self.stores + self.remote:
            c.wait()

    @staticmethod
    def scratch(picks):
        return [pltpu.SemaphoreType.DMA((len(picks),))] * 4 + [pltpu.VMEM(shape_of(a, l), a.dtype) for a, l in picks]


def in_hbm(arrays):
    return [pltpu.with_memory_space_constraint(a, pltpu.HBM) for a in arrays]


def distinct(picks):
    arrays, places = [], []
    for a, l in picks:
        spot = next((i for i, b in enumerate(arrays) if b is a), None)
        if spot is None:
            spot = len(arrays)
            arrays.append(a)
        places.append((spot, l))
    return arrays, places


def picked(refs, places):
    return [refs[i] if l is None else refs[i].at[l] for i, l in places]


def shape_of(a, l):
    return a.shape if l is None else a.shape[1:]


def all_gather_ctx(x, n, cid, places=None, weights=()):
    g = Grid(n)
    arrays, spots = distinct(weights)
    count = len(arrays)
    xs = [x] if places is None else [x, places]
    dma = pltpu.SemaphoreType.DMA
    vmem, anywhere = pl.BlockSpec(memory_space=pltpu.VMEM), pl.BlockSpec(memory_space=pl.ANY)
    parts = len(xs) + 1
    scratch = [dma((parts, 2, n)), dma((parts, n)), dma((2,))] + (Swap.scratch(weights) if count else [])
    arrays_in_vmem = [(v.shape, v.dtype) for v in xs] + [((n, *v.shape), v.dtype) for v in xs]
    return pl.pallas_call(
        functools.partial(gather_kernel, g, count, spots),
        out_shape=[jax.ShapeDtypeStruct((n, *v.shape), v.dtype) for v in xs]
        + [jax.ShapeDtypeStruct((2, *shape_of(a, l)), a.dtype) for a, l in weights],
        in_specs=[vmem] * len(xs) + [pl.BlockSpec(memory_space=pltpu.HBM)] * count,
        out_specs=[vmem] * len(xs) + [anywhere] * len(weights),
        scratch_shapes=scratch,
        compiler_params=pltpu.CompilerParams(collective_id=cid, has_side_effects=True, vmem_limit_bytes=grant(arrays_in_vmem, scratch)),
        name="ctx_gather",
    )(*xs, *in_hbm(arrays))


def exchange_kernel(count, spots, *refs):
    srcs, dsts = picked(refs[:count], spots), refs[count : count + len(spots)]
    c, f = lax.axis_index(CTX), lax.axis_index(FSDP)
    sem = pltpu.get_barrier_semaphore()
    pl.semaphore_signal(sem, inc=1, device_id=(c, 1 - f), device_id_type=MESH)
    pl.semaphore_wait(sem, 1)
    swap = Swap(srcs, dsts, *refs[count + len(spots) :], *[None] * len(spots))
    swap.begin()
    swap.end()


def exchange(picks, cid):
    arrays, spots = distinct(picks)
    vmem = pl.BlockSpec(memory_space=pltpu.VMEM)
    outs = [((2, *shape_of(a, l)), a.dtype) for a, l in picks]
    return pl.pallas_call(
        functools.partial(exchange_kernel, len(arrays), spots),
        out_shape=[jax.ShapeDtypeStruct(*o) for o in outs],
        in_specs=[pl.BlockSpec(memory_space=pltpu.HBM)] * len(arrays),
        out_specs=[vmem] * len(picks),
        scratch_shapes=[pltpu.SemaphoreType.DMA((len(picks),))] * 4,
        compiler_params=pltpu.CompilerParams(collective_id=cid, has_side_effects=True, vmem_limit_bytes=grant(outs)),
        name="exchange",
    )(*in_hbm(arrays))


HEADS = 9
KV_HEADS = 3
HEAD = 64
GROUP = HEADS // KV_HEADS
EPS = 1e-05
ROPE_BASE = 100000.0
F32, BF16 = jnp.float32, jnp.bfloat16
CHUNK = 256
SLACK = 1 << 20


def nn(a, b):
    return lax.dot_general(a, b, (((1,), (0,)), ((), ())), preferred_element_type=F32)


def nt(a, b):
    return lax.dot_general(a, b, (((1,), (1,)), ((), ())), preferred_element_type=F32)


def tn(a, b):
    return lax.dot_general(a, b, (((0,), (0,)), ((), ())), preferred_element_type=F32)


def rms(v, gain):
    return v * lax.rsqrt(jnp.mean(v * v, axis=-1, keepdims=True) + EPS) * gain


def rms_back(v, gain, e):
    r = lax.rsqrt(jnp.mean(v * v, axis=-1, keepdims=True) + EPS)
    eg = e * gain
    dv = r * eg - v * (r * r * r) * jnp.mean(eg * v, axis=-1, keepdims=True)
    return dv, jnp.sum(e * v * r, axis=0, keepdims=True)


def rope(t, cos, sin):
    width = t.shape[1]
    out = []
    for lo in range(0, width, 128):
        w = min(128, width - lo)
        u = t[:, lo : lo + w]
        if w == 128:
            lane = lax.broadcasted_iota(jnp.int32, u.shape, 1) % HEAD
            other = jnp.where(lane < HEAD // 2, pltpu.roll(u, 128 - HEAD // 2, 1), pltpu.roll(u, HEAD // 2, 1))
        else:
            other = jnp.concatenate([u[:, HEAD // 2 :], u[:, : HEAD // 2]], axis=1)
        out.append((lo, w, u * cos[:, :w] + other * sin[:, :w]))
    return out


def padded(shape, dtype):
    size = jnp.dtype(dtype).itemsize
    dims = [1, 1, *shape]
    tile = 32 // size
    dims[-1], dims[-2] = -(-dims[-1] // 128) * 128, -(-dims[-2] // tile) * tile
    return size * math.prod(dims)


def grant(arrays, scratch=()):
    total = sum(padded(s, t) for s, t in arrays)
    for v in scratch:
        if getattr(v, "memory_space", None) == pltpu.VMEM:
            total += padded(v.shape, v.dtype)
    return min(total + SLACK, 62 << 20)


def call(kernel, outs, args, name, scratch=(), prefetch=0, blob=None):
    vmem = pl.BlockSpec(memory_space=pltpu.VMEM)
    smem = pl.BlockSpec(memory_space=pltpu.SMEM)
    anywhere = pl.BlockSpec(memory_space=pl.ANY)
    room = grant([(a.shape, a.dtype) for a in args[prefetch:]] + list(outs), scratch)
    if blob is not None:
        new = isinstance(blob, tuple)
        return pl.pallas_call(
            kernel,
            out_shape=[jax.ShapeDtypeStruct(s, t) for s, t in outs] + [jax.ShapeDtypeStruct(blob if new else blob.shape, BF16)],
            in_specs=[vmem] * len(args) + ([] if new else [anywhere]),
            out_specs=[vmem] * len(outs) + [anywhere],
            scratch_shapes=list(scratch),
            input_output_aliases={} if new else {len(args): len(outs)},
            compiler_params=pltpu.CompilerParams(vmem_limit_bytes=room),
            name=name,
        )(*args, *([] if new else [blob]))
    return pl.pallas_call(
        kernel,
        out_shape=[jax.ShapeDtypeStruct(s, t) for s, t in outs],
        in_specs=[smem] * prefetch + [vmem] * (len(args) - prefetch),
        out_specs=[vmem] * len(outs),
        scratch_shapes=list(scratch),
        compiler_params=pltpu.CompilerParams(vmem_limit_bytes=room),
        name=name,
    )(*args)


def gain_of(ref, l):
    return jnp.concatenate([ref[0, l : l + 1].astype(F32), ref[1, l : l + 1].astype(F32)], axis=1)


def rows_of(ref):
    return jnp.concatenate([ref[s].astype(F32).T for s in range(ref.shape[0])], axis=0)


def put_turned(ref, value):
    r = ref.shape[2]
    for s in range(ref.shape[0]):
        ref[s] = value[s * r : (s + 1) * r].T.astype(ref.dtype)


def pre_kernel(l, x_ref, gain_ref, wq_ref, wk_ref, wv_ref, cos_ref, sin_ref, a_ref, q_ref, kv_ref, *turned):
    if turned:
        x = rows_of(x_ref)
        turned[0][...] = x
    else:
        x = x_ref[...]
    a = rms(x, gain_of(gain_ref, l)).astype(BF16)
    a_ref[...] = a
    cos, sin = cos_ref[...], sin_ref[...]
    for lo, w, piece in rope(nn(a, wq_ref[...]), cos, sin):
        q_ref[:, lo : lo + w] = piece.astype(BF16)
    keys = jnp.concatenate([piece for _, _, piece in rope(nn(a, wk_ref[...]), cos, sin)], axis=1)
    kv_ref[...] = jnp.concatenate([keys, nn(a, wv_ref[...])], axis=1).astype(BF16)


def pre(l, x, gain, wq, wk, wv, cos, sin):
    m, d, e = cos.shape[0], wq.shape[0], wk.shape[1]
    outs = [((m, d), BF16), ((m, d), BF16), ((m, 2 * e), BF16)] + ([((m, d), F32)] if x.ndim == 3 else [])
    return call(functools.partial(pre_kernel, l), outs, (x, gain, wq, wk, wv, cos, sin), "pre")


def half_of(u, src, dst):
    if src != dst:
        u = pltpu.roll(u, HEAD, 1)
    lane = lax.broadcasted_iota(jnp.int32, u.shape, 1)
    return jnp.where((lane < HEAD) if dst == 0 else (lane >= HEAD), u, 0.0)


def head_chunk(ref, s, h):
    lo = (h // 2) * 128
    width = ref.shape[-1]
    if lo + 128 <= width:
        return ref[s, :, lo : lo + 128].astype(F32)
    u = ref[s, :, lo:width].astype(F32)
    return jnp.concatenate([u, jnp.zeros_like(u)], axis=1)


def pack_heads(ref, s, dst, g, half, scale):
    rows = ref.shape[1] // 2
    for i in range(GROUP):
        h = g * GROUP + i
        u = half_of(head_chunk(ref, s, h) * scale, h % 2, half).astype(BF16)
        for part in range(2):
            dst[g * 2 + part, i * rows : (i + 1) * rows, :] = u[part * rows : (part + 1) * rows]


def sort_rows(block_ref, s, src, dst, n, rows):
    def one(j, carry):
        b = block_ref[j, s, 0] // rows
        dst[pl.ds(pl.multiple_of(b * rows, rows), rows), :] = src[j, s, 0:rows, :]
        dst[pl.ds(pl.multiple_of((2 * n - 1 - b) * rows, rows), rows), :] = src[j, s, rows : 2 * rows, :]
        return carry

    lax.fori_loop(0, n, one, 0)


def visible(c, block, rows, shape):
    key = lax.broadcasted_iota(jnp.int32, shape, 0) + c * CHUNK
    query = lax.broadcasted_iota(jnp.int32, shape, 1) % rows + block * rows
    return key <= query


def key_lanes(g):
    return (g // 2) * 128, g % 2


def value_lanes(g):
    return ((KV_HEADS + g) // 2) * 128, (KV_HEADS + g) % 2


def turn_rows(src, lo, dst, count):
    def one(c, carry):
        at = pl.ds(pl.multiple_of(c * CHUNK, CHUNK), CHUNK)
        dst[:, at] = src[at, lo : lo + 256].astype(F32).T.astype(BF16)
        return carry

    lax.fori_loop(0, count, one, 0)


def attend_kernel(
    n, block_ref, mine_ref, q_ref, kv_ref, o_ref, lse_ref, sorted_ref, turned_ref, qp_ref, st_ref, acc_ref, stat_ref
):
    rows = q_ref.shape[1] // 2
    wide = GROUP * rows
    groups = range(KV_HEADS)
    vlo = HEAD * KV_HEADS // 128 * 128
    voff = HEAD * KV_HEADS - vlo

    def sequence(s, carry):
        sort_rows(block_ref, s, kv_ref, sorted_ref, n, rows)
        turn_rows(sorted_ref, vlo, turned_ref, n * 2 * rows // CHUNK)
        for g in groups:
            pack_heads(q_ref, s, qp_ref, g, key_lanes(g)[1], HEAD**-0.5)
        low = mine_ref[s, 0] // rows
        for part in range(2):
            block = low if part == 0 else 2 * n - 1 - low
            last = block * rows // CHUNK
            stat_ref[...] = jnp.full_like(stat_ref, -1e30)

            def score(c, masked):
                at = pl.ds(pl.multiple_of(c * CHUNK, CHUNK), CHUNK)
                for g in groups:
                    klo, _ = key_lanes(g)
                    st = nt(sorted_ref[at, klo : klo + 128], qp_ref[g * 2 + part])
                    if masked:
                        st = jnp.where(visible(c, block, rows, st.shape), st, -1e30)
                    st_ref[g, at, :] = st
                    stat_ref[g] = jnp.maximum(stat_ref[g], jnp.max(st.reshape(CHUNK // 8, 8, wide), axis=0))

            def scores(c, carry):
                score(c, False)
                return carry

            lax.fori_loop(0, last, scores, 0)
            score(last, True)
            tops = [jnp.max(stat_ref[g], axis=0, keepdims=True) for g in groups]
            stat_ref[...] = jnp.zeros_like(stat_ref)
            acc_ref[...] = jnp.zeros_like(acc_ref)

            def mix(c, tops):
                at = pl.ds(pl.multiple_of(c * CHUNK, CHUNK), CHUNK)
                for g in groups:
                    p = jnp.exp(st_ref[g, at, :] - tops[g])
                    stat_ref[g] += jnp.sum(p.reshape(CHUNK // 8, 8, wide), axis=0)
                    acc_ref[g] += nn(turned_ref[voff + g * HEAD : voff + (g + 1) * HEAD, at], p.astype(BF16))
                return tops

            tops = lax.fori_loop(0, last + 1, mix, tuple(tops))
            for g in groups:
                total = jnp.sum(stat_ref[g], axis=0, keepdims=True)
                lse_ref[s, g * 2 + part] = tops[g] + jnp.log(total)
                out = (acc_ref[g] / total).T
                for i in range(GROUP):
                    h = g * GROUP + i
                    o_ref[s, part * rows : (part + 1) * rows, h * HEAD : (h + 1) * HEAD] = out[i * rows : (i + 1) * rows]
        return carry

    lax.fori_loop(0, q_ref.shape[0], sequence, 0)


def attend(blocks, mine, q, kv):
    seqs, r, d = q.shape
    n = kv.shape[0]
    wide = GROUP * r // 2
    scratch = [
        pltpu.VMEM((n * r, kv.shape[-1]), BF16),
        pltpu.VMEM((256, n * r), BF16),
        pltpu.VMEM((2 * KV_HEADS, wide, 128), BF16),
        pltpu.VMEM((KV_HEADS, n * r, wide), F32),
        pltpu.VMEM((KV_HEADS, HEAD, wide), F32),
        pltpu.VMEM((KV_HEADS, 8, wide), F32),
    ]
    outs = [((seqs, r, d), F32), ((seqs, 2 * KV_HEADS, 1, wide), F32)]
    return call(functools.partial(attend_kernel, n), outs, (blocks, mine, q, kv), "attend", scratch, 2)


def attend_back_kernel(
    n, block_ref, mine_ref, q_ref, kv_ref, do_ref, o_ref, lse_ref, dq_ref, dkv_ref,
    sorted_ref, turned_ref, qp_ref, dop_ref, acc_ref, delta_ref, dqt_ref,
):
    rows = q_ref.shape[1] // 2
    wide = GROUP * rows
    groups = range(KV_HEADS)

    def sequence(s, carry):
        sort_rows(block_ref, s, kv_ref, sorted_ref, n, rows)
        turn_rows(sorted_ref, 0, turned_ref, n * 2 * rows // CHUNK)
        for g in groups:
            pack_heads(q_ref, s, qp_ref, g, key_lanes(g)[1], HEAD**-0.5)
            pack_heads(do_ref, s, dop_ref, g, value_lanes(g)[1], 1.0)
        acc_ref[...] = jnp.zeros_like(acc_ref)
        low = mine_ref[s, 0] // rows
        for part in range(2):
            block = low if part == 0 else 2 * n - 1 - low
            last = block * rows // CHUNK
            deltas = []
            for g in groups:
                sums = []
                for i in range(GROUP):
                    h = g * GROUP + i
                    lanes = slice(h * HEAD, (h + 1) * HEAD)
                    at = slice(part * rows, (part + 1) * rows)
                    both = do_ref[s, at, lanes].astype(F32) * o_ref[s, at, lanes]
                    sums.append(jnp.sum(both, axis=1, keepdims=True))
                delta_ref[...] = jnp.concatenate(sums, axis=0) + jnp.zeros((wide, 128), F32)
                deltas.append(delta_ref[...].T[0:1])
            dqt_ref[...] = jnp.zeros_like(dqt_ref)

            def step(c, deltas, masked):
                at = pl.ds(pl.multiple_of(c * CHUNK, CHUNK), CHUNK)
                sums = [None] * (2 * KV_HEADS * HEAD // 128)
                for g in groups:
                    klo, _ = key_lanes(g)
                    vlo, _ = value_lanes(g)
                    qp, dop = qp_ref[g * 2 + part], dop_ref[g * 2 + part]
                    p = jnp.exp(nt(sorted_ref[at, klo : klo + 128], qp) - lse_ref[s, g * 2 + part])
                    if masked:
                        p = jnp.where(visible(c, block, rows, p.shape), p, 0.0)
                    dp = nt(sorted_ref[at, vlo : vlo + 128], dop)
                    ds = (p * (dp - deltas[g])).astype(BF16)
                    for lo, v in ((vlo // 128, nn(p.astype(BF16), dop)), (klo // 128, nn(ds, qp))):
                        sums[lo] = v if sums[lo] is None else sums[lo] + v
                    dqt_ref[g] += nn(turned_ref[g * HEAD : (g + 1) * HEAD, at], ds)
                for k, v in enumerate(sums):
                    acc_ref[at, k * 128 : (k + 1) * 128] += v
                return deltas

            deltas = lax.fori_loop(0, last, lambda c, t: step(c, t, False), tuple(deltas))
            step(last, deltas, True)
            for g in groups:
                dq = dqt_ref[g].T * HEAD**-0.5
                for i in range(GROUP):
                    h = g * GROUP + i
                    dq_ref[s, part * rows : (part + 1) * rows, h * HEAD : (h + 1) * HEAD] = dq[i * rows : (i + 1) * rows]

        def one(j, carry):
            b = block_ref[j, s, 0] // rows
            dkv_ref[j, s, 0:rows, :] = acc_ref[pl.ds(pl.multiple_of(b * rows, rows), rows), :].astype(BF16)
            dkv_ref[j, s, rows : 2 * rows, :] = acc_ref[
                pl.ds(pl.multiple_of((2 * n - 1 - b) * rows, rows), rows), :
            ].astype(BF16)
            return carry

        lax.fori_loop(0, n, one, 0)
        return carry

    lax.fori_loop(0, q_ref.shape[0], sequence, 0)


def attend_back(blocks, mine, q, kv, do, o, lse):
    seqs, r, d = q.shape
    n = kv.shape[0]
    wide = GROUP * r // 2
    scratch = [
        pltpu.VMEM((n * r, kv.shape[-1]), BF16),
        pltpu.VMEM((256, n * r), BF16),
        pltpu.VMEM((2 * KV_HEADS, wide, 128), BF16),
        pltpu.VMEM((2 * KV_HEADS, wide, 128), BF16),
        pltpu.VMEM((n * r, kv.shape[-1]), F32),
        pltpu.VMEM((wide, 128), F32),
        pltpu.VMEM((KV_HEADS, HEAD, wide), F32),
    ]
    outs = [((seqs, r, d), F32), (kv.shape, BF16)]
    args = (blocks, mine, q, kv, do, o, lse)
    return call(functools.partial(attend_back_kernel, n), outs, args, "attend_back", scratch, 2)


def down_at(wd_ref, i):
    per = wd_ref.shape[2] // CHUNK
    f = i // per
    return f, pl.ds(pl.multiple_of((i - f * per) * CHUNK, CHUNK), CHUNK)


def post_kernel(l, o_ref, x_ref, wo_ref, gain_ref, wg_ref, wu_ref, wd_ref, h_ref, b_ref, gate_ref, up_ref, y_ref, *turned):
    sum_ref = turned[0] if turned else y_ref
    h = x_ref[...] + nn(o_ref[...].astype(BF16), wo_ref[...])
    h_ref[...] = h
    sum_ref[...] = h
    b_ref[...] = rms(h, gain_of(gain_ref, l)).astype(BF16)

    def some(i, carry):
        at = pl.ds(pl.multiple_of(i * CHUNK, CHUNK), CHUNK)
        b = b_ref[...]
        gate, up = nn(b, wg_ref[:, at]), nn(b, wu_ref[:, at])
        gate_ref[:, at], up_ref[:, at] = gate, up
        m = (gate * jax.nn.sigmoid(gate) * up).astype(BF16)
        f, spot = down_at(wd_ref, i)
        sum_ref[...] += nt(m, wd_ref[f, :, spot])
        return carry

    lax.fori_loop(0, wg_ref.shape[1] // CHUNK, some, 0)
    if turned:
        put_turned(y_ref, sum_ref[...])


def post(l, o, x, wo, gain, wg, wu, wd, turned=None):
    m, d = x.shape
    ff = wg.shape[1]
    outs = [((m, d), F32), ((m, d), BF16), ((m, ff), F32), ((m, ff), F32), (turned, BF16) if turned else ((m, d), F32)]
    scratch = [pltpu.VMEM((m, d), F32)] if turned else []
    return call(functools.partial(post_kernel, l), outs, (o, x, wo, gain, wg, wu, wd), "post", scratch)


def put_tiles(blob, base, value, count):
    rows = value.shape[0] // 2
    if value.shape[1] < count * 128:
        value = jnp.concatenate([value, jnp.zeros((2 * rows, count * 128 - value.shape[1]), value.dtype)], axis=1)
    for f in range(2):
        for j in range(count):
            piece = value[f * rows : (f + 1) * rows, j * 128 : (j + 1) * 128]
            blob[f, pl.ds(base + j * (rows // 16), rows // 16)] = piece.reshape(rows // 16, 16, 128)


def put_norm(blob, at, dg):
    half = dg.shape[1] // 2
    for f in range(2):
        v = dg[:, f * half : (f + 1) * half]
        v = jnp.concatenate([v, jnp.zeros((1, 384 - half), F32)], axis=1)
        rows = jnp.concatenate([v[:, 0:128], v[:, 128:256], v[:, 256:384], jnp.zeros((13, 128), F32)], axis=0)
        blob[f, at] = rows.astype(BF16)


def wide_of(cols):
    return -(-cols // 128)


def ffn_back_kernel(l, base, new, *refs):
    dy_ref, h_ref, b_ref, gate_ref, up_ref, o_ref, gain_ref, wo_ref, wg_ref, wu_ref, wd_ref = refs[:11]
    dh_ref, do_ref, out_ref, blob_ref, dyb_ref, dyt_ref, db_ref, bt_ref, sem = refs[11 if new else 12 :]
    m, d = h_ref.shape
    ff = wg_ref.shape[1]
    half = d // 2 // 16
    up_at = (ff // 128) * half
    low_at = 2 * up_at
    out_at = low_at + (ff // 256) * (d // 16)
    norm_at = out_at + wide_of(d) * half
    dy = rows_of(dy_ref) if len(dy_ref.shape) == 3 else dy_ref[...]
    dh_ref[...] = dy
    dyb_ref[...] = dy.astype(BF16)
    dyt_ref[...] = dyb_ref[...].T
    db_ref[...] = jnp.zeros_like(db_ref)
    bt_ref[...] = b_ref[...].T

    def some(i, carry):
        at = pl.ds(pl.multiple_of(i * CHUNK, CHUNK), CHUNK)
        f, spot = down_at(wd_ref, i)
        dm = nn(dyb_ref[...], wd_ref[f, :, spot])
        gate, up = gate_ref[:, at], up_ref[:, at]
        sig = jax.nn.sigmoid(gate)
        silu = gate * sig
        mid = (silu * up).astype(BF16)
        dgate = (dm * up * sig * (1.0 + gate * (1.0 - sig))).astype(BF16)
        dup = (dm * silu).astype(BF16)
        db_ref[...] += nt(dgate, wg_ref[:, at]) + nt(dup, wu_ref[:, at])
        bt = bt_ref[...]
        put_tiles(blob_ref, i * (CHUNK // 128) * half, nn(bt, dgate).astype(BF16), CHUNK // 128)
        put_tiles(blob_ref, up_at + i * (CHUNK // 128) * half, nn(bt, dup).astype(BF16), CHUNK // 128)
        gd = nn(dyt_ref[...], mid).astype(BF16)
        per = wd_ref.shape[2] // CHUNK
        for j in range(CHUNK // 128):
            start = low_at + ((i - f * per) * (CHUNK // 128) + j) * (d // 16)
            blob_ref[f, pl.ds(start, d // 16)] = gd[:, j * 128 : (j + 1) * 128].reshape(d // 16, 16, 128)
        return carry

    lax.fori_loop(0, ff // CHUNK, some, 0)
    first = pltpu.make_async_copy(blob_ref.at[:, pl.ds(0, out_at)], out_ref.at[:, pl.ds(base, out_at)], sem.at[0])
    first.start()
    dv, dg = rms_back(h_ref[...], gain_of(gain_ref, l), db_ref[...])
    dh = dh_ref[...] + dv
    dh_ref[...] = dh
    dhb = dh.astype(BF16)
    do_ref[...] = nt(dhb, wo_ref[...]).astype(BF16)
    put_tiles(blob_ref, out_at, tn(o_ref[...].astype(BF16), dhb).astype(BF16), wide_of(d))
    put_norm(blob_ref, norm_at, dg)
    rest = norm_at + 1 - out_at
    second = pltpu.make_async_copy(
        blob_ref.at[:, pl.ds(out_at, rest)], out_ref.at[:, pl.ds(base + out_at, rest)], sem.at[1]
    )
    second.start()
    first.wait()
    second.wait()


def ffn_tiles(d, ff):
    return 2 * (ff // 128) * (d // 32) + (ff // 256) * (d // 16) + wide_of(d) * (d // 32) + 1


def ffn_back(l, blob, base, dy, h, b, gate, up, o, gain, wo, wg, wu, wd):
    m, d = h.shape
    ff = wg.shape[1]
    scratch = [
        pltpu.VMEM((2, ffn_tiles(d, ff), 16, 128), BF16),
        pltpu.VMEM((m, d), BF16),
        pltpu.VMEM((d, m), BF16),
        pltpu.VMEM((m, d), F32),
        pltpu.VMEM((d, m), BF16),
        pltpu.SemaphoreType.DMA((2,)),
    ]
    kernel = functools.partial(ffn_back_kernel, l, base, isinstance(blob, tuple))
    args = (dy, h, b, gate, up, o, gain, wo, wg, wu, wd)
    return call(kernel, [((m, d), F32), ((m, d), BF16)], args, "ffn_back", scratch, blob=blob)


def pre_tiles(d, e):
    return wide_of(d) * (d // 32) + wide_of(2 * e) * (d // 32) + 1


def pre_back_kernel(l, base, *refs):
    dq_ref, dkv_ref, a_ref, x_ref, dh_ref, gain_ref, wq_ref, wk_ref, wv_ref, cos_ref, sin_ref = refs[:11]
    dx_ref, out_ref, blob_ref, dqp_ref, sem = refs[12:]
    d = x_ref.shape[1]
    e = wk_ref.shape[1]
    half = d // 2 // 16
    cos, sin = cos_ref[...], -sin_ref[...]
    for lo, w, piece in rope(dq_ref[...], cos, sin):
        dqp_ref[:, lo : lo + w] = piece.astype(BF16)
    dqp = dqp_ref[...]
    dkv = dkv_ref[...]
    dkp = jnp.concatenate([piece for _, _, piece in rope(dkv[:, :e], cos, sin)], axis=1).astype(BF16)
    dvr = dkv[:, e:].astype(BF16)
    da = nt(dqp, wq_ref[...]) + nt(dkp, wk_ref[...]) + nt(dvr, wv_ref[...])
    dv, dg = rms_back(x_ref[...], gain_of(gain_ref, l), da)
    kv_at = wide_of(d) * half
    norm_at = kv_at + wide_of(2 * e) * half
    put_norm(blob_ref, norm_at, dg)
    left = blob_ref.shape[1] - norm_at - 1
    if left:
        blob_ref[:, pl.ds(norm_at + 1, left)] = jnp.zeros((2, left, 16, 128), BF16)
    at = a_ref[...].T
    put_tiles(blob_ref, 0, nn(at, dqp).astype(BF16), wide_of(d))
    put_tiles(blob_ref, kv_at, jnp.concatenate([nn(at, dkp), nn(at, dvr)], axis=1).astype(BF16), wide_of(2 * e))
    done = pltpu.make_async_copy(blob_ref, out_ref.at[:, pl.ds(base, blob_ref.shape[1])], sem)
    done.start()
    if len(dx_ref.shape) == 3:
        put_turned(dx_ref, dh_ref[...] + dv)
    else:
        dx_ref[...] = dh_ref[...] + dv
    done.wait()


def pre_back(l, shape, blob, base, tiles, dq, dkv, a, x, dh, gain, wq, wk, wv, cos, sin):
    m, d = x.shape
    scratch = [pltpu.VMEM((2, tiles, 16, 128), BF16), pltpu.VMEM((m, d), BF16), pltpu.SemaphoreType.DMA(())]
    args = (dq, dkv, a, x, dh, gain, wq, wk, wv, cos, sin)
    return call(functools.partial(pre_back_kernel, l, base), [(shape, F32)], args, "pre_back", scratch, blob=blob)


def unpack_kernel(places, blob, *outs):
    g_attn, gq, gk, gv, go, g_ffn, gg, gu, gd = outs
    half, d, e, ff = gq.shape[1], gq.shape[2], gk.shape[2], gg.shape[2]
    t = half // 16

    def take(base, at, rows, cols, out, l, skip=0):
        for lo in range(0, cols, 128):
            w = min(128, cols - lo)
            j = (skip + lo) // 128
            if (skip + lo) % 128 == 0:
                u = blob[pl.ds(base + at + j * (rows // 16), rows // 16)].reshape(rows, 128)[:, :w]
            else:
                u = blob[pl.ds(base + at + j * (rows // 16), rows // 16)].reshape(rows, 128)[:, 64:]
                if w > 64:
                    v = blob[pl.ds(base + at + (j + 1) * (rows // 16), rows // 16)].reshape(rows, 128)[:, : w - 64]
                    u = jnp.concatenate([u.astype(F32), v.astype(F32)], axis=1)
            out[l, :, lo : lo + w] = u.astype(F32)

    def norm(base, at, out, l):
        u = blob[base + at].astype(F32)
        row = jnp.concatenate([u[0:1], u[1:2], u[2:3]], axis=1)
        out[l : l + 1, :] = row[:, :half]

    for l, (ffn, att) in enumerate(places):
        up_at = (ff // 128) * t
        low_at = 2 * up_at
        out_at = low_at + (ff // 256) * (d // 16)
        take(ffn, 0, half, ff, gg, l)
        take(ffn, up_at, half, ff, gu, l)
        take(ffn, low_at, d, ff // 2, gd, l)
        take(ffn, out_at, half, d, go, l)
        norm(ffn, out_at + wide_of(d) * t, g_ffn, l)
        take(att, 0, half, d, gq, l)
        kv_at = wide_of(d) * t
        take(att, kv_at, half, e, gk, l)
        take(att, kv_at, half, e, gv, l, e)
        norm(att, kv_at + wide_of(2 * e) * t, g_attn, l)


def unpack(blob, places, shapes):
    return call(functools.partial(unpack_kernel, places), [(s, F32) for s in shapes], (blob,), "unpack")


def body(tokens, positions, norm_attn, w_query, w_key, w_value, w_out, norm_ffn, w_gate, w_up, w_down, cotangent):
    layers = norm_attn.shape[0]
    n = lax.axis_size(CTX)
    seqs, r, d = tokens.shape
    m = seqs * r
    e, ff = w_key.shape[2], w_gate.shape[2]
    own = (w_query, w_key, w_value, w_out, w_gate, w_up, jnp.swapaxes(w_down, 1, 2))
    shards = [(w, l) for l in range(layers) for w in own]
    full = exchange([(norm_attn, None), (norm_ffn, None), *shards[:3]], 0)
    gain_attn, gain_ffn, *full = full
    frequency = jnp.exp(jnp.arange(HEAD // 2, dtype=F32) * (-jnp.log(ROPE_BASE) / (HEAD // 2)))
    angles = positions.reshape(m, 1).astype(F32) * frequency
    cos, sin = jnp.cos(angles), jnp.sin(angles)
    cos = jnp.concatenate([cos] * 4, axis=1)
    sin = jnp.concatenate([-sin, sin] * 2, axis=1)
    x = jnp.swapaxes(tokens, 1, 2)
    kept = []
    weights = []

    def joined(w):
        return w.reshape(2 * w.shape[1], w.shape[2])

    for l in range(layers):
        wq, wk, wv = (joined(w) for w in full[l * len(own) : l * len(own) + 3])
        a, q, kv, *turned = pre(l, x, gain_attn, wq, wk, wv, cos, sin)
        if turned:
            (x,) = turned
        q = q.reshape(seqs, r, d)
        if l == 0:
            kv, places, *rest = all_gather_ctx(kv, n, 1, positions, shards[3:])
            full = [*full, *rest]
        else:
            (kv,) = all_gather_ctx(kv, n, 1 + l)
        wo, wg, wu = (joined(w) for w in full[l * len(own) + 3 : l * len(own) + 6])
        wd = full[l * len(own) + 6]
        weights.append((wq, wk, wv, wo, wg, wu, wd))
        kv = kv.reshape(n, seqs, r, 2 * e)
        o, lse = attend(places, positions, q, kv)
        turned = (seqs, d, r) if l == layers - 1 else None
        h, b, gate, up, y = post(l, o.reshape(m, d), x, wo, gain_ffn, wg, wu, wd, turned)
        kept.append((x, a, q, kv, o, lse, h, b, gate, up))
        x = y
    output = jnp.swapaxes(x, 1, 2)
    dy = jnp.swapaxes(cotangent, 1, 2)
    one, two = ffn_tiles(d, ff), pre_tiles(d, e)
    unit = 2 * n
    whole = -(-layers * (one + two) // unit) * unit
    blob = (2, whole, 16, 128)
    spots = []
    for l in reversed(range(layers)):
        wq, wk, wv, wo, wg, wu, wd = weights[l]
        x, a, q, kv, o, lse, h, b, gate, up = kept[l]
        start = (layers - 1 - l) * (one + two)
        spots.insert(0, (start, start + one))
        dh, do, blob = ffn_back(l, blob, start, dy, h, b, gate, up, o.reshape(m, d), gain_ffn, wo, wg, wu, wd)
        dq, dkv = attend_back(places, positions, q, kv, do.reshape(seqs, r, d), o, lse)
        dkv = reduce_scatter_ctx(dkv.reshape(n, m, 2 * e), n, 1 + layers + l)
        tiles = two if l else whole - start - one
        shape = (m, d) if l else (seqs, d, r)
        dy, blob = pre_back(
            l, shape, blob, start + one, tiles, dq.reshape(m, d), dkv, a, x, dh, gain_attn, wq, wk, wv, cos, sin
        )
    total = reduce_all(blob.reshape(2, n, -1, 128), n, 1 + 2 * layers)
    shapes = [norm_attn.shape, *[w.shape for w in own[:4]], norm_ffn.shape, *[w.shape for w in own[4:]]]
    grads = unpack(total.reshape(whole, 16, 128), spots, shapes)
    return (output, jnp.swapaxes(dy, 1, 2), *grads[:-1], jnp.swapaxes(grads[-1], 1, 2))


def solution(mesh):
    in_specs = (
        P("fsdp", "ctx", None),
        P("fsdp", "ctx"),
        P(None, "fsdp"),
        P(None, "fsdp", None),
        P(None, "fsdp", None),
        P(None, "fsdp", None),
        P(None, "fsdp", None),
        P(None, "fsdp"),
        P(None, "fsdp", None),
        P(None, "fsdp", None),
        P(None, "fsdp", None),
        P("fsdp", "ctx", None),
    )
    out_specs = (
        P("fsdp", "ctx", None),
        P("fsdp", "ctx", None),
        P(None, "fsdp"),
        P(None, "fsdp", None),
        P(None, "fsdp", None),
        P(None, "fsdp", None),
        P(None, "fsdp", None),
        P(None, "fsdp"),
        P(None, "fsdp", None),
        P(None, "fsdp", None),
        P(None, "fsdp", None),
    )
    return jax.shard_map(body, mesh=mesh, in_specs=in_specs, out_specs=out_specs, check_vma=False)
```

```python
import functools
import itertools
import math

import jax
import jax.numpy as jnp
from jax import lax
from jax.experimental import pallas as pl
from jax.experimental.pallas import tpu as pltpu
from jax.sharding import PartitionSpec as P

CTX, FSDP = "ctx", "fsdp"
MESH = pl.DeviceIdType.MESH
SHARES = ((0, 6), (1, 6), (2, 2), (3, 2))
SUM_SHARES = ((0, 6), (1, 6), (2, 2), (3, 2))


def factors(n):
    known = {16: (4, 2, 2), 64: (2, 4, 4, 2)}
    if n in known:
        return known[n]
    out, p = [], 2
    while n > 1:
        while n % p == 0:
            out.append(p)
            n //= p
        p += 1
    return tuple(out) or (1,)


class Grid:
    def __init__(self, n):
        self.n = n
        self.dims = factors(n)
        strides, s = [], 1
        for d in reversed(self.dims):
            strides.insert(0, s)
            s *= d
        self.strides = tuple(strides)
        self.all = list(itertools.product(*[range(d) for d in self.dims]))
        self.ident = {d: i for i, d in enumerate(self.all)}

    def locate(self):
        me = lax.axis_index(CTX)
        self.me = me
        self.at = [lax.rem(me // s, d) for s, d in zip(self.strides, self.dims)]

    def index(self, delta):
        out = 0
        for c, d, n, s in zip(self.at, delta, self.dims, self.strides):
            out = out + (c if isinstance(d, int) and d == 0 else lax.rem(c + d, n)) * s
        return out

    def slot(self, delta):
        return sum(d * s for d, s in zip(delta, self.strides))

    def peer(self, axis, j):
        return self.index(tuple(j if a == axis else 0 for a in range(len(self.dims))))

    def orders(self):
        rest = list(range(1, len(self.dims)))
        return [[0] + rest, [0] + rest[::-1]]


def put(x, d, a):
    return tuple(x if i == a else v for i, v in enumerate(d))


def entry_barrier(g, fsdp):
    sem = pltpu.get_barrier_semaphore()
    count = 0
    f = lax.axis_index(FSDP)
    for a, d in enumerate(g.dims):
        for j in range(1, d):
            pl.semaphore_signal(sem, inc=1, device_id=(g.peer(a, j), f), device_id_type=MESH)
            count += 1
    if fsdp:
        pl.semaphore_signal(sem, inc=1, device_id=(g.me, 1 - f), device_id_type=MESH)
        count += 1
    pl.semaphore_wait(sem, count)


class Gather:
    def __init__(self, g, order, own, slot, send, recv):
        self.g, self.order, self.own, self.slot, self.send, self.recv = g, order, own, slot, send, recv
        self.sent = []

    def copy(self, src, index, axis, step, label, way):
        g = self.g
        i = g.slot(label)
        return pltpu.make_async_remote_copy(
            src_ref=src, dst_ref=self.slot(index), send_sem=self.send.at[way, i], recv_sem=self.recv.at[i],
            device_id=(g.peer(axis, step % g.dims[axis]), lax.axis_index(FSDP)), device_id_type=MESH)

    def start(self, copy, cond):
        self.sent.append((copy, cond))
        if cond is None:
            copy.start()
        else:
            pl.when(cond)(copy.start)

    def spread(self, delta, stage, src):
        g = self.g
        index = g.index(delta)
        for a in self.order[stage:]:
            n, c = g.dims[a], g.at[a]
            if n > 2:
                self.start(self.copy(src, index, a, 1, put(n - 1, delta, a), 0), c < n - 1)
                self.start(self.copy(src, index, a, -1, put(1, delta, a), 1), c > 0)
            else:
                for j in range(1, n):
                    self.start(self.copy(src, index, a, j, put(n - j, delta, a), 0), None)

    def begin(self):
        self.spread((0,) * len(self.g.dims), 0, self.own)

    def labels(self, stage):
        g, a = self.g, self.order[stage]
        n = g.dims[a]
        before = [range(g.dims[i]) if i in self.order[:stage] else range(1) for i in range(len(g.dims))]
        out = []
        if n > 2:
            c = g.at[a]
            near = [sorted((s for s in range(n) if s != k), key=lambda s: abs(s - k)) for k in range(n)]
            steps = []
            for t in range(n - 1):
                v = (near[0][t]) % n
                for k in range(1, n):
                    v = jnp.where(c == k, (near[k][t] - k) % n, v)
                steps.append(v)
        else:
            steps = list(range(1, n))
        for s in steps:
            for d in itertools.product(*before):
                out.append(put(s, d, a))
        return out

    def arrive(self, label, stage):
        g, a = self.g, self.order[stage]
        n, c = g.dims[a], g.at[a]
        index = g.index(label)
        here = self.slot(index)
        pltpu.make_async_remote_copy(
            src_ref=here, dst_ref=here, send_sem=self.send.at[0, 0], recv_sem=self.recv.at[g.slot(label)],
            device_id=(g.peer(a, 1), lax.axis_index(FSDP)), device_id_type=MESH).wait_recv()
        if n > 2:
            k = label[a]
            below = c + k >= n
            up = jnp.logical_and(below, c < n - 1)
            down = jnp.logical_and(jnp.logical_not(below), c > 0)
            self.start(self.copy(here, index, a, 1, put(k - 1, label, a), 0), up)
            self.start(self.copy(here, index, a, -1, put(k + 1, label, a), 1), down)
        self.spread(label, stage + 1, here)

    def end(self):
        for copy, cond in self.sent:
            if cond is None:
                copy.wait_send()
            else:
                pl.when(cond)(copy.wait_send)


def run_gathers(g, gs):
    courses = [[(q, d, stage) for stage in range(len(g.dims)) for d in q.labels(stage)] for q in gs]
    for q, d, stage in interleave(courses):
        q.arrive(d, stage)


def interleave(lists):
    for i in range(max(map(len, lists))):
        for l in lists:
            if i < len(l):
                yield l[i]


def add_into(out, refs):
    rows = out.shape[0]
    step = max(s for s in range(16, 129, 16) if rows % s == 0)

    def some(i, carry):
        at = pl.ds(pl.multiple_of(i * step, step), step)
        out[at] = sum(r[at].astype(jnp.float32) for r in refs).astype(out.dtype)
        return carry

    lax.fori_loop(0, rows // step, some, 0)


def chosen(table, c):
    v = table[0]
    for k in range(1, len(table)):
        v = jnp.where(c == k, table[k], v)
    return v


class Reduce:
    def __init__(self, g, order, own, acc, land, send, recv):
        self.g, self.order, self.own, self.acc, self.land, self.send, self.recv = g, order, own, acc, land, send, recv
        self.sent = []

    @staticmethod
    def room(g, order):
        starts, total = [], 0
        for stage, a in enumerate(order):
            live = math.prod(g.dims[b] for b in order[stage:])
            starts.append(total)
            total += live // 2 if g.dims[a] == 2 else 2 * live
        return starts, total

    def spot(self, stage, way, label):
        g, a = self.g, self.order[stage]
        axes = self.order[stage + 1 :] if g.dims[a] == 2 else self.order[stage:]
        rank, live = 0, 1
        for b in axes:
            rank = rank + label[b] * live
            live *= g.dims[b]
        return self.room(g, self.order)[0][stage] + way * live + rank

    def ship(self, src, label, stage, step, way, at_label):
        g, axis = self.g, self.order[stage]
        spot = self.spot(stage, way, at_label)
        copy = pltpu.make_async_remote_copy(
            src_ref=src, dst_ref=self.land.at[spot], send_sem=self.send.at[g.slot(label)], recv_sem=self.recv.at[spot],
            device_id=(g.peer(axis, step), lax.axis_index(FSDP)), device_id_type=MESH)
        copy.start()
        self.sent.append(copy)

    def landed(self, stage, way, label):
        g = self.g
        spot = self.spot(stage, way, label)
        ref = self.land.at[spot]
        pltpu.make_async_remote_copy(
            src_ref=ref, dst_ref=ref, send_sem=self.send.at[0], recv_sem=self.recv.at[spot],
            device_id=(g.peer(self.order[0], 1), lax.axis_index(FSDP)), device_id_type=MESH).wait_recv()
        return ref

    def labels(self, stage):
        gone = self.order[:stage]
        ranges = [range(1) if i in gone else range(n) for i, n in enumerate(self.g.dims)]
        far = lambda d: -sum(1 for i in self.order[stage:] if d[i])
        return sorted(itertools.product(*ranges), key=far)

    def steps(self, stage):
        g, a = self.g, self.order[stage]
        n, c = g.dims[a], g.at[a]
        keep = [d for d in self.labels(stage) if d[a] == 0]
        out = []
        if n == 2:
            if stage == 0:
                out += [functools.partial(self.swap, put(1, d, a)) for d in keep]
            out += [functools.partial(self.take, d, stage) for d in keep]
        else:
            if stage == 0:
                out.append(self.copy_all)
            far = [sorted((k for k in range(1, n)), key=lambda k: -abs((p + k) % n - p)) for p in range(n)]
            for t in range(n - 1):
                k = chosen([far[p][t] for p in range(n)], c)
                out += [functools.partial(self.pass_on, put(k, d, a), stage) for d in keep]
            out += [functools.partial(self.close, d, stage) for d in keep]
        return out

    def course(self):
        return [step for stage in range(len(self.order)) for step in self.steps(stage)]

    def copy_all(self):
        for d in self.g.all:
            i = self.g.index(d)
            add_into(self.acc(i), [self.own(i)])

    def swap(self, d):
        self.ship(self.own(self.g.index(d)), d, 0, 1, 0, d)

    def next_ship(self, d, stage):
        if stage + 1 < len(self.order):
            a = self.order[stage + 1]
            if self.g.dims[a] == 2 and d[a]:
                self.ship(self.acc(self.g.index(d)), d, stage + 1, 1, 0, d)

    def take(self, d, stage):
        a = self.order[stage]
        i = self.g.index(d)
        ref = self.own(i) if stage == 0 else self.acc(i)
        add_into(self.acc(i), [ref, self.landed(stage, 0, put(1, d, a))])
        self.next_ship(d, stage)

    def pass_on(self, d, stage):
        g, a = self.g, self.order[stage]
        n, c = g.dims[a], g.at[a]
        k = d[a]
        up = c + k < n
        way = jnp.where(up, 0, 1)
        kept = self.acc(g.index(d))

        @pl.when(jnp.where(up, c > 0, c < n - 1))
        def _():
            add_into(kept, [kept, self.landed(stage, way, d)])

        self.ship(kept, d, stage, jnp.where(up, 1, n - 1), way, put(jnp.where(up, k - 1, lax.rem(k + 1, n)), d, a))

    def close(self, d, stage):
        g, a = self.g, self.order[stage]
        n, c = g.dims[a], g.at[a]
        kept = self.acc(g.index(d))

        @pl.when(c > 0)
        def _():
            add_into(kept, [kept, self.landed(stage, 0, d)])

        @pl.when(c < n - 1)
        def _():
            add_into(kept, [kept, self.landed(stage, 1, d)])

        self.next_ship(d, stage)

    def end(self):
        for copy in self.sent:
            copy.wait_send()


def scatter_kernel(g, x_ref, o_ref, acc, send, recv, *lands):
    g.locate()
    entry_barrier(g, False)
    rs = []
    for p, (r0, rn, order) in enumerate(reduce_parts(g, x_ref.shape[1], SUM_SHARES)):
        at = pl.ds(r0, rn)
        own = (lambda at: lambda i: x_ref.at[i, at])(at)
        kept = (lambda at: lambda i: acc.at[i, at])(at)
        rs.append(Reduce(g, order[::-1], own, kept, lands[p], send.at[p], recv.at[p]))
    for step in interleave([r.course() for r in rs]):
        step()
    o_ref[...] = acc[g.me].astype(jnp.float32)
    for r in rs:
        r.end()


def reduce_scatter_ctx(x, n, cid):
    g = Grid(n)
    _, rows, cols = x.shape
    cuts = reduce_parts(g, rows, SUM_SHARES)
    rooms = [Reduce.room(g, order[::-1])[1] for _, _, order in cuts]
    dma = pltpu.SemaphoreType.DMA
    scratch = [pltpu.VMEM((n, rows, cols), x.dtype), dma((len(cuts), n)), dma((len(cuts), max(rooms)))]
    scratch += [pltpu.VMEM((room, rn, cols), x.dtype) for room, (_, rn, _) in zip(rooms, cuts)]
    out = ((rows, cols), jnp.float32)
    return pl.pallas_call(
        functools.partial(scatter_kernel, g),
        out_shape=jax.ShapeDtypeStruct(*out),
        in_specs=[pl.BlockSpec(memory_space=pltpu.VMEM)],
        out_specs=pl.BlockSpec(memory_space=pltpu.VMEM),
        scratch_shapes=scratch,
        compiler_params=pltpu.CompilerParams(
            collective_id=cid, has_side_effects=True, vmem_limit_bytes=grant([(x.shape, x.dtype), out], scratch)
        ),
        name="ctx_reduce",
    )(x)


def row_cuts(rows, shares):
    tiles, total, seen, out = rows // 16, sum(shares), 0, []
    for s in shares:
        start = tiles * seen // total
        seen += s
        out.append((start * 16, (tiles * seen // total - start) * 16))
    return out


def reduce_parts(g, rows, shares):
    rest = list(range(1, len(g.dims)))
    orders = [[0] + rest, [0] + rest[::-1], rest + [0], rest[::-1] + [0]]
    return [(*cut, orders[k]) for cut, (k, _) in zip(row_cuts(rows, [s for _, s in shares]), shares) if cut[1]]


def reduce_all_kernel(g, x_ref, o_ref, kept, send, recv, gsend, grecv, psend, precv, *lands):
    g.locate()
    entry_barrier(g, True)
    f = lax.axis_index(FSDP)
    cuts = reduce_parts(g, x_ref.shape[2], SHARES)
    rs, gs = [], []
    for p, (r0, rn, order) in enumerate(cuts):
        at = (lambda r: lambda i: kept.at[i, r])(pl.ds(r0, rn))
        to = (lambda r: lambda i: o_ref.at[i, r])(pl.ds(r0, rn))
        rs.append(Reduce(g, order[::-1], at, at, lands[p], send.at[p], recv.at[p]))
        gs.append(Gather(g, order, to(g.me), to, gsend.at[p], grecv.at[p]))
    turns = [sorted(g.all, key=lambda d, a=r.order[0]: (d[a] == 0, -sum(1 for v in d if v))) for r in rs]
    pairs = {}
    for i in range(g.n):
        for p, (r0, rn, _) in enumerate(cuts):
            d = turns[p][i]
            k = g.index(d)
            at = pl.ds(r0, rn)
            c = pltpu.make_async_remote_copy(
                src_ref=x_ref.at[1 - f, k, at], dst_ref=kept.at[k, at], send_sem=psend.at[p, g.slot(d)],
                recv_sem=precv.at[p, g.slot(d)], device_id=(g.me, 1 - f), device_id_type=MESH)
            c.start()
            pairs[p, d] = c
    for i in range(g.n):
        for p, r in enumerate(rs):
            d = turns[p][i]
            k = g.index(d)
            pairs[p, d].wait_recv()
            add_into(r.acc(k), [r.acc(k), x_ref.at[f, k, pl.ds(cuts[p][0], cuts[p][1])]])
            a = r.order[0]
            if g.dims[a] == 2 and d[a]:
                r.swap(d)
    def begin(p):
        add_into(gs[p].own, [rs[p].acc(g.me)])
        gs[p].begin()

    skip = ("swap", "copy_all")
    courses = [[s for s in r.course() if getattr(s, "func", s).__name__ not in skip] for r in rs]
    for step in interleave([course + [functools.partial(begin, p)] for p, course in enumerate(courses)]):
        step()
    run_gathers(g, gs)
    for c in pairs.values():
        c.wait_send()
    for r in rs:
        r.end()
    for q in gs:
        q.end()


def reduce_all(x, n, cid):
    g = Grid(n)
    _, _, rows, cols = x.shape
    cuts = reduce_parts(g, rows, SHARES)
    parts = len(cuts)
    rooms = [Reduce.room(g, order[::-1])[1] for _, _, order in cuts]
    dma = pltpu.SemaphoreType.DMA
    scratch = [
        pltpu.VMEM((n, rows, cols), x.dtype),
        dma((parts, n)),
        dma((parts, max(rooms))),
        dma((parts, 2, n)),
        dma((parts, n)),
        dma((parts, n)),
        dma((parts, n)),
    ] + [pltpu.VMEM((room, rn, cols), x.dtype) for room, (_, rn, _) in zip(rooms, cuts)]
    out = ((n, rows, cols), x.dtype)
    return pl.pallas_call(
        functools.partial(reduce_all_kernel, g),
        out_shape=jax.ShapeDtypeStruct(*out),
        in_specs=[pl.BlockSpec(memory_space=pltpu.VMEM)],
        out_specs=pl.BlockSpec(memory_space=pltpu.VMEM),
        scratch_shapes=scratch,
        compiler_params=pltpu.CompilerParams(
            collective_id=cid, has_side_effects=True, vmem_limit_bytes=grant([out], scratch)
        ),
        name="grad_reduce",
    )(x)


def gather_kernel(g, count, spots, *refs):
    k = 2 if count else 1
    xs, ws = refs[:k], picked(refs[k : k + count], spots)
    refs = refs[k + count :]
    os, fulls = refs[:k], refs[k : k + len(spots)]
    refs = refs[k + len(spots) :]
    send, recv, local = refs[:3]
    g.locate()
    entry_barrier(g, bool(count))
    gs = []
    for p, (r0, rn, order) in enumerate(reduce_parts(g, xs[0].shape[0], SHARES)):
        at = pl.ds(r0, rn)
        slot = (lambda at: lambda i: os[0].at[i, at])(at)
        gs.append(Gather(g, order, xs[0].at[at], slot, send.at[p], recv.at[p]))
    if count:
        gs.append(Gather(g, g.orders()[0], xs[1], lambda i: os[1].at[i], send.at[len(gs)], recv.at[len(gs)]))
    for q in gs:
        q.begin()
    mine = [pltpu.make_async_copy(x, o.at[g.me], local.at[i]) for i, (x, o) in enumerate(zip(xs, os))]
    for c in mine:
        c.start()
    swap = Swap(ws, fulls, *refs[3:]) if count else None
    if count:
        swap.begin()
    run_gathers(g, gs)
    for c in mine:
        c.wait()
    if count:
        swap.end()
    for q in gs:
        q.end()


class Swap:
    def __init__(self, srcs, dsts, send, recv, load, store, *stages):
        c, f = lax.axis_index(CTX), lax.axis_index(FSDP)
        self.remote, self.loads, self.stores = [], [], []
        for i, (s, d, v) in enumerate(zip(srcs, dsts, stages)):
            self.remote.append(
                pltpu.make_async_remote_copy(
                    src_ref=s, dst_ref=d.at[f], send_sem=send.at[i], recv_sem=recv.at[i], device_id=(c, 1 - f),
                    device_id_type=MESH))
            self.loads.append(pltpu.make_async_copy(s, d.at[f] if v is None else v, load.at[i]))
            if v is not None:
                self.stores.append(pltpu.make_async_copy(v, d.at[f], store.at[i]))

    def begin(self):
        for c in self.remote + self.loads:
            c.start()
        for i, a in enumerate(self.loads):
            a.wait()
            if self.stores:
                self.stores[i].start()

    def end(self):
        for c in self.stores + self.remote:
            c.wait()

    @staticmethod
    def scratch(picks):
        return [pltpu.SemaphoreType.DMA((len(picks),))] * 4 + [pltpu.VMEM(shape_of(a, l), a.dtype) for a, l in picks]


def in_hbm(arrays):
    return [pltpu.with_memory_space_constraint(a, pltpu.HBM) for a in arrays]


def distinct(picks):
    arrays, places = [], []
    for a, l in picks:
        spot = next((i for i, b in enumerate(arrays) if b is a), None)
        if spot is None:
            spot = len(arrays)
            arrays.append(a)
        places.append((spot, l))
    return arrays, places


def picked(refs, places):
    return [refs[i] if l is None else refs[i].at[l] for i, l in places]


def shape_of(a, l):
    return a.shape if l is None else a.shape[1:]


def all_gather_ctx(x, n, cid, places=None, weights=()):
    g = Grid(n)
    arrays, spots = distinct(weights)
    count = len(arrays)
    xs = [x] if places is None else [x, places]
    dma = pltpu.SemaphoreType.DMA
    vmem, anywhere = pl.BlockSpec(memory_space=pltpu.VMEM), pl.BlockSpec(memory_space=pl.ANY)
    parts = len(SHARES) + 1
    scratch = [dma((parts, 2, n)), dma((parts, n)), dma((2,))] + (Swap.scratch(weights) if count else [])
    arrays_in_vmem = [(v.shape, v.dtype) for v in xs] + [((n, *v.shape), v.dtype) for v in xs]
    return pl.pallas_call(
        functools.partial(gather_kernel, g, count, spots),
        out_shape=[jax.ShapeDtypeStruct((n, *v.shape), v.dtype) for v in xs]
        + [jax.ShapeDtypeStruct((2, *shape_of(a, l)), a.dtype) for a, l in weights],
        in_specs=[vmem] * len(xs) + [pl.BlockSpec(memory_space=pltpu.HBM)] * count,
        out_specs=[vmem] * len(xs) + [anywhere] * len(weights),
        scratch_shapes=scratch,
        compiler_params=pltpu.CompilerParams(collective_id=cid, has_side_effects=True, vmem_limit_bytes=grant(arrays_in_vmem, scratch)),
        name="ctx_gather",
    )(*xs, *in_hbm(arrays))


def exchange_kernel(count, spots, *refs):
    srcs, dsts = picked(refs[:count], spots), refs[count : count + len(spots)]
    c, f = lax.axis_index(CTX), lax.axis_index(FSDP)
    sem = pltpu.get_barrier_semaphore()
    pl.semaphore_signal(sem, inc=1, device_id=(c, 1 - f), device_id_type=MESH)
    pl.semaphore_wait(sem, 1)
    swap = Swap(srcs, dsts, *refs[count + len(spots) :], *[None] * len(spots))
    swap.begin()
    swap.end()


def exchange(picks, cid):
    arrays, spots = distinct(picks)
    vmem = pl.BlockSpec(memory_space=pltpu.VMEM)
    outs = [((2, *shape_of(a, l)), a.dtype) for a, l in picks]
    return pl.pallas_call(
        functools.partial(exchange_kernel, len(arrays), spots),
        out_shape=[jax.ShapeDtypeStruct(*o) for o in outs],
        in_specs=[pl.BlockSpec(memory_space=pltpu.HBM)] * len(arrays),
        out_specs=[vmem] * len(picks),
        scratch_shapes=[pltpu.SemaphoreType.DMA((len(picks),))] * 4,
        compiler_params=pltpu.CompilerParams(collective_id=cid, has_side_effects=True, vmem_limit_bytes=grant(outs)),
        name="exchange",
    )(*in_hbm(arrays))


HEADS = 9
KV_HEADS = 3
HEAD = 64
GROUP = HEADS // KV_HEADS
EPS = 1e-05
ROPE_BASE = 100000.0
F32, BF16 = jnp.float32, jnp.bfloat16
CHUNK = 256
SLACK = 1 << 20


def nn(a, b):
    return lax.dot_general(a, b, (((1,), (0,)), ((), ())), preferred_element_type=F32)


def nt(a, b):
    return lax.dot_general(a, b, (((1,), (1,)), ((), ())), preferred_element_type=F32)


def tn(a, b):
    return lax.dot_general(a, b, (((0,), (0,)), ((), ())), preferred_element_type=F32)


def rms(v, gain):
    return v * lax.rsqrt(jnp.mean(v * v, axis=-1, keepdims=True) + EPS) * gain


def rms_back(v, gain, e):
    r = lax.rsqrt(jnp.mean(v * v, axis=-1, keepdims=True) + EPS)
    eg = e * gain
    dv = r * eg - v * (r * r * r) * jnp.mean(eg * v, axis=-1, keepdims=True)
    return dv, jnp.sum(e * v * r, axis=0, keepdims=True)


def rope(t, cos, sin):
    width = t.shape[1]
    out = []
    for lo in range(0, width, 128):
        w = min(128, width - lo)
        u = t[:, lo : lo + w]
        if w == 128:
            lane = lax.broadcasted_iota(jnp.int32, u.shape, 1) % HEAD
            other = jnp.where(lane < HEAD // 2, pltpu.roll(u, 128 - HEAD // 2, 1), pltpu.roll(u, HEAD // 2, 1))
        else:
            other = jnp.concatenate([u[:, HEAD // 2 :], u[:, : HEAD // 2]], axis=1)
        out.append((lo, w, u * cos[:, :w] + other * sin[:, :w]))
    return out


def padded(shape, dtype):
    size = jnp.dtype(dtype).itemsize
    dims = [1, 1, *shape]
    tile = 32 // size
    dims[-1], dims[-2] = -(-dims[-1] // 128) * 128, -(-dims[-2] // tile) * tile
    return size * math.prod(dims)


def grant(arrays, scratch=()):
    total = sum(padded(s, t) for s, t in arrays)
    for v in scratch:
        if getattr(v, "memory_space", None) == pltpu.VMEM:
            total += padded(v.shape, v.dtype)
    return min(total + SLACK, 62 << 20)


def call(kernel, outs, args, name, scratch=(), prefetch=0, blob=None):
    vmem = pl.BlockSpec(memory_space=pltpu.VMEM)
    smem = pl.BlockSpec(memory_space=pltpu.SMEM)
    anywhere = pl.BlockSpec(memory_space=pl.ANY)
    room = grant([(a.shape, a.dtype) for a in args[prefetch:]] + list(outs), scratch)
    if blob is not None:
        new = isinstance(blob, tuple)
        return pl.pallas_call(
            kernel,
            out_shape=[jax.ShapeDtypeStruct(s, t) for s, t in outs] + [jax.ShapeDtypeStruct(blob if new else blob.shape, BF16)],
            in_specs=[vmem] * len(args) + ([] if new else [anywhere]),
            out_specs=[vmem] * len(outs) + [anywhere],
            scratch_shapes=list(scratch),
            input_output_aliases={} if new else {len(args): len(outs)},
            compiler_params=pltpu.CompilerParams(vmem_limit_bytes=room),
            name=name,
        )(*args, *([] if new else [blob]))
    return pl.pallas_call(
        kernel,
        out_shape=[jax.ShapeDtypeStruct(s, t) for s, t in outs],
        in_specs=[smem] * prefetch + [vmem] * (len(args) - prefetch),
        out_specs=[vmem] * len(outs),
        scratch_shapes=list(scratch),
        compiler_params=pltpu.CompilerParams(vmem_limit_bytes=room),
        name=name,
    )(*args)


def gain_of(ref, l):
    return jnp.concatenate([ref[0, l : l + 1].astype(F32), ref[1, l : l + 1].astype(F32)], axis=1)


def rows_of(ref):
    return jnp.concatenate([ref[s].astype(F32).T for s in range(ref.shape[0])], axis=0)


def put_turned(ref, value):
    r = ref.shape[2]
    for s in range(ref.shape[0]):
        ref[s] = value[s * r : (s + 1) * r].T.astype(ref.dtype)


def pre_kernel(l, x_ref, gain_ref, wq_ref, wk_ref, wv_ref, cos_ref, sin_ref, a_ref, q_ref, kv_ref, *turned):
    if turned:
        x = rows_of(x_ref)
        turned[0][...] = x
    else:
        x = x_ref[...]
    a = rms(x, gain_of(gain_ref, l)).astype(BF16)
    a_ref[...] = a
    cos, sin = cos_ref[...], sin_ref[...]
    for lo, w, piece in rope(nn(a, wq_ref[...]), cos, sin):
        q_ref[:, lo : lo + w] = piece.astype(BF16)
    keys = jnp.concatenate([piece for _, _, piece in rope(nn(a, wk_ref[...]), cos, sin)], axis=1)
    kv_ref[...] = jnp.concatenate([keys, nn(a, wv_ref[...])], axis=1).astype(BF16)


def pre(l, x, gain, wq, wk, wv, cos, sin):
    m, d, e = cos.shape[0], wq.shape[0], wk.shape[1]
    outs = [((m, d), BF16), ((m, d), BF16), ((m, 2 * e), BF16)] + ([((m, d), F32)] if x.ndim == 3 else [])
    return call(functools.partial(pre_kernel, l), outs, (x, gain, wq, wk, wv, cos, sin), "pre")


def half_of(u, src, dst):
    if src != dst:
        u = pltpu.roll(u, HEAD, 1)
    lane = lax.broadcasted_iota(jnp.int32, u.shape, 1)
    return jnp.where((lane < HEAD) if dst == 0 else (lane >= HEAD), u, 0.0)


def head_chunk(ref, s, h):
    lo = (h // 2) * 128
    width = ref.shape[-1]
    if lo + 128 <= width:
        return ref[s, :, lo : lo + 128].astype(F32)
    u = ref[s, :, lo:width].astype(F32)
    return jnp.concatenate([u, jnp.zeros_like(u)], axis=1)


def pack_heads(ref, s, dst, g, half, scale):
    rows = ref.shape[1] // 2
    for i in range(GROUP):
        h = g * GROUP + i
        u = half_of(head_chunk(ref, s, h) * scale, h % 2, half).astype(BF16)
        for part in range(2):
            dst[g * 2 + part, i * rows : (i + 1) * rows, :] = u[part * rows : (part + 1) * rows]


def sort_rows(block_ref, s, src, dst, n, rows):
    def one(j, carry):
        b = block_ref[j, s, 0] // rows
        dst[pl.ds(pl.multiple_of(b * rows, rows), rows), :] = src[j, s, 0:rows, :]
        dst[pl.ds(pl.multiple_of((2 * n - 1 - b) * rows, rows), rows), :] = src[j, s, rows : 2 * rows, :]
        return carry

    lax.fori_loop(0, n, one, 0)


def visible(c, block, rows, shape):
    key = lax.broadcasted_iota(jnp.int32, shape, 0) + c * CHUNK
    query = lax.broadcasted_iota(jnp.int32, shape, 1) % rows + block * rows
    return key <= query


def key_lanes(g):
    return (g // 2) * 128, g % 2


def value_lanes(g):
    return ((KV_HEADS + g) // 2) * 128, (KV_HEADS + g) % 2


def turn_rows(src, lo, dst, count):
    def one(c, carry):
        at = pl.ds(pl.multiple_of(c * CHUNK, CHUNK), CHUNK)
        dst[:, at] = src[at, lo : lo + 256].astype(F32).T.astype(BF16)
        return carry

    lax.fori_loop(0, count, one, 0)


def attend_kernel(
    n, block_ref, mine_ref, q_ref, kv_ref, o_ref, lse_ref, sorted_ref, turned_ref, qp_ref, st_ref, acc_ref, stat_ref
):
    rows = q_ref.shape[1] // 2
    wide = GROUP * rows
    groups = range(KV_HEADS)
    vlo = HEAD * KV_HEADS // 128 * 128
    voff = HEAD * KV_HEADS - vlo

    def sequence(s, carry):
        sort_rows(block_ref, s, kv_ref, sorted_ref, n, rows)
        turn_rows(sorted_ref, vlo, turned_ref, n * 2 * rows // CHUNK)
        for g in groups:
            pack_heads(q_ref, s, qp_ref, g, key_lanes(g)[1], HEAD**-0.5)
        low = mine_ref[s, 0] // rows
        for part in range(2):
            block = low if part == 0 else 2 * n - 1 - low
            last = block * rows // CHUNK
            stat_ref[...] = jnp.full_like(stat_ref, -1e30)

            def score(c, masked):
                at = pl.ds(pl.multiple_of(c * CHUNK, CHUNK), CHUNK)
                for g in groups:
                    klo, _ = key_lanes(g)
                    st = nt(sorted_ref[at, klo : klo + 128], qp_ref[g * 2 + part])
                    if masked:
                        st = jnp.where(visible(c, block, rows, st.shape), st, -1e30)
                    st_ref[g, at, :] = st
                    stat_ref[g] = jnp.maximum(stat_ref[g], jnp.max(st.reshape(CHUNK // 8, 8, wide), axis=0))

            def scores(c, carry):
                score(c, False)
                return carry

            lax.fori_loop(0, last, scores, 0)
            score(last, True)
            tops = [jnp.max(stat_ref[g], axis=0, keepdims=True) for g in groups]
            stat_ref[...] = jnp.zeros_like(stat_ref)
            acc_ref[...] = jnp.zeros_like(acc_ref)

            def mix(c, tops):
                at = pl.ds(pl.multiple_of(c * CHUNK, CHUNK), CHUNK)
                for g in groups:
                    p = jnp.exp(st_ref[g, at, :] - tops[g])
                    stat_ref[g] += jnp.sum(p.reshape(CHUNK // 8, 8, wide), axis=0)
                    acc_ref[g] += nn(turned_ref[voff + g * HEAD : voff + (g + 1) * HEAD, at], p.astype(BF16))
                return tops

            tops = lax.fori_loop(0, last + 1, mix, tuple(tops))
            for g in groups:
                total = jnp.sum(stat_ref[g], axis=0, keepdims=True)
                lse_ref[s, g * 2 + part] = tops[g] + jnp.log(total)
                out = (acc_ref[g] / total).T
                for i in range(GROUP):
                    h = g * GROUP + i
                    o_ref[s, part * rows : (part + 1) * rows, h * HEAD : (h + 1) * HEAD] = out[i * rows : (i + 1) * rows]
        return carry

    lax.fori_loop(0, q_ref.shape[0], sequence, 0)


def attend(blocks, mine, q, kv):
    seqs, r, d = q.shape
    n = kv.shape[0]
    wide = GROUP * r // 2
    scratch = [
        pltpu.VMEM((n * r, kv.shape[-1]), BF16),
        pltpu.VMEM((256, n * r), BF16),
        pltpu.VMEM((2 * KV_HEADS, wide, 128), BF16),
        pltpu.VMEM((KV_HEADS, n * r, wide), F32),
        pltpu.VMEM((KV_HEADS, HEAD, wide), F32),
        pltpu.VMEM((KV_HEADS, 8, wide), F32),
    ]
    outs = [((seqs, r, d), F32), ((seqs, 2 * KV_HEADS, 1, wide), F32)]
    return call(functools.partial(attend_kernel, n), outs, (blocks, mine, q, kv), "attend", scratch, 2)


def attend_back_kernel(
    n, block_ref, mine_ref, q_ref, kv_ref, do_ref, o_ref, lse_ref, dq_ref, dkv_ref,
    sorted_ref, turned_ref, qp_ref, dop_ref, acc_ref, delta_ref, dqt_ref,
):
    rows = q_ref.shape[1] // 2
    wide = GROUP * rows
    groups = range(KV_HEADS)

    def sequence(s, carry):
        sort_rows(block_ref, s, kv_ref, sorted_ref, n, rows)
        turn_rows(sorted_ref, 0, turned_ref, n * 2 * rows // CHUNK)
        for g in groups:
            pack_heads(q_ref, s, qp_ref, g, key_lanes(g)[1], HEAD**-0.5)
            pack_heads(do_ref, s, dop_ref, g, value_lanes(g)[1], 1.0)
        acc_ref[...] = jnp.zeros_like(acc_ref)
        low = mine_ref[s, 0] // rows
        for part in range(2):
            block = low if part == 0 else 2 * n - 1 - low
            last = block * rows // CHUNK
            deltas = []
            for g in groups:
                sums = []
                for i in range(GROUP):
                    h = g * GROUP + i
                    lanes = slice(h * HEAD, (h + 1) * HEAD)
                    at = slice(part * rows, (part + 1) * rows)
                    both = do_ref[s, at, lanes].astype(F32) * o_ref[s, at, lanes]
                    sums.append(jnp.sum(both, axis=1, keepdims=True))
                delta_ref[...] = jnp.concatenate(sums, axis=0) + jnp.zeros((wide, 128), F32)
                deltas.append(delta_ref[...].T[0:1])
            dqt_ref[...] = jnp.zeros_like(dqt_ref)

            def step(c, deltas, masked):
                at = pl.ds(pl.multiple_of(c * CHUNK, CHUNK), CHUNK)
                sums = [None] * (2 * KV_HEADS * HEAD // 128)
                for g in groups:
                    klo, _ = key_lanes(g)
                    vlo, _ = value_lanes(g)
                    qp, dop = qp_ref[g * 2 + part], dop_ref[g * 2 + part]
                    p = jnp.exp(nt(sorted_ref[at, klo : klo + 128], qp) - lse_ref[s, g * 2 + part])
                    if masked:
                        p = jnp.where(visible(c, block, rows, p.shape), p, 0.0)
                    dp = nt(sorted_ref[at, vlo : vlo + 128], dop)
                    ds = (p * (dp - deltas[g])).astype(BF16)
                    for lo, v in ((vlo // 128, nn(p.astype(BF16), dop)), (klo // 128, nn(ds, qp))):
                        sums[lo] = v if sums[lo] is None else sums[lo] + v
                    dqt_ref[g] += nn(turned_ref[g * HEAD : (g + 1) * HEAD, at], ds)
                for k, v in enumerate(sums):
                    acc_ref[at, k * 128 : (k + 1) * 128] += v
                return deltas

            deltas = lax.fori_loop(0, last, lambda c, t: step(c, t, False), tuple(deltas))
            step(last, deltas, True)
            for g in groups:
                dq = dqt_ref[g].T * HEAD**-0.5
                for i in range(GROUP):
                    h = g * GROUP + i
                    dq_ref[s, part * rows : (part + 1) * rows, h * HEAD : (h + 1) * HEAD] = dq[i * rows : (i + 1) * rows]

        def one(j, carry):
            b = block_ref[j, s, 0] // rows
            dkv_ref[j, s, 0:rows, :] = acc_ref[pl.ds(pl.multiple_of(b * rows, rows), rows), :].astype(BF16)
            dkv_ref[j, s, rows : 2 * rows, :] = acc_ref[
                pl.ds(pl.multiple_of((2 * n - 1 - b) * rows, rows), rows), :
            ].astype(BF16)
            return carry

        lax.fori_loop(0, n, one, 0)
        return carry

    lax.fori_loop(0, q_ref.shape[0], sequence, 0)


def attend_back(blocks, mine, q, kv, do, o, lse):
    seqs, r, d = q.shape
    n = kv.shape[0]
    wide = GROUP * r // 2
    scratch = [
        pltpu.VMEM((n * r, kv.shape[-1]), BF16),
        pltpu.VMEM((256, n * r), BF16),
        pltpu.VMEM((2 * KV_HEADS, wide, 128), BF16),
        pltpu.VMEM((2 * KV_HEADS, wide, 128), BF16),
        pltpu.VMEM((n * r, kv.shape[-1]), F32),
        pltpu.VMEM((wide, 128), F32),
        pltpu.VMEM((KV_HEADS, HEAD, wide), F32),
    ]
    outs = [((seqs, r, d), F32), (kv.shape, BF16)]
    args = (blocks, mine, q, kv, do, o, lse)
    return call(functools.partial(attend_back_kernel, n), outs, args, "attend_back", scratch, 2)


def down_at(wd_ref, i):
    per = wd_ref.shape[2] // CHUNK
    f = i // per
    return f, pl.ds(pl.multiple_of((i - f * per) * CHUNK, CHUNK), CHUNK)


def post_kernel(l, o_ref, x_ref, wo_ref, gain_ref, wg_ref, wu_ref, wd_ref, h_ref, b_ref, gate_ref, up_ref, y_ref, *turned):
    sum_ref = turned[0] if turned else y_ref
    h = x_ref[...] + nn(o_ref[...].astype(BF16), wo_ref[...])
    h_ref[...] = h
    sum_ref[...] = h
    b_ref[...] = rms(h, gain_of(gain_ref, l)).astype(BF16)

    def some(i, carry):
        at = pl.ds(pl.multiple_of(i * CHUNK, CHUNK), CHUNK)
        b = b_ref[...]
        gate, up = nn(b, wg_ref[:, at]), nn(b, wu_ref[:, at])
        gate_ref[:, at], up_ref[:, at] = gate, up
        m = (gate * jax.nn.sigmoid(gate) * up).astype(BF16)
        f, spot = down_at(wd_ref, i)
        sum_ref[...] += nt(m, wd_ref[f, :, spot])
        return carry

    lax.fori_loop(0, wg_ref.shape[1] // CHUNK, some, 0)
    if turned:
        put_turned(y_ref, sum_ref[...])


def post(l, o, x, wo, gain, wg, wu, wd, turned=None):
    m, d = x.shape
    ff = wg.shape[1]
    outs = [((m, d), F32), ((m, d), BF16), ((m, ff), F32), ((m, ff), F32), (turned, BF16) if turned else ((m, d), F32)]
    scratch = [pltpu.VMEM((m, d), F32)] if turned else []
    return call(functools.partial(post_kernel, l), outs, (o, x, wo, gain, wg, wu, wd), "post", scratch)


def put_tiles(blob, base, value, count):
    rows = value.shape[0] // 2
    if value.shape[1] < count * 128:
        value = jnp.concatenate([value, jnp.zeros((2 * rows, count * 128 - value.shape[1]), value.dtype)], axis=1)
    for f in range(2):
        for j in range(count):
            piece = value[f * rows : (f + 1) * rows, j * 128 : (j + 1) * 128]
            blob[f, pl.ds(base + j * (rows // 16), rows // 16)] = piece.reshape(rows // 16, 16, 128)


def put_norm(blob, at, dg):
    half = dg.shape[1] // 2
    for f in range(2):
        v = dg[:, f * half : (f + 1) * half]
        v = jnp.concatenate([v, jnp.zeros((1, 384 - half), F32)], axis=1)
        rows = jnp.concatenate([v[:, 0:128], v[:, 128:256], v[:, 256:384], jnp.zeros((13, 128), F32)], axis=0)
        blob[f, at] = rows.astype(BF16)


def wide_of(cols):
    return -(-cols // 128)


def ffn_back_kernel(l, base, new, *refs):
    dy_ref, h_ref, b_ref, gate_ref, up_ref, o_ref, gain_ref, wo_ref, wg_ref, wu_ref, wd_ref = refs[:11]
    dh_ref, do_ref, out_ref, blob_ref, dyb_ref, dyt_ref, db_ref, bt_ref, sem = refs[11 if new else 12 :]
    m, d = h_ref.shape
    ff = wg_ref.shape[1]
    half = d // 2 // 16
    up_at = (ff // 128) * half
    low_at = 2 * up_at
    out_at = low_at + (ff // 256) * (d // 16)
    norm_at = out_at + wide_of(d) * half
    dy = rows_of(dy_ref) if len(dy_ref.shape) == 3 else dy_ref[...]
    dh_ref[...] = dy
    dyb_ref[...] = dy.astype(BF16)
    dyt_ref[...] = dyb_ref[...].T
    db_ref[...] = jnp.zeros_like(db_ref)
    bt_ref[...] = b_ref[...].T

    def some(i, carry):
        at = pl.ds(pl.multiple_of(i * CHUNK, CHUNK), CHUNK)
        f, spot = down_at(wd_ref, i)
        dm = nn(dyb_ref[...], wd_ref[f, :, spot])
        gate, up = gate_ref[:, at], up_ref[:, at]
        sig = jax.nn.sigmoid(gate)
        silu = gate * sig
        mid = (silu * up).astype(BF16)
        dgate = (dm * up * sig * (1.0 + gate * (1.0 - sig))).astype(BF16)
        dup = (dm * silu).astype(BF16)
        db_ref[...] += nt(dgate, wg_ref[:, at]) + nt(dup, wu_ref[:, at])
        bt = bt_ref[...]
        put_tiles(blob_ref, i * (CHUNK // 128) * half, nn(bt, dgate).astype(BF16), CHUNK // 128)
        put_tiles(blob_ref, up_at + i * (CHUNK // 128) * half, nn(bt, dup).astype(BF16), CHUNK // 128)
        gd = nn(dyt_ref[...], mid).astype(BF16)
        per = wd_ref.shape[2] // CHUNK
        for j in range(CHUNK // 128):
            start = low_at + ((i - f * per) * (CHUNK // 128) + j) * (d // 16)
            blob_ref[f, pl.ds(start, d // 16)] = gd[:, j * 128 : (j + 1) * 128].reshape(d // 16, 16, 128)
        return carry

    lax.fori_loop(0, ff // CHUNK, some, 0)
    first = pltpu.make_async_copy(blob_ref.at[:, pl.ds(0, out_at)], out_ref.at[:, pl.ds(base, out_at)], sem.at[0])
    first.start()
    dv, dg = rms_back(h_ref[...], gain_of(gain_ref, l), db_ref[...])
    dh = dh_ref[...] + dv
    dh_ref[...] = dh
    dhb = dh.astype(BF16)
    do_ref[...] = nt(dhb, wo_ref[...]).astype(BF16)
    put_tiles(blob_ref, out_at, tn(o_ref[...].astype(BF16), dhb).astype(BF16), wide_of(d))
    put_norm(blob_ref, norm_at, dg)
    rest = norm_at + 1 - out_at
    second = pltpu.make_async_copy(
        blob_ref.at[:, pl.ds(out_at, rest)], out_ref.at[:, pl.ds(base + out_at, rest)], sem.at[1]
    )
    second.start()
    first.wait()
    second.wait()


def ffn_tiles(d, ff):
    return 2 * (ff // 128) * (d // 32) + (ff // 256) * (d // 16) + wide_of(d) * (d // 32) + 1


def ffn_back(l, blob, base, dy, h, b, gate, up, o, gain, wo, wg, wu, wd):
    m, d = h.shape
    ff = wg.shape[1]
    scratch = [
        pltpu.VMEM((2, ffn_tiles(d, ff), 16, 128), BF16),
        pltpu.VMEM((m, d), BF16),
        pltpu.VMEM((d, m), BF16),
        pltpu.VMEM((m, d), F32),
        pltpu.VMEM((d, m), BF16),
        pltpu.SemaphoreType.DMA((2,)),
    ]
    kernel = functools.partial(ffn_back_kernel, l, base, isinstance(blob, tuple))
    args = (dy, h, b, gate, up, o, gain, wo, wg, wu, wd)
    return call(kernel, [((m, d), F32), ((m, d), BF16)], args, "ffn_back", scratch, blob=blob)


def pre_tiles(d, e):
    return wide_of(d) * (d // 32) + wide_of(2 * e) * (d // 32) + 1


def pre_back_kernel(l, base, *refs):
    dq_ref, dkv_ref, a_ref, x_ref, dh_ref, gain_ref, wq_ref, wk_ref, wv_ref, cos_ref, sin_ref = refs[:11]
    dx_ref, out_ref, blob_ref, dqp_ref, sem = refs[12:]
    d = x_ref.shape[1]
    e = wk_ref.shape[1]
    half = d // 2 // 16
    cos, sin = cos_ref[...], -sin_ref[...]
    for lo, w, piece in rope(dq_ref[...], cos, sin):
        dqp_ref[:, lo : lo + w] = piece.astype(BF16)
    dqp = dqp_ref[...]
    dkv = dkv_ref[...]
    dkp = jnp.concatenate([piece for _, _, piece in rope(dkv[:, :e], cos, sin)], axis=1).astype(BF16)
    dvr = dkv[:, e:].astype(BF16)
    da = nt(dqp, wq_ref[...]) + nt(dkp, wk_ref[...]) + nt(dvr, wv_ref[...])
    dv, dg = rms_back(x_ref[...], gain_of(gain_ref, l), da)
    kv_at = wide_of(d) * half
    norm_at = kv_at + wide_of(2 * e) * half
    put_norm(blob_ref, norm_at, dg)
    left = blob_ref.shape[1] - norm_at - 1
    if left:
        blob_ref[:, pl.ds(norm_at + 1, left)] = jnp.zeros((2, left, 16, 128), BF16)
    at = a_ref[...].T
    put_tiles(blob_ref, 0, nn(at, dqp).astype(BF16), wide_of(d))
    put_tiles(blob_ref, kv_at, jnp.concatenate([nn(at, dkp), nn(at, dvr)], axis=1).astype(BF16), wide_of(2 * e))
    done = pltpu.make_async_copy(blob_ref, out_ref.at[:, pl.ds(base, blob_ref.shape[1])], sem)
    done.start()
    if len(dx_ref.shape) == 3:
        put_turned(dx_ref, dh_ref[...] + dv)
    else:
        dx_ref[...] = dh_ref[...] + dv
    done.wait()


def pre_back(l, shape, blob, base, tiles, dq, dkv, a, x, dh, gain, wq, wk, wv, cos, sin):
    m, d = x.shape
    scratch = [pltpu.VMEM((2, tiles, 16, 128), BF16), pltpu.VMEM((m, d), BF16), pltpu.SemaphoreType.DMA(())]
    args = (dq, dkv, a, x, dh, gain, wq, wk, wv, cos, sin)
    return call(functools.partial(pre_back_kernel, l, base), [(shape, F32)], args, "pre_back", scratch, blob=blob)


def unpack_kernel(places, blob, *outs):
    g_attn, gq, gk, gv, go, g_ffn, gg, gu, gd = outs
    half, d, e, ff = gq.shape[1], gq.shape[2], gk.shape[2], gg.shape[2]
    t = half // 16

    def take(base, at, rows, cols, out, l, skip=0):
        for lo in range(0, cols, 128):
            w = min(128, cols - lo)
            j = (skip + lo) // 128
            if (skip + lo) % 128 == 0:
                u = blob[pl.ds(base + at + j * (rows // 16), rows // 16)].reshape(rows, 128)[:, :w]
            else:
                u = blob[pl.ds(base + at + j * (rows // 16), rows // 16)].reshape(rows, 128)[:, 64:]
                if w > 64:
                    v = blob[pl.ds(base + at + (j + 1) * (rows // 16), rows // 16)].reshape(rows, 128)[:, : w - 64]
                    u = jnp.concatenate([u.astype(F32), v.astype(F32)], axis=1)
            out[l, :, lo : lo + w] = u.astype(F32)

    def norm(base, at, out, l):
        u = blob[base + at].astype(F32)
        row = jnp.concatenate([u[0:1], u[1:2], u[2:3]], axis=1)
        out[l : l + 1, :] = row[:, :half]

    for l, (ffn, att) in enumerate(places):
        up_at = (ff // 128) * t
        low_at = 2 * up_at
        out_at = low_at + (ff // 256) * (d // 16)
        take(ffn, 0, half, ff, gg, l)
        take(ffn, up_at, half, ff, gu, l)
        take(ffn, low_at, d, ff // 2, gd, l)
        take(ffn, out_at, half, d, go, l)
        norm(ffn, out_at + wide_of(d) * t, g_ffn, l)
        take(att, 0, half, d, gq, l)
        kv_at = wide_of(d) * t
        take(att, kv_at, half, e, gk, l)
        take(att, kv_at, half, e, gv, l, e)
        norm(att, kv_at + wide_of(2 * e) * t, g_attn, l)


def unpack(blob, places, shapes):
    return call(functools.partial(unpack_kernel, places), [(s, F32) for s in shapes], (blob,), "unpack")


def body(tokens, positions, norm_attn, w_query, w_key, w_value, w_out, norm_ffn, w_gate, w_up, w_down, cotangent):
    layers = norm_attn.shape[0]
    n = lax.axis_size(CTX)
    seqs, r, d = tokens.shape
    m = seqs * r
    e, ff = w_key.shape[2], w_gate.shape[2]
    own = (w_query, w_key, w_value, w_out, w_gate, w_up, jnp.swapaxes(w_down, 1, 2))
    shards = [(w, l) for l in range(layers) for w in own]
    full = exchange([(norm_attn, None), (norm_ffn, None), *shards[:3]], 0)
    gain_attn, gain_ffn, *full = full
    frequency = jnp.exp(jnp.arange(HEAD // 2, dtype=F32) * (-jnp.log(ROPE_BASE) / (HEAD // 2)))
    angles = positions.reshape(m, 1).astype(F32) * frequency
    cos, sin = jnp.cos(angles), jnp.sin(angles)
    cos = jnp.concatenate([cos] * 4, axis=1)
    sin = jnp.concatenate([-sin, sin] * 2, axis=1)
    x = jnp.swapaxes(tokens, 1, 2)
    kept = []
    weights = []

    def joined(w):
        return w.reshape(2 * w.shape[1], w.shape[2])

    for l in range(layers):
        wq, wk, wv = (joined(w) for w in full[l * len(own) : l * len(own) + 3])
        a, q, kv, *turned = pre(l, x, gain_attn, wq, wk, wv, cos, sin)
        if turned:
            (x,) = turned
        q = q.reshape(seqs, r, d)
        if l == 0:
            kv, places, *rest = all_gather_ctx(kv, n, 1, positions, shards[3:])
            full = [*full, *rest]
        else:
            (kv,) = all_gather_ctx(kv, n, 1 + l)
        wo, wg, wu = (joined(w) for w in full[l * len(own) + 3 : l * len(own) + 6])
        wd = full[l * len(own) + 6]
        weights.append((wq, wk, wv, wo, wg, wu, wd))
        kv = kv.reshape(n, seqs, r, 2 * e)
        o, lse = attend(places, positions, q, kv)
        turned = (seqs, d, r) if l == layers - 1 else None
        h, b, gate, up, y = post(l, o.reshape(m, d), x, wo, gain_ffn, wg, wu, wd, turned)
        kept.append((x, a, q, kv, o, lse, h, b, gate, up))
        x = y
    output = jnp.swapaxes(x, 1, 2)
    dy = jnp.swapaxes(cotangent, 1, 2)
    one, two = ffn_tiles(d, ff), pre_tiles(d, e)
    unit = 2 * n
    whole = -(-layers * (one + two) // unit) * unit
    blob = (2, whole, 16, 128)
    spots = []
    for l in reversed(range(layers)):
        wq, wk, wv, wo, wg, wu, wd = weights[l]
        x, a, q, kv, o, lse, h, b, gate, up = kept[l]
        start = (layers - 1 - l) * (one + two)
        spots.insert(0, (start, start + one))
        dh, do, blob = ffn_back(l, blob, start, dy, h, b, gate, up, o.reshape(m, d), gain_ffn, wo, wg, wu, wd)
        dq, dkv = attend_back(places, positions, q, kv, do.reshape(seqs, r, d), o, lse)
        dkv = reduce_scatter_ctx(dkv.reshape(n, m, 2 * e), n, 1 + layers + l)
        tiles = two if l else whole - start - one
        shape = (m, d) if l else (seqs, d, r)
        dy, blob = pre_back(
            l, shape, blob, start + one, tiles, dq.reshape(m, d), dkv, a, x, dh, gain_attn, wq, wk, wv, cos, sin
        )
    total = reduce_all(blob.reshape(2, n, -1, 128), n, 1 + 2 * layers)
    shapes = [norm_attn.shape, *[w.shape for w in own[:4]], norm_ffn.shape, *[w.shape for w in own[4:]]]
    grads = unpack(total.reshape(whole, 16, 128), spots, shapes)
    return (output, jnp.swapaxes(dy, 1, 2), *grads[:-1], jnp.swapaxes(grads[-1], 1, 2))


def solution(mesh):
    in_specs = (
        P("fsdp", "ctx", None),
        P("fsdp", "ctx"),
        P(None, "fsdp"),
        P(None, "fsdp", None),
        P(None, "fsdp", None),
        P(None, "fsdp", None),
        P(None, "fsdp", None),
        P(None, "fsdp"),
        P(None, "fsdp", None),
        P(None, "fsdp", None),
        P(None, "fsdp", None),
        P("fsdp", "ctx", None),
    )
    out_specs = (
        P("fsdp", "ctx", None),
        P("fsdp", "ctx", None),
        P(None, "fsdp"),
        P(None, "fsdp", None),
        P(None, "fsdp", None),
        P(None, "fsdp", None),
        P(None, "fsdp", None),
        P(None, "fsdp"),
        P(None, "fsdp", None),
        P(None, "fsdp", None),
        P(None, "fsdp", None),
    )
    return jax.shard_map(body, mesh=mesh, in_specs=in_specs, out_specs=out_specs, check_vma=False)
```
